32 devices in a mesh: chan: 4 (over y, x), tm: 8 (over z, core).
Axes of the slice: x: 2, y: 2, z: 4, core: 2. Of those that a mesh axis runs over, the one named last changes fastest.
Arguments:
- volts: bfloat16 [4, 2048, 512], P('chan', 'tm'), may hold values from -120 to 120
- picks: int32 [4, 8], P('chan'), may hold values from 0 to 63, as said below
- angles: float32 [64], replicated, may hold values from -3.140625 to 3.140625
Outputs:
- cleaned: float32 [4, 2048, 512], P('chan', 'tm')
The draws below stay inside these ranges and needn't reach their ends.
Inputs may be any that keep to these rules, and one draw needn't show every extreme that they name: No index appears twice among all groups' picks.
All inputs are finite; a program needn't handle non-finite values.
Results may differ from the reference program's by a relative error of at most 0.00035.
Values sent between devices are 32-bit elements; how exact they have to be, the bound alone decides.
No kernel may reach another device: no remote copies, remote signals or barrier semaphores. Data moves between devices by JAX's collectives and lax.ppermute only.
A program may use at most 64 MiB of HBM per device.

```python
import math
import jax
import jax.numpy as jnp
from jax import lax

M = 256
SEG = 256
HORIZON = 256
SEGS_DEV = 1
K = 8
DIRS = 64
WSTEPS = 4
GROUPS = 4
SAMPLES = 2048
N_TM = 8


def draw_volts(key, part):
    base_key = jax.random.fold_in(key, 11)
    scale_key = jax.random.fold_in(key, 12)
    group_scale = (3.0 ** (jnp.arange(GROUPS).astype(jnp.float32) / max(GROUPS - 1, 1)))[:, None, None]
    base = jax.random.truncated_normal(base_key, -4.0, 4.0, (GROUPS, SAMPLES, 2 * M), jnp.float32)
    row_scale = jnp.exp(jax.random.uniform(scale_key, (GROUPS, SAMPLES, 1), jnp.float32, 0.0, math.log(10.0)))
    return jnp.clip(base * row_scale * group_scale, -120.0, 120.0).astype(jnp.bfloat16)


def draw_picks(key, part):
    order = jax.random.permutation(jax.random.fold_in(key, 21), DIRS)
    return order[:GROUPS * K].reshape(GROUPS, K).astype(jnp.int32)


def setup_inputs(seed: int = 0) -> dict:
    splits = jax.random.split(jax.random.key(seed), 4)
    return {
        "volts": draw_volts(jax.random.fold_in(splits[3], 71), 0),
        "picks": draw_picks(jax.random.fold_in(splits[3], 71), 0),
        "angles": jnp.clip(jax.random.uniform(splits[2], (DIRS,), jnp.float32, -3.140625, 3.140625), -3.140625, 3.140625),
    }


LOADING = 0.1
STEER_LOADING = 0.05
TINY_LEVEL = 1e-06
PRECISE = lax.Precision.HIGHEST

def steering_rows(angle_sel, antennas):
    position = jnp.arange(antennas).astype(jnp.float32)
    phase = jnp.pi * jnp.sin(angle_sel)[:, None] * position[None, :]
    norming = jnp.sqrt(jnp.asarray(antennas, jnp.float32))
    real_part = jnp.cos(phase) / norming
    imag_part = jnp.sin(phase) / norming
    upper = jnp.concatenate([real_part, imag_part], axis=1)
    lower = jnp.concatenate([-imag_part, real_part], axis=1)
    return jnp.concatenate([upper, lower], axis=0)

def null_factor(steer_rows):
    count = steer_rows.shape[0]
    steer_gram = jnp.dot(steer_rows, steer_rows.T, precision=PRECISE) + STEER_LOADING * jnp.eye(count, dtype=jnp.float32)
    chol_gram = jnp.linalg.cholesky(steer_gram)
    return jax.scipy.linalg.solve_triangular(chol_gram, steer_rows, lower=True)

def segment_term(voltage, forget):
    segments = voltage.shape[0] // SEG
    pieces = voltage.astype(jnp.float32).reshape(segments, SEG, voltage.shape[1])
    seg_grams = jnp.einsum('sli,slj->sij', pieces, pieces, precision=PRECISE)
    powers = (segments - 1 - jnp.arange(segments)).astype(jnp.float32)
    return jnp.einsum('s,sij->ij', jnp.power(forget, powers), seg_grams, precision=PRECISE)

def halves(full_gram, antennas):
    real_half = full_gram[:antennas, :antennas] + full_gram[antennas:, antennas:]
    imag_half = full_gram[antennas:, :antennas] - full_gram[:antennas, antennas:]
    return jnp.stack([real_half, imag_half])

def solve_block(voltage, covariance, band_level, null_rows):
    antennas = covariance.shape[1]
    volt_float = voltage.astype(jnp.float32)
    inner = jnp.dot(volt_float, null_rows.T, precision=PRECISE)
    projected = volt_float - jnp.dot(inner, null_rows, precision=PRECISE)
    upper = jnp.concatenate([covariance[0], -covariance[1]], axis=1)
    lower = jnp.concatenate([covariance[1], covariance[0]], axis=1)
    loaded = jnp.concatenate([upper, lower], axis=0) / band_level + LOADING * jnp.eye(2 * antennas, dtype=jnp.float32)
    omega = 1.0 / jnp.sqrt(jnp.sum(loaded * loaded))
    iterate = omega * projected
    for sweep in range(WSTEPS):
        iterate = iterate + omega * (projected - jnp.dot(iterate, loaded, precision=PRECISE))
    return iterate

def reference(volts, picks, angles):
    antennas = volts.shape[2] // 2
    rows_dev = SEG * SEGS_DEV
    forget = jnp.asarray(1.0 - 1.0 / HORIZON, jnp.float32)
    forget_dev = jnp.power(forget, jnp.asarray(SEGS_DEV, jnp.float32))
    blocks = volts.reshape(GROUPS * N_TM, rows_dev, 2 * antennas)
    terms = lax.map(lambda voltage: halves(segment_term(voltage, forget), antennas), blocks)
    terms = jnp.swapaxes(terms.reshape(GROUPS, N_TM, 2, antennas, antennas), 0, 1)

    def advance(state_sum, term_now):
        state_sum = forget_dev * state_sum + term_now
        return (state_sum, state_sum)
    _, covs = lax.scan(advance, jnp.zeros_like(terms[0]), terms)
    power_level = jnp.trace(covs[:, :, 0], axis1=-2, axis2=-1) / antennas
    band_level = lax.optimization_barrier(jnp.mean(power_level, axis=1)) + TINY_LEVEL
    null_all = lax.map(lambda angle_sel: null_factor(steering_rows(angle_sel, antennas)), angles[picks])
    outputs = []
    for group in range(GROUPS):
        group_blocks = blocks[group * N_TM:(group + 1) * N_TM]
        null_rows = null_all[group]
        cleaned = lax.map(lambda entry: solve_block(entry[0], entry[1], entry[2], null_rows), (group_blocks, covs[:, group], band_level))
        outputs.append(cleaned.reshape(N_TM * rows_dev, 2 * antennas))
    return jnp.stack(outputs)
```

```python
import jax
import jax.numpy as jnp
from jax import lax
from jax.experimental import pallas as pl
from jax.experimental.pallas import tpu as pltpu
from jax.sharding import PartitionSpec as P

SEG = 256
HORIZON = 256
LOADING = 0.1
STEER_LOADING = 0.05
TINY_LEVEL = 1e-06
PRECISE = lax.Precision.HIGHEST
RADIX = 4
F32 = jnp.float32
BF16 = jnp.bfloat16
VM = pl.BlockSpec(memory_space=pltpu.VMEM)
SM = pl.BlockSpec(memory_space=pltpu.SMEM)


def gram_kernel(parity_ref, volts_ref, keep_ref, give_ref, power_ref, mixed_ref):
    antennas = volts_ref.shape[1] // 2
    segments = volts_ref.shape[0] // SEG
    half = antennas // 2
    forget = 1.0 - 1.0 / HORIZON
    mixed = None
    for seg in range(segments):
        a = volts_ref[seg * SEG : (seg + 1) * SEG, :antennas]
        b = volts_ref[seg * SEG : (seg + 1) * SEG, antennas:]
        left = jnp.concatenate([a, b, b, -a], axis=0)
        right = jnp.concatenate([a, b, a, b], axis=0)
        term = lax.dot_general(
            left, right, (((0,), (0,)), ((), ())), preferred_element_type=F32
        )
        mixed = term if mixed is None else forget * mixed + term
    mixed_ref[...] = mixed
    row = lax.broadcasted_iota(jnp.int32, mixed.shape, 0)
    column = lax.broadcasted_iota(jnp.int32, mixed.shape, 1)
    trace = jnp.sum(jnp.where(row == column, mixed, 0.0))
    power_ref[...] = jnp.full(power_ref.shape, trace / antennas, F32)
    parity = parity_ref[0]
    keep_ref[...] = mixed_ref[pl.ds(pl.multiple_of(parity * half, half), half), :]
    give_ref[...] = mixed_ref[pl.ds(pl.multiple_of((1 - parity) * half, half), half), :]


def split(value):
    high = value.astype(BF16)
    return high, (value - high.astype(F32)).astype(BF16)


def dot3(left, right):
    (lh, ll), (rh, rl) = left, right
    return (
        jnp.dot(lh, rh, preferred_element_type=F32)
        + jnp.dot(lh, rl, preferred_element_type=F32)
        + jnp.dot(ll, rh, preferred_element_type=F32)
    )


def stacked(high_low, first, second):
    return tuple(
        jnp.concatenate(
            [
                jnp.concatenate([part[first], part[second]], axis=1),
                jnp.concatenate([part[second], -part[first]], axis=1),
            ],
            axis=0,
        )
        for part in high_low
    )


def whiten_kernel(parity_ref, band_ref, own_ref, other_ref, w_ref, out_ref, mixed_ref):
    half, antennas = own_ref.shape
    parity = parity_ref[0]
    mixed_ref[pl.ds(pl.multiple_of(parity * half, half), half), :] = own_ref[...]
    mixed_ref[pl.ds(pl.multiple_of((1 - parity) * half, half), half), :] = other_ref[...]
    mixed = mixed_ref[...]
    flipped = mixed.T
    scale = 0.5 / band_ref[0:1, 0:1]
    row = lax.broadcasted_iota(jnp.int32, mixed.shape, 0)
    column = lax.broadcasted_iota(jnp.int32, mixed.shape, 1)
    re = (mixed + flipped) * scale + jnp.where(row == column, LOADING, 0.0)
    im = (mixed - flipped) * scale
    omega = 1.0 / jnp.sqrt(2.0 * jnp.sum(re * re + im * im, keepdims=True))
    a_re, a_im = omega * re, omega * im
    (rh, rl), (ih, il) = split(a_re), split(a_im)
    lhs = tuple(
        jnp.concatenate(
            [jnp.concatenate([r, -i], axis=1), jnp.concatenate([i, r], axis=1)], axis=0
        )
        for r, i in ((rh, ih), (rl, il))
    )
    a_col = jnp.concatenate([a_re, a_im], axis=0)
    a_high, a_low = jnp.concatenate([rh, ih], axis=0), jnp.concatenate([rl, il], axis=0)
    square = dot3(lhs, (a_high, a_low))
    first, second = split(square - 2.0 * a_col), split(3.0 * a_col - square)
    samples = w_ref.shape[0]
    left, right = slice(0, antennas), slice(antennas, 2 * antennas)

    def turn(u, v):
        parts = zip(split(u), split(v), strict=True)
        return tuple(
            jnp.concatenate(
                [jnp.concatenate([p, q], axis=1), jnp.concatenate([q, -p], axis=1)], axis=0
            )
            for p, q in parts
        )

    w_u, w_v = w_ref[:, left], w_ref[:, right]
    step = dot3(turn(w_u, w_v), first)
    u, v = 2.0 * w_u + step[:samples], 2.0 * w_v + step[samples:]
    step = dot3(turn(u, v), second)
    out_ref[:, left] = omega * (w_u + 2.0 * u - step[:samples])
    out_ref[:, right] = omega * (w_v + 2.0 * v - step[samples:])


def steering_rows(angle_sel, antennas):
    position = jnp.arange(antennas).astype(F32)
    phase = jnp.pi * jnp.sin(angle_sel)[:, None] * position[None, :]
    norming = jnp.sqrt(jnp.asarray(antennas, F32))
    real_part = jnp.cos(phase) / norming
    imag_part = jnp.sin(phase) / norming
    upper = jnp.concatenate([real_part, imag_part], axis=1)
    lower = jnp.concatenate([-imag_part, real_part], axis=1)
    return jnp.concatenate([upper, lower], axis=0)


def null_factor(steer_rows):
    count = steer_rows.shape[0]
    steer_gram = jnp.dot(steer_rows, steer_rows.T, precision=PRECISE) + STEER_LOADING * jnp.eye(
        count, dtype=F32
    )
    chol_gram = jnp.linalg.cholesky(steer_gram)
    return jax.scipy.linalg.solve_triangular(chol_gram, steer_rows, lower=True)


def swap_cores(value, members):
    return lax.ppermute(value, "tm", [(i, i ^ 1) for i in range(members)])


def earlier_chips(value, members, decay):
    chips = members // 2
    stride, window, total = 1, value, None
    while stride < chips:
        gained = None
        for step in range(1, RADIX):
            shift = 2 * stride * step
            if shift >= members:
                break
            got = lax.ppermute(window, "tm", [(i, i + shift) for i in range(members - shift)])
            got = got if step == 1 else decay ** (stride * (step - 1)) * got
            gained = got if gained is None else gained + got
        total = gained if total is None else total + decay ** (stride - 1) * gained
        window = window + decay**stride * gained
        stride *= RADIX
    return jnp.zeros_like(value) if total is None else total


def sum_groups(value):
    groups = lax.axis_size("chan")
    if groups & (groups - 1):
        return lax.psum(value, "chan")
    step = 1
    while step < groups:
        value = value + lax.ppermute(value, "chan", [(i, i ^ step) for i in range(groups)])
        step *= 2
    return value


def on_device(volts, picks, angles):
    voltage = volts[0]
    rows, width = voltage.shape
    antennas = width // 2
    half = antennas // 2
    segments = rows // SEG
    members = lax.axis_size("tm")
    odd = lax.axis_index("tm") % 2
    parity = odd.reshape(1).astype(jnp.int32)
    is_odd = odd == 1
    decay = (1.0 - 1.0 / HORIZON) ** segments

    keep, give, power = pl.pallas_call(
        gram_kernel,
        out_shape=(
            jax.ShapeDtypeStruct((half, antennas), F32),
            jax.ShapeDtypeStruct((half, antennas), F32),
            jax.ShapeDtypeStruct((8, 128), F32),
        ),
        in_specs=[SM, VM],
        out_specs=(VM, VM, VM),
        scratch_shapes=[pltpu.VMEM((antennas, antennas), F32)],
        cost_estimate=pl.CostEstimate(
            flops=4 * rows * width * antennas, bytes_accessed=rows * width * 2, transcendentals=0
        ),
        name="segment_gram",
    )(parity, voltage)

    got = swap_cores(give, members)
    mine, theirs = jnp.where(is_odd, 1.0, decay), jnp.where(is_odd, decay, 1.0)
    pair = mine * keep + theirs * got
    before = earlier_chips(pair, members, decay * decay)
    even_cov = decay * before + jnp.where(is_odd, got, keep)
    odd_cov = decay * decay * before + pair
    own = jnp.where(is_odd, odd_cov, even_cov)
    other = swap_cores(jnp.where(is_odd, even_cov, odd_cov), members)

    level = sum_groups(power)
    level_before = earlier_chips(level, members, decay * decay)
    got_level = swap_cores(jnp.stack([level, level_before]), members)
    level_even = jnp.where(is_odd, got_level, jnp.stack([level, level_before]))
    level_odd = jnp.where(is_odd, jnp.stack([level, level_before]), got_level)
    level_chips = decay * level_even[1] + level_odd[1]
    level_own = decay * level_chips + level_even[0]
    level_own = jnp.where(is_odd, decay * level_own + level_odd[0], level_own)
    band = level_own / lax.axis_size("chan") + TINY_LEVEL

    selector = (picks[0][:, None] == jnp.arange(angles.shape[0], dtype=jnp.int32)[None, :]).astype(F32)
    angle_sel = jnp.dot(selector, angles, precision=PRECISE)
    null_rows = null_factor(steering_rows(angle_sel, antennas))
    volt_float = voltage.astype(F32)
    inner = jnp.dot(volt_float, null_rows.T, precision=PRECISE)
    projected = volt_float - jnp.dot(inner, null_rows, precision=PRECISE)

    cleaned = pl.pallas_call(
        whiten_kernel,
        out_shape=jax.ShapeDtypeStruct((rows, width), F32),
        in_specs=[SM, VM, VM, VM, VM],
        out_specs=VM,
        scratch_shapes=[pltpu.VMEM((antennas, antennas), F32)],
        cost_estimate=pl.CostEstimate(
            flops=18 * rows * width * width, bytes_accessed=rows * width * 8, transcendentals=0
        ),
        name="whiten",
    )(parity, band, own, other, projected)
    return cleaned[None]


def solution(mesh):
    placed = (P("chan", "tm", None), P("chan", None), P())
    return jax.shard_map(
        on_device, mesh=mesh, in_specs=placed, out_specs=P("chan", "tm", None), check_vma=False
    )
```

```python
import jax
import jax.numpy as jnp
from jax import lax
from jax.experimental import pallas as pl
from jax.experimental.pallas import tpu as pltpu
from jax.sharding import PartitionSpec as P


SEG = 256
HORIZON = 256
LOADING = 0.1
STEER_LOADING = 0.05
TINY_LEVEL = 1e-06
PRECISE = lax.Precision.HIGHEST
RADIX = 4
F32 = jnp.float32
BF16 = jnp.bfloat16
VM = pl.BlockSpec(memory_space=pltpu.VMEM)
SM = pl.BlockSpec(memory_space=pltpu.SMEM)
PARAMS = pltpu.CompilerParams(vmem_limit_bytes=24 * 2**20)


def gram_kernel(parity_ref, volts_ref, keep_ref, give_ref, power_ref, mixed_ref):
    antennas = volts_ref.shape[1] // 2
    segments = volts_ref.shape[0] // SEG
    half = antennas // 2
    forget = 1.0 - 1.0 / HORIZON
    mixed = None
    for seg in range(segments):
        a = volts_ref[seg * SEG : (seg + 1) * SEG, :antennas]
        b = volts_ref[seg * SEG : (seg + 1) * SEG, antennas:]
        left = jnp.concatenate([a, b, b, -a], axis=0)
        right = jnp.concatenate([a, b, a, b], axis=0)
        term = lax.dot_general(
            left, right, (((0,), (0,)), ((), ())), preferred_element_type=F32
        )
        mixed = term if mixed is None else forget * mixed + term
    mixed_ref[...] = mixed
    row = lax.broadcasted_iota(jnp.int32, mixed.shape, 0)
    column = lax.broadcasted_iota(jnp.int32, mixed.shape, 1)
    trace = jnp.sum(jnp.where(row == column, mixed, 0.0))
    power_ref[...] = jnp.full(power_ref.shape, trace / antennas, F32)
    parity = parity_ref[0]
    keep_ref[...] = mixed_ref[pl.ds(pl.multiple_of(parity * half, half), half), :]
    give_ref[...] = mixed_ref[pl.ds(pl.multiple_of((1 - parity) * half, half), half), :]


def split(value):
    high = value.astype(BF16)
    return high, (value - high.astype(F32)).astype(BF16)


def dot3(left, right):
    (lh, ll), (rh, rl) = left, right
    return (
        jnp.dot(lh, rh, preferred_element_type=F32)
        + jnp.dot(lh, rl, preferred_element_type=F32)
        + jnp.dot(ll, rh, preferred_element_type=F32)
    )


def whiten_kernel(parity_ref, band_ref, own_ref, other_ref, w_ref, out_ref, mixed_ref):
    half, antennas = own_ref.shape
    parity = parity_ref[0]
    mixed_ref[pl.ds(pl.multiple_of(parity * half, half), half), :] = own_ref[...]
    mixed_ref[pl.ds(pl.multiple_of((1 - parity) * half, half), half), :] = other_ref[...]
    mixed = mixed_ref[...]
    flipped = mixed.T
    scale = 0.5 / band_ref[0:1, 0:1]
    row = lax.broadcasted_iota(jnp.int32, mixed.shape, 0)
    column = lax.broadcasted_iota(jnp.int32, mixed.shape, 1)
    re = (mixed + flipped) * scale + jnp.where(row == column, LOADING, 0.0)
    im = (mixed - flipped) * scale
    omega = 1.0 / jnp.sqrt(2.0 * jnp.sum(re * re + im * im, keepdims=True))
    a_re, a_im = omega * re, omega * im
    (rh, rl), (ih, il) = split(a_re), split(a_im)
    lhs = tuple(
        jnp.concatenate(
            [jnp.concatenate([r, -i], axis=1), jnp.concatenate([i, r], axis=1)], axis=0
        )
        for r, i in ((rh, ih), (rl, il))
    )
    a_col = jnp.concatenate([a_re, a_im], axis=0)
    a_high, a_low = jnp.concatenate([rh, ih], axis=0), jnp.concatenate([rl, il], axis=0)
    square = dot3(lhs, (a_high, a_low))
    first, second = split(square - 2.0 * a_col), split(3.0 * a_col - square)
    samples = w_ref.shape[0]
    left, right = slice(0, antennas), slice(antennas, 2 * antennas)

    def turn(u, v):
        parts = zip(split(u), split(v), strict=True)
        return tuple(
            jnp.concatenate(
                [jnp.concatenate([p, q], axis=1), jnp.concatenate([q, -p], axis=1)], axis=0
            )
            for p, q in parts
        )

    w_u, w_v = w_ref[:, left], w_ref[:, right]
    step = dot3(turn(w_u, w_v), first)
    u, v = 2.0 * w_u + step[:samples], 2.0 * w_v + step[samples:]
    step = dot3(turn(u, v), second)
    out_ref[:, left] = omega * (w_u + 2.0 * u - step[:samples])
    out_ref[:, right] = omega * (w_v + 2.0 * v - step[samples:])


def complex_inverse(re, im):
    size = re.shape[0]
    row = lax.broadcasted_iota(jnp.int32, re.shape, 0)
    column = lax.broadcasted_iota(jnp.int32, re.shape, 1)
    for j in range(size):
        here = column[:1] == j
        col_re, col_im = re[:, j : j + 1], im[:, j : j + 1]
        scale = 1.0 / re[j : j + 1, j : j + 1]
        row_re = jnp.where(here, scale, re[j : j + 1] * scale)
        row_im = jnp.where(here, 0.0, im[j : j + 1] * scale)
        rest_re, rest_im = jnp.where(column == j, 0.0, re), jnp.where(column == j, 0.0, im)
        rest_re = rest_re - (col_re * row_re - col_im * row_im)
        rest_im = rest_im - (col_re * row_im + col_im * row_re)
        re = jnp.where(row == j, row_re, rest_re)
        im = jnp.where(row == j, row_im, rest_im)
    return re, im


def across(left, right):
    return lax.dot_general(
        left, right, (((1,), (1,)), ((), ())), precision=PRECISE, preferred_element_type=F32
    )


def null_kernel(picks_ref, angles_ref, volts_ref, out_ref):
    antennas = volts_ref.shape[1] // 2
    count = picks_ref.shape[1]
    row = lax.broadcasted_iota(jnp.int32, (count, 128), 0)
    angle = jnp.zeros((count, 128), F32)
    for k in range(count):
        angle = jnp.where(row == k, angles_ref[picks_ref[0, k]], angle)
    turn = (jnp.pi * jnp.sin(angle))[:, :1]
    position = lax.broadcasted_iota(jnp.int32, (count, antennas), 1).astype(F32)
    phase = turn * position
    norming = antennas**0.5
    re, im = jnp.cos(phase) / norming, jnp.sin(phase) / norming
    both = jnp.concatenate([re, im], axis=1)
    turned = jnp.concatenate([-im, re], axis=1)
    eye = lax.broadcasted_iota(jnp.int32, (count, count), 0) == lax.broadcasted_iota(
        jnp.int32, (count, count), 1
    )
    gram_re = across(both, both) + jnp.where(eye, STEER_LOADING, 0.0)
    gram_im = across(both, turned)
    inv_re, inv_im = complex_inverse(gram_re, gram_im)
    steer = jnp.concatenate([both, turned], axis=0)
    inverse = jnp.concatenate(
        [
            jnp.concatenate([inv_re, inv_im], axis=1),
            jnp.concatenate([-inv_im, inv_re], axis=1),
        ],
        axis=0,
    )
    back = jnp.dot(inverse, steer, precision=PRECISE, preferred_element_type=F32)
    volts = volts_ref[...]
    nt = (((1,), (1,)), ((), ()))
    inner = sum(
        lax.dot_general(volts, part, nt, preferred_element_type=F32) for part in split(steer)
    )
    out_ref[...] = volts.astype(F32) - dot3(split(inner), split(back))


def swap_cores(value, members):
    return lax.ppermute(value, "tm", [(i, i ^ 1) for i in range(members)])


def earlier_chips(value, members, decay):
    chips = members // 2
    stride, window, total = 1, value, None
    while stride < chips:
        gained = None
        for step in range(1, RADIX):
            shift = 2 * stride * step
            if shift >= members:
                break
            got = lax.ppermute(window, "tm", [(i, i + shift) for i in range(members - shift)])
            got = got if step == 1 else decay ** (stride * (step - 1)) * got
            gained = got if gained is None else gained + got
        total = gained if total is None else total + decay ** (stride - 1) * gained
        window = window + decay**stride * gained
        stride *= RADIX
    return jnp.zeros_like(value) if total is None else total


def sum_groups(value):
    groups = lax.axis_size("chan")
    if groups & (groups - 1):
        return lax.psum(value, "chan")
    step = 1
    while step < groups:
        got = lax.ppermute(value, "chan", [(i, i ^ step) for i in range(groups)])
        value = value + got
        step *= 2
    return value


def steps(volts, picks, angles):
    voltage = volts[0]
    rows, width = voltage.shape
    antennas = width // 2
    half = antennas // 2
    segments = rows // SEG
    members = lax.axis_size("tm")
    odd = lax.axis_index("tm") % 2
    parity = odd.reshape(1).astype(jnp.int32)
    is_odd = odd == 1
    decay = (1.0 - 1.0 / HORIZON) ** segments

    keep, give, power = pl.pallas_call(
        gram_kernel,
        out_shape=(
            jax.ShapeDtypeStruct((half, antennas), F32),
            jax.ShapeDtypeStruct((half, antennas), F32),
            jax.ShapeDtypeStruct((8, 128), F32),
        ),
        in_specs=[SM, VM],
        out_specs=(VM, VM, VM),
        scratch_shapes=[pltpu.VMEM((antennas, antennas), F32)],
        cost_estimate=pl.CostEstimate(
            flops=4 * rows * width * antennas, bytes_accessed=rows * width * 2, transcendentals=0
        ),
        compiler_params=PARAMS,
        name="segment_gram",
    )(parity, voltage)

    got = swap_cores(give, members)
    mine, theirs = jnp.where(is_odd, 1.0, decay), jnp.where(is_odd, decay, 1.0)
    pair = mine * keep + theirs * got
    before = earlier_chips(pair, members, decay * decay)
    even_cov = decay * before + jnp.where(is_odd, got, keep)
    odd_cov = decay * decay * before + pair
    own = jnp.where(is_odd, odd_cov, even_cov)
    other = swap_cores(jnp.where(is_odd, even_cov, odd_cov), members)

    level = sum_groups(power)
    level_before = earlier_chips(level, members, decay * decay)
    got_level = swap_cores(jnp.stack([level, level_before]), members)
    level_even = jnp.where(is_odd, got_level, jnp.stack([level, level_before]))
    level_odd = jnp.where(is_odd, jnp.stack([level, level_before]), got_level)
    level_chips = decay * level_even[1] + level_odd[1]
    level_own = decay * level_chips + level_even[0]
    level_own = jnp.where(is_odd, decay * level_own + level_odd[0], level_own)
    band = level_own / lax.axis_size("chan") + TINY_LEVEL

    projected = pl.pallas_call(
        null_kernel,
        out_shape=jax.ShapeDtypeStruct((rows, width), F32),
        in_specs=[SM, SM, VM],
        out_specs=VM,
        cost_estimate=pl.CostEstimate(
            flops=4 * rows * width * 128, bytes_accessed=rows * width * 6, transcendentals=0
        ),
        compiler_params=PARAMS,
        name="null",
    )(picks, angles, voltage)

    cleaned = pl.pallas_call(
        whiten_kernel,
        out_shape=jax.ShapeDtypeStruct((rows, width), F32),
        in_specs=[SM, VM, VM, VM, VM],
        out_specs=VM,
        scratch_shapes=[pltpu.VMEM((antennas, antennas), F32)],
        cost_estimate=pl.CostEstimate(
            flops=18 * rows * width * width, bytes_accessed=rows * width * 8, transcendentals=0
        ),
        compiler_params=PARAMS,
        name="whiten",
    )(parity, band, own, other, projected)
    return cleaned[None]


def solution(mesh):
    placed = (P("chan", "tm", None), P("chan", None), P())
    return jax.shard_map(
        steps, mesh=mesh, in_specs=placed, out_specs=P("chan", "tm", None), check_vma=False
    )
```

```python
import jax
import jax.numpy as jnp
from jax import lax
from jax.experimental import pallas as pl
from jax.experimental.pallas import tpu as pltpu
from jax.sharding import PartitionSpec as P


SEG = 256
HORIZON = 256
LOADING = 0.1
STEER_LOADING = 0.05
TINY_LEVEL = 1e-06
PRECISE = lax.Precision.HIGHEST
F32 = jnp.float32
BF16 = jnp.bfloat16
VM = pl.BlockSpec(memory_space=pltpu.VMEM)
SM = pl.BlockSpec(memory_space=pltpu.SMEM)
PARAMS = pltpu.CompilerParams(vmem_limit_bytes=24 * 2**20)


def gram_kernel(parity_ref, volts_ref, keep_ref, give_ref, power_ref, mixed_ref):
    antennas = volts_ref.shape[1] // 2
    segments = volts_ref.shape[0] // SEG
    half = antennas // 2
    forget = 1.0 - 1.0 / HORIZON
    mixed = None
    for seg in range(segments):
        a = volts_ref[seg * SEG : (seg + 1) * SEG, :antennas]
        b = volts_ref[seg * SEG : (seg + 1) * SEG, antennas:]
        left = jnp.concatenate([a, b, b, -a], axis=0)
        right = jnp.concatenate([a, b, a, b], axis=0)
        term = lax.dot_general(
            left, right, (((0,), (0,)), ((), ())), preferred_element_type=F32
        )
        mixed = term if mixed is None else forget * mixed + term
    mixed_ref[...] = mixed
    row = lax.broadcasted_iota(jnp.int32, mixed.shape, 0)
    column = lax.broadcasted_iota(jnp.int32, mixed.shape, 1)
    trace = jnp.sum(jnp.where(row == column, mixed, 0.0))
    power_ref[...] = jnp.full(power_ref.shape, trace / antennas, F32)
    parity = parity_ref[0]
    keep_ref[...] = mixed_ref[pl.ds(pl.multiple_of(parity * half, half), half), :]
    give_ref[...] = mixed_ref[pl.ds(pl.multiple_of((1 - parity) * half, half), half), :]


def split(value):
    high = value.astype(BF16)
    return high, (value - high.astype(F32)).astype(BF16)


def dot3(left, right):
    (lh, ll), (rh, rl) = left, right
    return (
        jnp.dot(lh, rh, preferred_element_type=F32)
        + jnp.dot(lh, rl, preferred_element_type=F32)
        + jnp.dot(ll, rh, preferred_element_type=F32)
    )


def beside(first, second):
    return jnp.concatenate([first, second], axis=1)


def over(first, second):
    return jnp.concatenate([first, second], axis=0)


def square_kernel(parity_ref, own_ref, other_ref, cov_ref, square_ref, stats_ref, mixed_ref):
    half, antennas = own_ref.shape
    parity = parity_ref[0]
    mixed_ref[pl.ds(pl.multiple_of(parity * half, half), half), :] = own_ref[...]
    mixed_ref[pl.ds(pl.multiple_of((1 - parity) * half, half), half), :] = other_ref[...]
    mixed = mixed_ref[...]
    row = lax.broadcasted_iota(jnp.int32, mixed.shape, 0)
    column = lax.broadcasted_iota(jnp.int32, mixed.shape, 1)
    trace = jnp.sum(jnp.where(row == column, mixed, 0.0), keepdims=True)
    unit = 1.0 / (trace / antennas + TINY_LEVEL)
    mixed = mixed * unit
    flipped = mixed.T
    re, im = 0.5 * (mixed + flipped), 0.5 * (mixed - flipped)
    cov_ref[:antennas, :], cov_ref[antennas:, :] = re, im
    (rh, rl), (ih, il) = split(re), split(im)
    full = tuple(over(beside(r, -i), beside(i, r)) for r, i in ((rh, ih), (rl, il)))
    square_ref[...] = dot3(full, (over(rh, ih), over(rl, il)))
    norm = jnp.sum(mixed * mixed, keepdims=True)
    lane = lax.broadcasted_iota(jnp.int32, stats_ref.shape, 1)
    stats_ref[...] = jnp.where(lane == 0, norm, jnp.where(lane == 1, trace * unit, unit))


def whiten_kernel(band_ref, stats_ref, cov_ref, square_ref, w_ref, out_ref):
    samples = w_ref.shape[0]
    antennas = cov_ref.shape[1]
    norm, trace, unit = stats_ref[0:1, 0:1], stats_ref[0:1, 1:2], stats_ref[0:1, 2:3]
    beta = 1.0 / (unit * band_ref[0:1, 0:1])
    total = 2.0 * (
        beta * (beta * norm + 2.0 * LOADING * trace) + LOADING * LOADING * antennas
    )
    omega = 1.0 / jnp.sqrt(total)
    slope, shift = omega * beta, omega * LOADING
    cov, square = cov_ref[...], square_ref[...]
    bend = (slope * slope) * square
    first = split(bend + (2.0 * slope * (shift - 1.0)) * cov)
    second = split((slope * (3.0 - 2.0 * shift)) * cov - bend)
    left, right = slice(0, antennas), slice(antennas, 2 * antennas)

    def turn(u, v):
        parts = zip(split(u), split(v), strict=True)
        return tuple(over(beside(p, q), beside(q, -p)) for p, q in parts)

    w_u, w_v = w_ref[:, left], w_ref[:, right]
    step = dot3(turn(w_u, w_v), first)
    keep = 2.0 + shift * (shift - 2.0)
    u, v = keep * w_u + step[:samples], keep * w_v + step[samples:]
    step = dot3(turn(u, v), second)
    keep = 2.0 - shift * (3.0 - shift)
    out_ref[:, left] = omega * (w_u + keep * u - step[:samples])
    out_ref[:, right] = omega * (w_v + keep * v - step[samples:])


def complex_inverse(re, im):
    size = re.shape[0]
    row = lax.broadcasted_iota(jnp.int32, re.shape, 0)
    column = lax.broadcasted_iota(jnp.int32, re.shape, 1)
    for j in range(size):
        here = column[:1] == j
        col_re, col_im = re[:, j : j + 1], im[:, j : j + 1]
        scale = 1.0 / re[j : j + 1, j : j + 1]
        row_re = jnp.where(here, scale, re[j : j + 1] * scale)
        row_im = jnp.where(here, 0.0, im[j : j + 1] * scale)
        rest_re, rest_im = jnp.where(column == j, 0.0, re), jnp.where(column == j, 0.0, im)
        rest_re = rest_re - (col_re * row_re - col_im * row_im)
        rest_im = rest_im - (col_re * row_im + col_im * row_re)
        re = jnp.where(row == j, row_re, rest_re)
        im = jnp.where(row == j, row_im, rest_im)
    return re, im


def across(left, right):
    return lax.dot_general(
        left, right, (((1,), (1,)), ((), ())), precision=PRECISE, preferred_element_type=F32
    )


def null_kernel(picks_ref, angles_ref, volts_ref, out_ref):
    antennas = volts_ref.shape[1] // 2
    count = picks_ref.shape[1]
    row = lax.broadcasted_iota(jnp.int32, (count, 128), 0)
    angle = jnp.zeros((count, 128), F32)
    for k in range(count):
        angle = jnp.where(row == k, angles_ref[picks_ref[0, k]], angle)
    turn = (jnp.pi * jnp.sin(angle))[:, :1]
    position = lax.broadcasted_iota(jnp.int32, (count, antennas), 1).astype(F32)
    phase = turn * position
    norming = antennas**0.5
    re, im = jnp.cos(phase) / norming, jnp.sin(phase) / norming
    both = jnp.concatenate([re, im], axis=1)
    turned = jnp.concatenate([-im, re], axis=1)
    eye = lax.broadcasted_iota(jnp.int32, (count, count), 0) == lax.broadcasted_iota(
        jnp.int32, (count, count), 1
    )
    gram_re = across(both, both) + jnp.where(eye, STEER_LOADING, 0.0)
    gram_im = across(both, turned)
    inv_re, inv_im = complex_inverse(gram_re, gram_im)
    steer = jnp.concatenate([both, turned], axis=0)
    inverse = jnp.concatenate(
        [
            jnp.concatenate([inv_re, inv_im], axis=1),
            jnp.concatenate([-inv_im, inv_re], axis=1),
        ],
        axis=0,
    )
    back = jnp.dot(inverse, steer, precision=PRECISE, preferred_element_type=F32)
    volts = volts_ref[...]
    nt = (((1,), (1,)), ((), ()))
    inner = sum(
        lax.dot_general(volts, part, nt, preferred_element_type=F32) for part in split(steer)
    )
    out_ref[...] = volts.astype(F32) - dot3(split(inner), split(back))


def exchange(value, axis, mask):
    return lax.ppermute(value, axis, [(i, i ^ mask) for i in range(lax.axis_size(axis))])


def choose(index, values):
    chosen = jnp.asarray(values[0], F32)
    for i, value in enumerate(values[1:], 1):
        chosen = jnp.where(index == i, value, chosen)
    return chosen


def earlier_chips(value, decay, mirrored):
    chips = lax.axis_size("tm") // 2
    chip = lax.axis_index("tm") // 2
    length, total, before = 1, value, None
    while length < chips:
        mask = 2 * length - 1 if mirrored else length
        got = exchange(total, "tm", 2 * mask)
        upper = (chip // length) % 2 == 1
        weight = jnp.where(upper, choose(chip % length, [decay**i for i in range(length)]), 0.0)
        before = weight * got if before is None else before + weight * got
        if 2 * length < chips:
            far = decay**length
            total = jnp.where(upper, 1.0, far) * total + jnp.where(upper, far, 1.0) * got
        length *= 2
    return jnp.zeros_like(value) if before is None else before


def sum_groups(value):
    groups = lax.axis_size("chan")
    if groups & (groups - 1):
        return lax.psum(value, "chan")
    step = 1
    while step < groups:
        got = exchange(value, "chan", step)
        value = value + got
        step *= 2
    return value


def steps(volts, picks, angles):
    voltage = volts[0]
    rows, width = voltage.shape
    antennas = width // 2
    half = antennas // 2
    segments = rows // SEG
    odd = lax.axis_index("tm") % 2
    parity = odd.reshape(1).astype(jnp.int32)
    is_odd = odd == 1
    decay = (1.0 - 1.0 / HORIZON) ** segments

    keep, give, power = pl.pallas_call(
        gram_kernel,
        out_shape=(
            jax.ShapeDtypeStruct((half, antennas), F32),
            jax.ShapeDtypeStruct((half, antennas), F32),
            jax.ShapeDtypeStruct((8, 128), F32),
        ),
        in_specs=[SM, VM],
        out_specs=(VM, VM, VM),
        scratch_shapes=[pltpu.VMEM((antennas, antennas), F32)],
        cost_estimate=pl.CostEstimate(
            flops=4 * rows * width * antennas, bytes_accessed=rows * width * 2, transcendentals=0
        ),
        compiler_params=PARAMS,
        name="segment_gram",
    )(parity, voltage)

    got = exchange(give, "tm", 1)
    mine, theirs = jnp.where(is_odd, 1.0, decay), jnp.where(is_odd, decay, 1.0)
    pair = mine * keep + theirs * got
    before = earlier_chips(pair, decay * decay, True)
    even_cov = decay * before + jnp.where(is_odd, got, keep)
    odd_cov = decay * decay * before + pair
    own = jnp.where(is_odd, odd_cov, even_cov)
    other = exchange(jnp.where(is_odd, even_cov, odd_cov), "tm", 1)

    level = sum_groups(power)
    level_before = earlier_chips(level, decay * decay, False)
    levels = jnp.concatenate([level, level_before], axis=0)
    got_levels = exchange(levels, "tm", 1)
    level_even = jnp.where(is_odd, got_levels, levels)
    level_odd = jnp.where(is_odd, levels, got_levels)
    level_own = decay * (decay * level_even[8:] + level_odd[8:]) + level_even[:8]
    level_own = jnp.where(is_odd, decay * level_own + level_odd[:8], level_own)
    band = level_own / lax.axis_size("chan") + TINY_LEVEL

    projected = pl.pallas_call(
        null_kernel,
        out_shape=jax.ShapeDtypeStruct((rows, width), F32),
        in_specs=[SM, SM, VM],
        out_specs=VM,
        cost_estimate=pl.CostEstimate(
            flops=4 * rows * width * 128, bytes_accessed=rows * width * 6, transcendentals=0
        ),
        compiler_params=PARAMS,
        name="null",
    )(picks, angles, voltage)

    cov, square, stats = pl.pallas_call(
        square_kernel,
        out_shape=(
            jax.ShapeDtypeStruct((width, antennas), F32),
            jax.ShapeDtypeStruct((width, antennas), F32),
            jax.ShapeDtypeStruct((8, 128), F32),
        ),
        in_specs=[SM, VM, VM],
        out_specs=(VM, VM, VM),
        scratch_shapes=[pltpu.VMEM((antennas, antennas), F32)],
        cost_estimate=pl.CostEstimate(
            flops=6 * width * width * antennas, bytes_accessed=width * antennas * 8, transcendentals=0
        ),
        compiler_params=PARAMS,
        name="square",
    )(parity, own, other)

    cleaned = pl.pallas_call(
        whiten_kernel,
        out_shape=jax.ShapeDtypeStruct((rows, width), F32),
        in_specs=[VM] * 5,
        out_specs=VM,
        cost_estimate=pl.CostEstimate(
            flops=12 * rows * width * width, bytes_accessed=rows * width * 8, transcendentals=0
        ),
        compiler_params=PARAMS,
        name="whiten",
    )(band, stats, cov, square, projected)
    return cleaned[None]


def solution(mesh):
    placed = (P("chan", "tm", None), P("chan", None), P())
    return jax.shard_map(
        steps, mesh=mesh, in_specs=placed, out_specs=P("chan", "tm", None), check_vma=False
    )
```

```python
import jax
import jax.numpy as jnp
from jax import lax
from jax.experimental import pallas as pl
from jax.experimental.pallas import tpu as pltpu
from jax.sharding import PartitionSpec as P


SEG = 256
HORIZON = 256
DIRECT = 4
LOADING = 0.1
STEER_LOADING = 0.05
TINY_LEVEL = 1e-06
PRECISE = lax.Precision.HIGHEST
F32 = jnp.float32
BF16 = jnp.bfloat16
VM = pl.BlockSpec(memory_space=pltpu.VMEM)
SM = pl.BlockSpec(memory_space=pltpu.SMEM)
PARAMS = pltpu.CompilerParams(vmem_limit_bytes=24 * 2**20)


def gram_kernel(parity_ref, volts_ref, keep_ref, give_ref, power_ref, mixed_ref):
    antennas = volts_ref.shape[1] // 2
    segments = volts_ref.shape[0] // SEG
    half = antennas // 2
    forget = 1.0 - 1.0 / HORIZON
    mixed = None
    for seg in range(segments):
        a = volts_ref[seg * SEG : (seg + 1) * SEG, :antennas]
        b = volts_ref[seg * SEG : (seg + 1) * SEG, antennas:]
        left = jnp.concatenate([a, b, b, -a], axis=0)
        right = jnp.concatenate([a, b, a, b], axis=0)
        term = lax.dot_general(
            left, right, (((0,), (0,)), ((), ())), preferred_element_type=F32
        )
        mixed = term if mixed is None else forget * mixed + term
    mixed_ref[...] = mixed
    row = lax.broadcasted_iota(jnp.int32, mixed.shape, 0)
    column = lax.broadcasted_iota(jnp.int32, mixed.shape, 1)
    trace = jnp.sum(jnp.where(row == column, mixed, 0.0))
    power_ref[...] = jnp.full(power_ref.shape, trace / antennas, F32)
    parity = parity_ref[0]
    keep_ref[...] = mixed_ref[pl.ds(pl.multiple_of(parity * half, half), half), :]
    give_ref[...] = mixed_ref[pl.ds(pl.multiple_of((1 - parity) * half, half), half), :]


def split(value):
    high = value.astype(BF16)
    return high, (value - high.astype(F32)).astype(BF16)


def dot3(left, right):
    (lh, ll), (rh, rl) = left, right
    return (
        jnp.dot(lh, rh, preferred_element_type=F32)
        + jnp.dot(lh, rl, preferred_element_type=F32)
        + jnp.dot(ll, rh, preferred_element_type=F32)
    )


def beside(first, second):
    return jnp.concatenate([first, second], axis=1)


def over(first, second):
    return jnp.concatenate([first, second], axis=0)


def square_kernel(parity_ref, own_ref, other_ref, cov_ref, square_ref, stats_ref, mixed_ref):
    half, antennas = own_ref.shape
    parity = parity_ref[0]
    mixed_ref[pl.ds(pl.multiple_of(parity * half, half), half), :] = own_ref[...]
    mixed_ref[pl.ds(pl.multiple_of((1 - parity) * half, half), half), :] = other_ref[...]
    mixed = mixed_ref[...]
    row = lax.broadcasted_iota(jnp.int32, mixed.shape, 0)
    column = lax.broadcasted_iota(jnp.int32, mixed.shape, 1)
    trace = jnp.sum(jnp.where(row == column, mixed, 0.0), keepdims=True)
    unit = 1.0 / (trace / antennas + TINY_LEVEL)
    mixed = mixed * unit
    flipped = mixed.T
    re, im = 0.5 * (mixed + flipped), 0.5 * (mixed - flipped)
    cov_ref[:antennas, :], cov_ref[antennas:, :] = re, im
    (rh, rl), (ih, il) = split(re), split(im)
    full = tuple(over(beside(r, -i), beside(i, r)) for r, i in ((rh, ih), (rl, il)))
    square_ref[...] = dot3(full, (over(rh, ih), over(rl, il)))
    norm = jnp.sum(mixed * mixed, keepdims=True)
    lane = lax.broadcasted_iota(jnp.int32, stats_ref.shape, 1)
    stats_ref[...] = jnp.where(lane == 0, norm, jnp.where(lane == 1, trace * unit, unit))


def whiten_kernel(band_ref, stats_ref, cov_ref, square_ref, w_ref, out_ref):
    samples = w_ref.shape[0]
    antennas = cov_ref.shape[1]
    norm, trace, unit = stats_ref[0:1, 0:1], stats_ref[0:1, 1:2], stats_ref[0:1, 2:3]
    beta = 1.0 / (unit * band_ref[0:1, 0:1])
    total = 2.0 * (
        beta * (beta * norm + 2.0 * LOADING * trace) + LOADING * LOADING * antennas
    )
    omega = 1.0 / jnp.sqrt(total)
    slope, shift = omega * beta, omega * LOADING
    cov, square = cov_ref[...], square_ref[...]
    bend = (slope * slope) * square
    first = split(bend + (2.0 * slope * (shift - 1.0)) * cov)
    second = split((slope * (3.0 - 2.0 * shift)) * cov - bend)
    left, right = slice(0, antennas), slice(antennas, 2 * antennas)

    def turn(u, v):
        parts = zip(split(u), split(v), strict=True)
        return tuple(over(beside(p, q), beside(q, -p)) for p, q in parts)

    w_u, w_v = w_ref[:, left], w_ref[:, right]
    step = dot3(turn(w_u, w_v), first)
    keep = 2.0 + shift * (shift - 2.0)
    u, v = keep * w_u + step[:samples], keep * w_v + step[samples:]
    step = dot3(turn(u, v), second)
    keep = 2.0 - shift * (3.0 - shift)
    out_ref[:, left] = omega * (w_u + keep * u - step[:samples])
    out_ref[:, right] = omega * (w_v + keep * v - step[samples:])


def complex_inverse(re, im):
    size = re.shape[0]
    row = lax.broadcasted_iota(jnp.int32, re.shape, 0)
    column = lax.broadcasted_iota(jnp.int32, re.shape, 1)
    for j in range(size):
        here = column[:1] == j
        col_re, col_im = re[:, j : j + 1], im[:, j : j + 1]
        scale = 1.0 / re[j : j + 1, j : j + 1]
        row_re = jnp.where(here, scale, re[j : j + 1] * scale)
        row_im = jnp.where(here, 0.0, im[j : j + 1] * scale)
        rest_re, rest_im = jnp.where(column == j, 0.0, re), jnp.where(column == j, 0.0, im)
        rest_re = rest_re - (col_re * row_re - col_im * row_im)
        rest_im = rest_im - (col_re * row_im + col_im * row_re)
        re = jnp.where(row == j, row_re, rest_re)
        im = jnp.where(row == j, row_im, rest_im)
    return re, im


def across(left, right):
    return lax.dot_general(
        left, right, (((1,), (1,)), ((), ())), precision=PRECISE, preferred_element_type=F32
    )


def null_kernel(picks_ref, angles_ref, volts_ref, out_ref):
    antennas = volts_ref.shape[1] // 2
    count = picks_ref.shape[1]
    row = lax.broadcasted_iota(jnp.int32, (count, 128), 0)
    angle = jnp.zeros((count, 128), F32)
    for k in range(count):
        angle = jnp.where(row == k, angles_ref[picks_ref[0, k]], angle)
    turn = (jnp.pi * jnp.sin(angle))[:, :1]
    position = lax.broadcasted_iota(jnp.int32, (count, antennas), 1).astype(F32)
    phase = turn * position
    norming = antennas**0.5
    re, im = jnp.cos(phase) / norming, jnp.sin(phase) / norming
    both = jnp.concatenate([re, im], axis=1)
    turned = jnp.concatenate([-im, re], axis=1)
    eye = lax.broadcasted_iota(jnp.int32, (count, count), 0) == lax.broadcasted_iota(
        jnp.int32, (count, count), 1
    )
    gram_re = across(both, both) + jnp.where(eye, STEER_LOADING, 0.0)
    gram_im = across(both, turned)
    inv_re, inv_im = complex_inverse(gram_re, gram_im)
    steer = jnp.concatenate([both, turned], axis=0)
    inverse = jnp.concatenate(
        [
            jnp.concatenate([inv_re, inv_im], axis=1),
            jnp.concatenate([-inv_im, inv_re], axis=1),
        ],
        axis=0,
    )
    back = jnp.dot(inverse, steer, precision=PRECISE, preferred_element_type=F32)
    volts = volts_ref[...]
    nt = (((1,), (1,)), ((), ()))
    inner = sum(
        lax.dot_general(volts, part, nt, preferred_element_type=F32) for part in split(steer)
    )
    out_ref[...] = volts.astype(F32) - dot3(split(inner), split(back))


def exchange(value, axis, mask):
    return lax.ppermute(value, axis, [(i, i ^ mask) for i in range(lax.axis_size(axis))])


def choose(index, values):
    chosen = jnp.asarray(values[0], F32)
    for i, value in enumerate(values[1:], 1):
        chosen = jnp.where(index == i, value, chosen)
    return chosen


def earlier_chips(value, decay, mirrored=False, rider=None):
    chips = lax.axis_size("tm") // 2
    chip = lax.axis_index("tm") // 2
    length, total, before = 1, value, None
    while length < chips:
        last = 2 * length == chips
        mask = 2 * length - 1 if mirrored else length
        rows = total.shape[0]
        if last and rider is not None:
            total = jnp.concatenate([total, rider], axis=0)
        got = exchange(total, "tm", 2 * mask)
        if last and rider is not None:
            got, rider = got[:rows], got[rows:]
        upper = (chip // length) % 2 == 1
        weight = jnp.where(upper, choose(chip % length, [decay**i for i in range(length)]), 0.0)
        before = weight * got if before is None else before + weight * got
        if not last:
            far = decay**length
            total = jnp.where(upper, 1.0, far) * total + jnp.where(upper, far, 1.0) * got
        length *= 2
    before = jnp.zeros_like(value) if before is None else before
    return before if rider is None else (before, rider)


def earlier_levels(level, opposite, decay):
    chips = lax.axis_size("tm") // 2
    chip = lax.axis_index("tm") // 2
    before = 0.0
    for mask in range(1, chips):
        if mask == chips - 1:
            got = opposite
        else:
            got = exchange(level, "tm", 2 * mask)
        weights = [decay ** (c - 1 - (c ^ mask)) if c ^ mask < c else 0.0 for c in range(chips)]
        before = before + choose(chip, weights) * got
    return before


def sum_groups(value):
    groups = lax.axis_size("chan")
    if groups & (groups - 1):
        return lax.psum(value, "chan")
    step = 1
    while step < groups:
        got = exchange(value, "chan", step)
        value = value + got
        step *= 2
    return value


def steps(volts, picks, angles):
    voltage = volts[0]
    rows, width = voltage.shape
    antennas = width // 2
    half = antennas // 2
    segments = rows // SEG
    odd = lax.axis_index("tm") % 2
    parity = odd.reshape(1).astype(jnp.int32)
    is_odd = odd == 1
    decay = (1.0 - 1.0 / HORIZON) ** segments

    keep, give, power = pl.pallas_call(
        gram_kernel,
        out_shape=(
            jax.ShapeDtypeStruct((half, antennas), F32),
            jax.ShapeDtypeStruct((half, antennas), F32),
            jax.ShapeDtypeStruct((8, 128), F32),
        ),
        in_specs=[SM, VM],
        out_specs=(VM, VM, VM),
        scratch_shapes=[pltpu.VMEM((antennas, antennas), F32)],
        cost_estimate=pl.CostEstimate(
            flops=4 * rows * width * antennas, bytes_accessed=rows * width * 2, transcendentals=0
        ),
        compiler_params=PARAMS,
        name="segment_gram",
    )(parity, voltage)

    got = exchange(give, "tm", 1)
    mine, theirs = jnp.where(is_odd, 1.0, decay), jnp.where(is_odd, decay, 1.0)
    pair = mine * keep + theirs * got
    level = sum_groups(power)
    direct = lax.axis_size("tm") // 2 == DIRECT
    if direct:
        wide = jnp.concatenate([level] * (antennas // level.shape[1]), axis=1)
        before, opposite = earlier_chips(pair, decay * decay, True, wide)
        level_before = earlier_levels(level, opposite[:, : level.shape[1]], decay * decay)
    else:
        before = earlier_chips(pair, decay * decay, True)
        level_before = earlier_chips(level, decay * decay)
    even_cov = decay * before + jnp.where(is_odd, got, keep)
    odd_cov = decay * decay * before + pair
    own = jnp.where(is_odd, odd_cov, even_cov)
    other = exchange(jnp.where(is_odd, even_cov, odd_cov), "tm", 1)

    levels = jnp.concatenate([level, level_before], axis=0)
    got_levels = exchange(levels, "tm", 1)
    level_even = jnp.where(is_odd, got_levels, levels)
    level_odd = jnp.where(is_odd, levels, got_levels)
    level_own = decay * (decay * level_even[8:] + level_odd[8:]) + level_even[:8]
    level_own = jnp.where(is_odd, decay * level_own + level_odd[:8], level_own)
    band = level_own / lax.axis_size("chan") + TINY_LEVEL

    projected = pl.pallas_call(
        null_kernel,
        out_shape=jax.ShapeDtypeStruct((rows, width), F32),
        in_specs=[SM, SM, VM],
        out_specs=VM,
        cost_estimate=pl.CostEstimate(
            flops=4 * rows * width * 128, bytes_accessed=rows * width * 6, transcendentals=0
        ),
        compiler_params=PARAMS,
        name="null",
    )(picks, angles, voltage)

    cov, square, stats = pl.pallas_call(
        square_kernel,
        out_shape=(
            jax.ShapeDtypeStruct((width, antennas), F32),
            jax.ShapeDtypeStruct((width, antennas), F32),
            jax.ShapeDtypeStruct((8, 128), F32),
        ),
        in_specs=[SM, VM, VM],
        out_specs=(VM, VM, VM),
        scratch_shapes=[pltpu.VMEM((antennas, antennas), F32)],
        cost_estimate=pl.CostEstimate(
            flops=6 * width * width * antennas, bytes_accessed=width * antennas * 8, transcendentals=0
        ),
        compiler_params=PARAMS,
        name="square",
    )(parity, own, other)

    cleaned = pl.pallas_call(
        whiten_kernel,
        out_shape=jax.ShapeDtypeStruct((rows, width), F32),
        in_specs=[VM] * 5,
        out_specs=VM,
        cost_estimate=pl.CostEstimate(
            flops=12 * rows * width * width, bytes_accessed=rows * width * 8, transcendentals=0
        ),
        compiler_params=PARAMS,
        name="whiten",
    )(band, stats, cov, square, projected)
    return cleaned[None]


def solution(mesh):
    placed = (P("chan", "tm", None), P("chan", None), P())
    return jax.shard_map(
        steps, mesh=mesh, in_specs=placed, out_specs=P("chan", "tm", None), check_vma=False
    )
```

```python
import jax
import jax.numpy as jnp
from jax import lax
from jax.experimental import pallas as pl
from jax.experimental.pallas import tpu as pltpu
from jax.sharding import PartitionSpec as P


SEG = 256
HORIZON = 256
CHUNKS = 4
DIRECT = 4
LOADING = 0.1
STEER_LOADING = 0.05
TINY_LEVEL = 1e-06
PRECISE = lax.Precision.HIGHEST
F32 = jnp.float32
BF16 = jnp.bfloat16
VM = pl.BlockSpec(memory_space=pltpu.VMEM)
SM = pl.BlockSpec(memory_space=pltpu.SMEM)
PARAMS = pltpu.CompilerParams(vmem_limit_bytes=24 * 2**20)


def gram_kernel(parity_ref, volts_ref, keep_ref, give_ref, power_ref, mixed_ref):
    antennas = volts_ref.shape[1] // 2
    segments = volts_ref.shape[0] // SEG
    half = antennas // 2
    forget = 1.0 - 1.0 / HORIZON
    mixed = None
    for seg in range(segments):
        a = volts_ref[seg * SEG : (seg + 1) * SEG, :antennas]
        b = volts_ref[seg * SEG : (seg + 1) * SEG, antennas:]
        left = jnp.concatenate([a, b, b, -a], axis=0)
        right = jnp.concatenate([a, b, a, b], axis=0)
        term = lax.dot_general(
            left, right, (((0,), (0,)), ((), ())), preferred_element_type=F32
        )
        mixed = term if mixed is None else forget * mixed + term
    mixed_ref[...] = mixed
    row = lax.broadcasted_iota(jnp.int32, mixed.shape, 0)
    column = lax.broadcasted_iota(jnp.int32, mixed.shape, 1)
    trace = jnp.sum(jnp.where(row == column, mixed, 0.0))
    power_ref[...] = jnp.full(power_ref.shape, trace / antennas, F32)
    parity = parity_ref[0]
    keep_ref[...] = mixed_ref[pl.ds(pl.multiple_of(parity * half, half), half), :]
    give_ref[...] = mixed_ref[pl.ds(pl.multiple_of((1 - parity) * half, half), half), :]


def split(value):
    high = value.astype(BF16)
    return high, (value - high.astype(F32)).astype(BF16)


def dot3(left, right):
    (lh, ll), (rh, rl) = left, right
    return (
        jnp.dot(lh, rh, preferred_element_type=F32)
        + jnp.dot(lh, rl, preferred_element_type=F32)
        + jnp.dot(ll, rh, preferred_element_type=F32)
    )


def beside(first, second):
    return jnp.concatenate([first, second], axis=1)


def over(first, second):
    return jnp.concatenate([first, second], axis=0)


def turn(u, v):
    parts = zip(split(u), split(v), strict=True)
    return tuple(over(beside(p, q), beside(q, -p)) for p, q in parts)


def square_kernel(parity_ref, own_ref, other_ref, cov_ref, square_ref, stats_ref, mixed_ref):
    half, antennas = own_ref.shape
    parity = parity_ref[0]
    mixed_ref[pl.ds(pl.multiple_of(parity * half, half), half), :] = own_ref[...]
    mixed_ref[pl.ds(pl.multiple_of((1 - parity) * half, half), half), :] = other_ref[...]
    mixed = mixed_ref[...]
    flipped = mixed.T
    re, im = 0.5 * (mixed + flipped), 0.5 * (mixed - flipped)
    cov_ref[:antennas, :], cov_ref[antennas:, :] = re, im
    (rh, rl), (ih, il) = split(re), split(im)
    full = tuple(over(beside(r, -i), beside(i, r)) for r, i in ((rh, ih), (rl, il)))
    square_ref[...] = dot3(full, (over(rh, ih), over(rl, il)))
    row = lax.broadcasted_iota(jnp.int32, mixed.shape, 0)
    column = lax.broadcasted_iota(jnp.int32, mixed.shape, 1)
    trace = jnp.sum(jnp.where(row == column, mixed, 0.0), keepdims=True)
    norm = jnp.sum(mixed * mixed, keepdims=True)
    stats_ref[:8, :] = jnp.broadcast_to(norm, (8, stats_ref.shape[1]))
    stats_ref[8:, :] = jnp.broadcast_to(trace, (8, stats_ref.shape[1]))


def whiten_kernel(
    band_ref, stats_ref, cov_ref, square_ref, w_ref, high_ref, low_ref, out_ref, done_ref, sems
):
    samples = w_ref.shape[0]
    antennas = cov_ref.shape[1]
    size = samples // CHUNKS

    def wide(row):
        return jnp.concatenate([row] * (antennas // row.shape[1]), axis=1)

    norm, trace, band = wide(stats_ref[0:1, :]), wide(stats_ref[8:9, :]), wide(band_ref[0:1, :])
    beta = 1.0 / band
    total = 2.0 * (beta * (beta * norm + 2.0 * LOADING * trace) + LOADING * LOADING * antennas)
    omega = 1.0 / jnp.sqrt(total)
    slope, shift = omega * beta, omega * LOADING
    cov, square = cov_ref[...], square_ref[...]
    bend = (slope * slope) * square
    first = split(bend + (2.0 * slope * (shift - 1.0)) * cov)
    second = split((slope * (3.0 - 2.0 * shift)) * cov - bend)
    left, right = slice(0, antennas), slice(antennas, 2 * antennas)
    keep_first, keep_second = 2.0 + shift * (shift - 2.0), 2.0 - shift * (3.0 - shift)
    for n in range(CHUNKS):
        rows, both = slice(n * size, (n + 1) * size), slice(2 * n * size, 2 * (n + 1) * size)
        w_u, w_v = w_ref[rows, left], w_ref[rows, right]
        step = dot3((high_ref[both, :], low_ref[both, :]), first)
        u, v = keep_first * w_u + step[:size], keep_first * w_v + step[size:]
        step = dot3(turn(u, v), second)
        done_ref[rows, left] = omega * (w_u + keep_second * u - step[:size])
        done_ref[rows, right] = omega * (w_v + keep_second * v - step[size:])
        pltpu.make_async_copy(done_ref.at[rows], out_ref.at[rows], sems.at[n]).start()
    for n in range(CHUNKS):
        rows = slice(n * size, (n + 1) * size)
        pltpu.make_async_copy(done_ref.at[rows], out_ref.at[rows], sems.at[n]).wait()


def complex_inverse(re, im):
    size = re.shape[0]
    row = lax.broadcasted_iota(jnp.int32, re.shape, 0)
    column = lax.broadcasted_iota(jnp.int32, re.shape, 1)
    for j in range(size):
        here = column[:1] == j
        col_re, col_im = re[:, j : j + 1], im[:, j : j + 1]
        scale = 1.0 / re[j : j + 1, j : j + 1]
        row_re = jnp.where(here, scale, re[j : j + 1] * scale)
        row_im = jnp.where(here, 0.0, im[j : j + 1] * scale)
        rest_re, rest_im = jnp.where(column == j, 0.0, re), jnp.where(column == j, 0.0, im)
        rest_re = rest_re - (col_re * row_re - col_im * row_im)
        rest_im = rest_im - (col_re * row_im + col_im * row_re)
        re = jnp.where(row == j, row_re, rest_re)
        im = jnp.where(row == j, row_im, rest_im)
    return re, im


def across(left, right):
    return lax.dot_general(
        left, right, (((1,), (1,)), ((), ())), precision=PRECISE, preferred_element_type=F32
    )


def null_kernel(picks_ref, angles_ref, volts_ref, out_ref, high_ref, low_ref):
    antennas = volts_ref.shape[1] // 2
    count = picks_ref.shape[1]
    row = lax.broadcasted_iota(jnp.int32, (count, 128), 0)
    angle = jnp.zeros((count, 128), F32)
    for k in range(count):
        angle = jnp.where(row == k, angles_ref[picks_ref[0, k]], angle)
    rate = (jnp.pi * jnp.sin(angle))[:, :1]
    position = lax.broadcasted_iota(jnp.int32, (count, antennas), 1).astype(F32)
    phase = rate * position
    norming = antennas**0.5
    re, im = jnp.cos(phase) / norming, jnp.sin(phase) / norming
    both = jnp.concatenate([re, im], axis=1)
    turned = jnp.concatenate([-im, re], axis=1)
    eye = lax.broadcasted_iota(jnp.int32, (count, count), 0) == lax.broadcasted_iota(
        jnp.int32, (count, count), 1
    )
    gram_re = across(both, both) + jnp.where(eye, STEER_LOADING, 0.0)
    gram_im = across(both, turned)
    inv_re, inv_im = complex_inverse(gram_re, gram_im)
    steer = jnp.concatenate([both, turned], axis=0)
    inverse = jnp.concatenate(
        [
            jnp.concatenate([inv_re, inv_im], axis=1),
            jnp.concatenate([-inv_im, inv_re], axis=1),
        ],
        axis=0,
    )
    back = jnp.dot(inverse, steer, precision=PRECISE, preferred_element_type=F32)
    volts = volts_ref[...]
    nt = (((1,), (1,)), ((), ()))
    inner = sum(
        lax.dot_general(volts, part, nt, preferred_element_type=F32) for part in split(steer)
    )
    nulled = volts.astype(F32) - dot3(split(inner), split(back))
    out_ref[...] = nulled
    size = volts.shape[0] // CHUNKS
    for n in range(CHUNKS):
        rows, both = slice(n * size, (n + 1) * size), slice(2 * n * size, 2 * (n + 1) * size)
        high, low = turn(nulled[rows, :antennas], nulled[rows, antennas:])
        high_ref[both, :], low_ref[both, :] = high, low


def exchange(value, axis, mask):
    return lax.ppermute(value, axis, [(i, i ^ mask) for i in range(lax.axis_size(axis))])


def choose(index, values):
    chosen = jnp.asarray(values[0], F32)
    for i, value in enumerate(values[1:], 1):
        chosen = jnp.where(index == i, value, chosen)
    return chosen


def earlier_chips(value, decay, mirrored=False, rider=None):
    chips = lax.axis_size("tm") // 2
    chip = lax.axis_index("tm") // 2
    length, total, before = 1, value, None
    while length < chips:
        last = 2 * length == chips
        mask = 2 * length - 1 if mirrored else length
        rows = total.shape[0]
        if last and rider is not None:
            total = jnp.concatenate([total, rider], axis=0)
        got = exchange(total, "tm", 2 * mask)
        if last and rider is not None:
            got, rider = got[:rows], got[rows:]
        upper = (chip // length) % 2 == 1
        weight = jnp.where(upper, choose(chip % length, [decay**i for i in range(length)]), 0.0)
        before = weight * got if before is None else before + weight * got
        if not last:
            far = decay**length
            total = jnp.where(upper, 1.0, far) * total + jnp.where(upper, far, 1.0) * got
        length *= 2
    before = jnp.zeros_like(value) if before is None else before
    return before if rider is None else (before, rider)


def earlier_levels(level, opposite, decay):
    chips = lax.axis_size("tm") // 2
    chip = lax.axis_index("tm") // 2
    before = 0.0
    for mask in range(1, chips):
        if mask == chips - 1:
            got = opposite
        else:
            got = exchange(level, "tm", 2 * mask)
        weights = [decay ** (c - 1 - (c ^ mask)) if c ^ mask < c else 0.0 for c in range(chips)]
        before = before + choose(chip, weights) * got
    return before


def sum_groups(value):
    groups = lax.axis_size("chan")
    if groups & (groups - 1):
        return lax.psum(value, "chan")
    step = 1
    while step < groups:
        got = exchange(value, "chan", step)
        value = value + got
        step *= 2
    return value


def steps(volts, picks, angles):
    voltage = volts[0]
    rows, width = voltage.shape
    antennas = width // 2
    half = antennas // 2
    segments = rows // SEG
    odd = lax.axis_index("tm") % 2
    parity = odd.reshape(1).astype(jnp.int32)
    is_odd = odd == 1
    decay = (1.0 - 1.0 / HORIZON) ** segments

    keep, give, power = pl.pallas_call(
        gram_kernel,
        out_shape=(
            jax.ShapeDtypeStruct((half, antennas), F32),
            jax.ShapeDtypeStruct((half, antennas), F32),
            jax.ShapeDtypeStruct((8, 128), F32),
        ),
        in_specs=[SM, VM],
        out_specs=(VM, VM, VM),
        scratch_shapes=[pltpu.VMEM((antennas, antennas), F32)],
        cost_estimate=pl.CostEstimate(
            flops=4 * rows * width * antennas, bytes_accessed=rows * width * 2, transcendentals=0
        ),
        compiler_params=PARAMS,
        name="segment_gram",
    )(parity, voltage)

    got = exchange(give, "tm", 1)
    mine, theirs = jnp.where(is_odd, 1.0, decay), jnp.where(is_odd, decay, 1.0)
    pair = mine * keep + theirs * got
    level = sum_groups(power)
    direct = lax.axis_size("tm") // 2 == DIRECT
    if direct:
        wide = jnp.concatenate([level] * (antennas // level.shape[1]), axis=1)
        before, opposite = earlier_chips(pair, decay * decay, True, wide)
        level_before = earlier_levels(level, opposite[:, : level.shape[1]], decay * decay)
    else:
        before = earlier_chips(pair, decay * decay, True)
        level_before = earlier_chips(level, decay * decay)
    even_cov = decay * before + jnp.where(is_odd, got, keep)
    odd_cov = decay * decay * before + pair
    own = jnp.where(is_odd, odd_cov, even_cov)
    other = exchange(jnp.where(is_odd, even_cov, odd_cov), "tm", 1)

    levels = jnp.concatenate([level, level_before], axis=0)
    got_levels = exchange(levels, "tm", 1)
    level_even = jnp.where(is_odd, got_levels, levels)
    level_odd = jnp.where(is_odd, levels, got_levels)
    level_own = decay * (decay * level_even[8:] + level_odd[8:]) + level_even[:8]
    level_own = jnp.where(is_odd, decay * level_own + level_odd[:8], level_own)
    band = level_own / lax.axis_size("chan") + TINY_LEVEL

    projected, high, low = pl.pallas_call(
        null_kernel,
        out_shape=(
            jax.ShapeDtypeStruct((rows, width), F32),
            jax.ShapeDtypeStruct((2 * rows, width), BF16),
            jax.ShapeDtypeStruct((2 * rows, width), BF16),
        ),
        in_specs=[SM, SM, VM],
        out_specs=(VM, VM, VM),
        cost_estimate=pl.CostEstimate(
            flops=4 * rows * width * 128, bytes_accessed=rows * width * 6, transcendentals=0
        ),
        compiler_params=PARAMS,
        name="null",
    )(picks, angles, voltage)

    cov, square, stats = pl.pallas_call(
        square_kernel,
        out_shape=(
            jax.ShapeDtypeStruct((width, antennas), F32),
            jax.ShapeDtypeStruct((width, antennas), F32),
            jax.ShapeDtypeStruct((16, 128), F32),
        ),
        in_specs=[SM, VM, VM],
        out_specs=(VM, VM, VM),
        scratch_shapes=[pltpu.VMEM((antennas, antennas), F32)],
        cost_estimate=pl.CostEstimate(
            flops=6 * width * width * antennas, bytes_accessed=width * antennas * 8, transcendentals=0
        ),
        compiler_params=PARAMS,
        name="square",
    )(parity, own, other)

    cleaned = pl.pallas_call(
        whiten_kernel,
        out_shape=jax.ShapeDtypeStruct((rows, width), F32),
        in_specs=[VM] * 7,
        out_specs=pl.BlockSpec(memory_space=pl.ANY),
        scratch_shapes=[pltpu.VMEM((rows, width), F32), pltpu.SemaphoreType.DMA((CHUNKS,))],
        cost_estimate=pl.CostEstimate(
            flops=12 * rows * width * width, bytes_accessed=rows * width * 8, transcendentals=0
        ),
        compiler_params=PARAMS,
        name="whiten",
    )(band, stats, cov, square, projected, high, low)
    return cleaned[None]


def solution(mesh):
    placed = (P("chan", "tm", None), P("chan", None), P())
    return jax.shard_map(
        steps, mesh=mesh, in_specs=placed, out_specs=P("chan", "tm", None), check_vma=False
    )
```

```python
import jax
import jax.numpy as jnp
from jax import lax
from jax.experimental import pallas as pl
from jax.experimental.pallas import tpu as pltpu
from jax.sharding import PartitionSpec as P


SEG = 256
HORIZON = 256
PIECES = 2
CHUNKS = 4
DIRECT = 4
LOADING = 0.1
STEER_LOADING = 0.05
TINY_LEVEL = 1e-06
PRECISE = lax.Precision.HIGHEST
F32 = jnp.float32
BF16 = jnp.bfloat16
VM = pl.BlockSpec(memory_space=pltpu.VMEM)
SM = pl.BlockSpec(memory_space=pltpu.SMEM)
PARAMS = pltpu.CompilerParams(vmem_limit_bytes=24 * 2**20)


def gram_kernel(parity_ref, volts_ref, keep_ref, give_ref, power_ref, mixed_ref):
    antennas = volts_ref.shape[1] // 2
    segments = volts_ref.shape[0] // SEG
    half = antennas // 2
    forget = 1.0 - 1.0 / HORIZON
    mixed = None
    for seg in range(segments):
        a = volts_ref[seg * SEG : (seg + 1) * SEG, :antennas]
        b = volts_ref[seg * SEG : (seg + 1) * SEG, antennas:]
        left = jnp.concatenate([a, b, b, -a], axis=0)
        right = jnp.concatenate([a, b, a, b], axis=0)
        term = lax.dot_general(
            left, right, (((0,), (0,)), ((), ())), preferred_element_type=F32
        )
        mixed = term if mixed is None else forget * mixed + term
    mixed_ref[...] = mixed
    row = lax.broadcasted_iota(jnp.int32, mixed.shape, 0)
    column = lax.broadcasted_iota(jnp.int32, mixed.shape, 1)
    trace = jnp.sum(jnp.where(row == column, mixed, 0.0))
    power_ref[...] = jnp.full(power_ref.shape, trace / antennas, F32)
    parity = parity_ref[0]
    keep_ref[...] = mixed_ref[pl.ds(pl.multiple_of(parity * half, half), half), :]
    give_ref[...] = mixed_ref[pl.ds(pl.multiple_of((1 - parity) * half, half), half), :]


def split(value):
    high = value.astype(BF16)
    return high, (value - high.astype(F32)).astype(BF16)


def dot3(left, right):
    (lh, ll), (rh, rl) = left, right
    return (
        jnp.dot(lh, rh, preferred_element_type=F32)
        + jnp.dot(lh, rl, preferred_element_type=F32)
        + jnp.dot(ll, rh, preferred_element_type=F32)
    )


def beside(first, second):
    return jnp.concatenate([first, second], axis=1)


def over(first, second):
    return jnp.concatenate([first, second], axis=0)


def turn(u, v):
    parts = zip(split(u), split(v), strict=True)
    return tuple(over(beside(p, q), beside(q, -p)) for p, q in parts)


def square_kernel(parity_ref, *refs):
    pieces, (cov_ref, square_ref, stats_ref, mixed_ref) = refs[:-4], refs[-4:]
    size, antennas = pieces[0].shape
    half = antennas // 2
    parity = parity_ref[0]
    for k, (own_ref, other_ref) in enumerate(zip(pieces[:PIECES], pieces[PIECES:], strict=True)):
        mixed_ref[pl.ds(pl.multiple_of(parity * half + k * size, size), size), :] = own_ref[...]
        mixed_ref[pl.ds(pl.multiple_of((1 - parity) * half + k * size, size), size), :] = other_ref[...]
    mixed = mixed_ref[...]
    flipped = mixed.T
    re, im = 0.5 * (mixed + flipped), 0.5 * (mixed - flipped)
    cov_ref[:antennas, :], cov_ref[antennas:, :] = re, im
    (rh, rl), (ih, il) = split(re), split(im)
    full = tuple(over(beside(r, -i), beside(i, r)) for r, i in ((rh, ih), (rl, il)))
    square_ref[...] = dot3(full, (over(rh, ih), over(rl, il)))
    row = lax.broadcasted_iota(jnp.int32, mixed.shape, 0)
    column = lax.broadcasted_iota(jnp.int32, mixed.shape, 1)
    trace = jnp.sum(jnp.where(row == column, mixed, 0.0), keepdims=True)
    norm = jnp.sum(mixed * mixed, keepdims=True)
    stats_ref[:8, :] = jnp.broadcast_to(norm, (8, stats_ref.shape[1]))
    stats_ref[8:, :] = jnp.broadcast_to(trace, (8, stats_ref.shape[1]))


def whiten_kernel(
    band_ref, stats_ref, cov_ref, square_ref, w_ref, high_ref, low_ref, out_ref, done_ref, sems
):
    samples = w_ref.shape[0]
    antennas = cov_ref.shape[1]
    size = samples // CHUNKS

    def wide(row):
        return jnp.concatenate([row] * (antennas // row.shape[1]), axis=1)

    norm, trace, band = wide(stats_ref[0:1, :]), wide(stats_ref[8:9, :]), wide(band_ref[0:1, :])
    beta = 1.0 / band
    total = 2.0 * (beta * (beta * norm + 2.0 * LOADING * trace) + LOADING * LOADING * antennas)
    omega = 1.0 / jnp.sqrt(total)
    slope, shift = omega * beta, omega * LOADING
    cov, square = cov_ref[...], square_ref[...]
    bend = (slope * slope) * square
    first = split(bend + (2.0 * slope * (shift - 1.0)) * cov)
    second = split((slope * (3.0 - 2.0 * shift)) * cov - bend)
    left, right = slice(0, antennas), slice(antennas, 2 * antennas)
    keep_first, keep_second = 2.0 + shift * (shift - 2.0), 2.0 - shift * (3.0 - shift)
    for n in range(CHUNKS):
        rows, both = slice(n * size, (n + 1) * size), slice(2 * n * size, 2 * (n + 1) * size)
        w_u, w_v = w_ref[rows, left], w_ref[rows, right]
        step = dot3((high_ref[both, :], low_ref[both, :]), first)
        u, v = keep_first * w_u + step[:size], keep_first * w_v + step[size:]
        step = dot3(turn(u, v), second)
        done_ref[rows, left] = omega * (w_u + keep_second * u - step[:size])
        done_ref[rows, right] = omega * (w_v + keep_second * v - step[size:])
        pltpu.make_async_copy(done_ref.at[rows], out_ref.at[rows], sems.at[n]).start()
    for n in range(CHUNKS):
        rows = slice(n * size, (n + 1) * size)
        pltpu.make_async_copy(done_ref.at[rows], out_ref.at[rows], sems.at[n]).wait()


def complex_inverse(re, im):
    size = re.shape[0]
    row = lax.broadcasted_iota(jnp.int32, re.shape, 0)
    column = lax.broadcasted_iota(jnp.int32, re.shape, 1)
    for j in range(size):
        here = column[:1] == j
        col_re, col_im = re[:, j : j + 1], im[:, j : j + 1]
        scale = 1.0 / re[j : j + 1, j : j + 1]
        row_re = jnp.where(here, scale, re[j : j + 1] * scale)
        row_im = jnp.where(here, 0.0, im[j : j + 1] * scale)
        rest_re, rest_im = jnp.where(column == j, 0.0, re), jnp.where(column == j, 0.0, im)
        rest_re = rest_re - (col_re * row_re - col_im * row_im)
        rest_im = rest_im - (col_re * row_im + col_im * row_re)
        re = jnp.where(row == j, row_re, rest_re)
        im = jnp.where(row == j, row_im, rest_im)
    return re, im


def across(left, right):
    return lax.dot_general(
        left, right, (((1,), (1,)), ((), ())), precision=PRECISE, preferred_element_type=F32
    )


def null_kernel(picks_ref, angles_ref, volts_ref, out_ref, high_ref, low_ref):
    antennas = volts_ref.shape[1] // 2
    count = picks_ref.shape[1]
    row = lax.broadcasted_iota(jnp.int32, (count, 128), 0)
    angle = jnp.zeros((count, 128), F32)
    for k in range(count):
        angle = jnp.where(row == k, angles_ref[picks_ref[0, k]], angle)
    rate = (jnp.pi * jnp.sin(angle))[:, :1]
    position = lax.broadcasted_iota(jnp.int32, (count, antennas), 1).astype(F32)
    phase = rate * position
    norming = antennas**0.5
    re, im = jnp.cos(phase) / norming, jnp.sin(phase) / norming
    both = jnp.concatenate([re, im], axis=1)
    turned = jnp.concatenate([-im, re], axis=1)
    eye = lax.broadcasted_iota(jnp.int32, (count, count), 0) == lax.broadcasted_iota(
        jnp.int32, (count, count), 1
    )
    gram_re = across(both, both) + jnp.where(eye, STEER_LOADING, 0.0)
    gram_im = across(both, turned)
    inv_re, inv_im = complex_inverse(gram_re, gram_im)
    steer = jnp.concatenate([both, turned], axis=0)
    inverse = jnp.concatenate(
        [
            jnp.concatenate([inv_re, inv_im], axis=1),
            jnp.concatenate([-inv_im, inv_re], axis=1),
        ],
        axis=0,
    )
    back = jnp.dot(inverse, steer, precision=PRECISE, preferred_element_type=F32)
    volts = volts_ref[...]
    nt = (((1,), (1,)), ((), ()))
    inner = sum(
        lax.dot_general(volts, part, nt, preferred_element_type=F32) for part in split(steer)
    )
    nulled = volts.astype(F32) - dot3(split(inner), split(back))
    out_ref[...] = nulled
    size = volts.shape[0] // CHUNKS
    for n in range(CHUNKS):
        rows, both = slice(n * size, (n + 1) * size), slice(2 * n * size, 2 * (n + 1) * size)
        high, low = turn(nulled[rows, :antennas], nulled[rows, antennas:])
        high_ref[both, :], low_ref[both, :] = high, low


def exchange(value, axis, mask):
    return lax.ppermute(value, axis, [(i, i ^ mask) for i in range(lax.axis_size(axis))])


def choose(index, values):
    chosen = jnp.asarray(values[0], F32)
    for i, value in enumerate(values[1:], 1):
        chosen = jnp.where(index == i, value, chosen)
    return chosen


def earlier_chips(values, decay, mirrored=False, rider=None):
    chips = lax.axis_size("tm") // 2
    chip = lax.axis_index("tm") // 2
    length, totals, before = 1, list(values), [None] * len(values)
    while length < chips:
        last = 2 * length == chips
        mask = 2 * length - 1 if mirrored else length
        upper = (chip // length) % 2 == 1
        weight = jnp.where(upper, choose(chip % length, [decay**i for i in range(length)]), 0.0)
        far = decay**length
        for k, total in enumerate(totals):
            rows = total.shape[0]
            loaded = last and rider is not None and k == len(totals) - 1
            if loaded:
                total = jnp.concatenate([total, rider], axis=0)
            got = exchange(total, "tm", 2 * mask)
            if loaded:
                got, rider = got[:rows], got[rows:]
            before[k] = weight * got if before[k] is None else before[k] + weight * got
            if not last:
                totals[k] = jnp.where(upper, 1.0, far) * total + jnp.where(upper, far, 1.0) * got
        length *= 2
    before = [jnp.zeros_like(v) if b is None else b for v, b in zip(values, before, strict=True)]
    return before if rider is None else (before, rider)


def earlier_levels(level, opposite, decay):
    chips = lax.axis_size("tm") // 2
    chip = lax.axis_index("tm") // 2
    before = 0.0
    for mask in range(1, chips):
        if mask == chips - 1:
            got = opposite
        else:
            got = exchange(level, "tm", 2 * mask)
        weights = [decay ** (c - 1 - (c ^ mask)) if c ^ mask < c else 0.0 for c in range(chips)]
        before = before + choose(chip, weights) * got
    return before


def sum_groups(value):
    groups = lax.axis_size("chan")
    if groups & (groups - 1):
        return lax.psum(value, "chan")
    step = 1
    while step < groups:
        got = exchange(value, "chan", step)
        value = value + got
        step *= 2
    return value


def steps(volts, picks, angles):
    voltage = volts[0]
    rows, width = voltage.shape
    antennas = width // 2
    half = antennas // 2
    segments = rows // SEG
    odd = lax.axis_index("tm") % 2
    parity = odd.reshape(1).astype(jnp.int32)
    is_odd = odd == 1
    decay = (1.0 - 1.0 / HORIZON) ** segments

    keep, give, power = pl.pallas_call(
        gram_kernel,
        out_shape=(
            jax.ShapeDtypeStruct((half, antennas), F32),
            jax.ShapeDtypeStruct((half, antennas), F32),
            jax.ShapeDtypeStruct((8, 128), F32),
        ),
        in_specs=[SM, VM],
        out_specs=(VM, VM, VM),
        scratch_shapes=[pltpu.VMEM((antennas, antennas), F32)],
        cost_estimate=pl.CostEstimate(
            flops=4 * rows * width * antennas, bytes_accessed=rows * width * 2, transcendentals=0
        ),
        compiler_params=PARAMS,
        name="segment_gram",
    )(parity, voltage)

    got = exchange(give, "tm", 1)
    mine, theirs = jnp.where(is_odd, 1.0, decay), jnp.where(is_odd, decay, 1.0)
    size = half // PIECES
    cut = [slice(k * size, (k + 1) * size) for k in range(PIECES)]
    pairs = lax.optimization_barrier([mine * keep[c] + theirs * got[c] for c in cut])
    level = sum_groups(power)
    if lax.axis_size("tm") // 2 == DIRECT:
        wide = jnp.concatenate([level] * (antennas // level.shape[1]), axis=1)
        before, opposite = earlier_chips(pairs, decay * decay, True, wide)
        level_before = earlier_levels(level, opposite[:, : level.shape[1]], decay * decay)
    else:
        before = earlier_chips(pairs, decay * decay, True)
        (level_before,) = earlier_chips([level], decay * decay)
    owns, others = [], []
    for k, c in enumerate(cut):
        even_cov = decay * before[k] + jnp.where(is_odd, got[c], keep[c])
        odd_cov = decay * decay * before[k] + pairs[k]
        owns.append(jnp.where(is_odd, odd_cov, even_cov))
        others.append(exchange(jnp.where(is_odd, even_cov, odd_cov), "tm", 1))

    levels = jnp.concatenate([level, level_before], axis=0)
    got_levels = exchange(levels, "tm", 1)
    level_even = jnp.where(is_odd, got_levels, levels)
    level_odd = jnp.where(is_odd, levels, got_levels)
    level_own = decay * (decay * level_even[8:] + level_odd[8:]) + level_even[:8]
    level_own = jnp.where(is_odd, decay * level_own + level_odd[:8], level_own)
    band = level_own / lax.axis_size("chan") + TINY_LEVEL

    projected, high, low = pl.pallas_call(
        null_kernel,
        out_shape=(
            jax.ShapeDtypeStruct((rows, width), F32),
            jax.ShapeDtypeStruct((2 * rows, width), BF16),
            jax.ShapeDtypeStruct((2 * rows, width), BF16),
        ),
        in_specs=[SM, SM, VM],
        out_specs=(VM, VM, VM),
        cost_estimate=pl.CostEstimate(
            flops=4 * rows * width * 128, bytes_accessed=rows * width * 6, transcendentals=0
        ),
        compiler_params=PARAMS,
        name="null",
    )(picks, angles, voltage)

    cov, square, stats = pl.pallas_call(
        square_kernel,
        out_shape=(
            jax.ShapeDtypeStruct((width, antennas), F32),
            jax.ShapeDtypeStruct((width, antennas), F32),
            jax.ShapeDtypeStruct((16, 128), F32),
        ),
        in_specs=[SM] + [VM] * (2 * PIECES),
        out_specs=(VM, VM, VM),
        scratch_shapes=[pltpu.VMEM((antennas, antennas), F32)],
        cost_estimate=pl.CostEstimate(
            flops=6 * width * width * antennas, bytes_accessed=width * antennas * 8, transcendentals=0
        ),
        compiler_params=PARAMS,
        name="square",
    )(parity, *owns, *others)

    cleaned = pl.pallas_call(
        whiten_kernel,
        out_shape=jax.ShapeDtypeStruct((rows, width), F32),
        in_specs=[VM] * 7,
        out_specs=pl.BlockSpec(memory_space=pl.ANY),
        scratch_shapes=[pltpu.VMEM((rows, width), F32), pltpu.SemaphoreType.DMA((CHUNKS,))],
        cost_estimate=pl.CostEstimate(
            flops=12 * rows * width * width, bytes_accessed=rows * width * 8, transcendentals=0
        ),
        compiler_params=PARAMS,
        name="whiten",
    )(band, stats, cov, square, projected, high, low)
    return cleaned[None]


def solution(mesh):
    placed = (P("chan", "tm", None), P("chan", None), P())
    return jax.shard_map(
        steps, mesh=mesh, in_specs=placed, out_specs=P("chan", "tm", None), check_vma=False
    )
```

```python
import jax
import jax.numpy as jnp
from jax import lax
from jax.experimental import pallas as pl
from jax.experimental.pallas import tpu as pltpu
from jax.sharding import PartitionSpec as P


SEG = 256
HORIZON = 256
CHUNKS = 4
DIRECT = 4
LOADING = 0.1
STEER_LOADING = 0.05
TINY_LEVEL = 1e-06
PRECISE = lax.Precision.HIGHEST
F32 = jnp.float32
BF16 = jnp.bfloat16
VM = pl.BlockSpec(memory_space=pltpu.VMEM)
SM = pl.BlockSpec(memory_space=pltpu.SMEM)
PARAMS = pltpu.CompilerParams(vmem_limit_bytes=24 * 2**20)


def gram_kernel(parity_ref, volts_ref, keep_ref, give_ref, power_ref, mixed_ref):
    antennas = volts_ref.shape[1] // 2
    segments = volts_ref.shape[0] // SEG
    half = antennas // 2
    forget = 1.0 - 1.0 / HORIZON
    mixed = None
    for seg in range(segments):
        a = volts_ref[seg * SEG : (seg + 1) * SEG, :antennas]
        b = volts_ref[seg * SEG : (seg + 1) * SEG, antennas:]
        left = jnp.concatenate([a, b, b, -a], axis=0)
        right = jnp.concatenate([a, b, a, b], axis=0)
        term = lax.dot_general(
            left, right, (((0,), (0,)), ((), ())), preferred_element_type=F32
        )
        mixed = term if mixed is None else forget * mixed + term
    mixed_ref[...] = mixed
    row = lax.broadcasted_iota(jnp.int32, mixed.shape, 0)
    column = lax.broadcasted_iota(jnp.int32, mixed.shape, 1)
    trace = jnp.sum(jnp.where(row == column, mixed, 0.0))
    power_ref[...] = jnp.full(power_ref.shape, trace / antennas, F32)
    parity = parity_ref[0]
    keep_ref[...] = mixed_ref[pl.ds(pl.multiple_of(parity * half, half), half), :]
    give_ref[...] = mixed_ref[pl.ds(pl.multiple_of((1 - parity) * half, half), half), :]


def split(value):
    high = value.astype(BF16)
    return high, (value - high.astype(F32)).astype(BF16)


def dot3(left, right):
    (lh, ll), (rh, rl) = left, right
    return (
        jnp.dot(lh, rh, preferred_element_type=F32)
        + jnp.dot(lh, rl, preferred_element_type=F32)
        + jnp.dot(ll, rh, preferred_element_type=F32)
    )


def beside(first, second):
    return jnp.concatenate([first, second], axis=1)


def over(first, second):
    return jnp.concatenate([first, second], axis=0)


def turn(u, v):
    parts = zip(split(u), split(v), strict=True)
    return tuple(over(beside(p, q), beside(q, -p)) for p, q in parts)


def square_kernel(parity_ref, own_ref, other_ref, cov_ref, square_ref, stats_ref, mixed_ref):
    half, antennas = own_ref.shape
    parity = parity_ref[0]
    mixed_ref[pl.ds(pl.multiple_of(parity * half, half), half), :] = own_ref[...]
    mixed_ref[pl.ds(pl.multiple_of((1 - parity) * half, half), half), :] = other_ref[...]
    mixed = mixed_ref[...]
    flipped = mixed.T
    re, im = 0.5 * (mixed + flipped), 0.5 * (mixed - flipped)
    cov_ref[:antennas, :], cov_ref[antennas:, :] = re, im
    (rh, rl), (ih, il) = split(re), split(im)
    full = tuple(over(beside(r, -i), beside(i, r)) for r, i in ((rh, ih), (rl, il)))
    square_ref[...] = dot3(full, (over(rh, ih), over(rl, il)))
    row = lax.broadcasted_iota(jnp.int32, mixed.shape, 0)
    column = lax.broadcasted_iota(jnp.int32, mixed.shape, 1)
    trace = jnp.sum(jnp.where(row == column, mixed, 0.0), keepdims=True)
    norm = jnp.sum(mixed * mixed, keepdims=True)
    stats_ref[:8, :] = jnp.broadcast_to(norm, (8, stats_ref.shape[1]))
    stats_ref[8:, :] = jnp.broadcast_to(trace, (8, stats_ref.shape[1]))


def whiten_kernel(
    band_ref, stats_ref, cov_ref, square_ref, w_ref, high_ref, low_ref, out_ref, done_ref, sems
):
    samples = w_ref.shape[0]
    antennas = cov_ref.shape[1]
    size = samples // CHUNKS

    def wide(row):
        return jnp.concatenate([row] * (antennas // row.shape[1]), axis=1)

    norm, trace, band = wide(stats_ref[0:1, :]), wide(stats_ref[8:9, :]), wide(band_ref[0:1, :])
    beta = 1.0 / band
    total = 2.0 * (beta * (beta * norm + 2.0 * LOADING * trace) + LOADING * LOADING * antennas)
    omega = 1.0 / jnp.sqrt(total)
    slope, shift = omega * beta, omega * LOADING
    cov, square = cov_ref[...], square_ref[...]
    bend = (slope * slope) * square
    first = split(bend + (2.0 * slope * (shift - 1.0)) * cov)
    second = split((slope * (3.0 - 2.0 * shift)) * cov - bend)
    left, right = slice(0, antennas), slice(antennas, 2 * antennas)
    keep_first, keep_second = 2.0 + shift * (shift - 2.0), 2.0 - shift * (3.0 - shift)
    for n in range(CHUNKS):
        rows, both = slice(n * size, (n + 1) * size), slice(2 * n * size, 2 * (n + 1) * size)
        w_u, w_v = w_ref[rows, left], w_ref[rows, right]
        step = dot3((high_ref[both, :], low_ref[both, :]), first)
        u, v = keep_first * w_u + step[:size], keep_first * w_v + step[size:]
        step = dot3(turn(u, v), second)
        done_ref[rows, left] = omega * (w_u + keep_second * u - step[:size])
        done_ref[rows, right] = omega * (w_v + keep_second * v - step[size:])
        pltpu.make_async_copy(done_ref.at[rows], out_ref.at[rows], sems.at[n]).start()
    for n in range(CHUNKS):
        rows = slice(n * size, (n + 1) * size)
        pltpu.make_async_copy(done_ref.at[rows], out_ref.at[rows], sems.at[n]).wait()


def complex_inverse(re, im):
    size = re.shape[0]
    row = lax.broadcasted_iota(jnp.int32, re.shape, 0)
    column = lax.broadcasted_iota(jnp.int32, re.shape, 1)
    for j in range(size):
        here = column[:1] == j
        col_re, col_im = re[:, j : j + 1], im[:, j : j + 1]
        scale = 1.0 / re[j : j + 1, j : j + 1]
        row_re = jnp.where(here, scale, re[j : j + 1] * scale)
        row_im = jnp.where(here, 0.0, im[j : j + 1] * scale)
        rest_re, rest_im = jnp.where(column == j, 0.0, re), jnp.where(column == j, 0.0, im)
        rest_re = rest_re - (col_re * row_re - col_im * row_im)
        rest_im = rest_im - (col_re * row_im + col_im * row_re)
        re = jnp.where(row == j, row_re, rest_re)
        im = jnp.where(row == j, row_im, rest_im)
    return re, im


def across(left, right):
    return lax.dot_general(
        left, right, (((1,), (1,)), ((), ())), precision=PRECISE, preferred_element_type=F32
    )


def null_kernel(picks_ref, angles_ref, volts_ref, out_ref, high_ref, low_ref):
    antennas = volts_ref.shape[1] // 2
    count = picks_ref.shape[1]
    row = lax.broadcasted_iota(jnp.int32, (count, 128), 0)
    angle = jnp.zeros((count, 128), F32)
    for k in range(count):
        angle = jnp.where(row == k, angles_ref[picks_ref[0, k]], angle)
    rate = (jnp.pi * jnp.sin(angle))[:, :1]
    position = lax.broadcasted_iota(jnp.int32, (count, antennas), 1).astype(F32)
    phase = rate * position
    norming = antennas**0.5
    re, im = jnp.cos(phase) / norming, jnp.sin(phase) / norming
    both = jnp.concatenate([re, im], axis=1)
    turned = jnp.concatenate([-im, re], axis=1)
    eye = lax.broadcasted_iota(jnp.int32, (count, count), 0) == lax.broadcasted_iota(
        jnp.int32, (count, count), 1
    )
    gram_re = across(both, both) + jnp.where(eye, STEER_LOADING, 0.0)
    gram_im = across(both, turned)
    inv_re, inv_im = complex_inverse(gram_re, gram_im)
    steer = jnp.concatenate([both, turned], axis=0)
    inverse = jnp.concatenate(
        [
            jnp.concatenate([inv_re, inv_im], axis=1),
            jnp.concatenate([-inv_im, inv_re], axis=1),
        ],
        axis=0,
    )
    back = jnp.dot(inverse, steer, precision=PRECISE, preferred_element_type=F32)
    volts = volts_ref[...]
    nt = (((1,), (1,)), ((), ()))
    inner = sum(
        lax.dot_general(volts, part, nt, preferred_element_type=F32) for part in split(steer)
    )
    nulled = volts.astype(F32) - dot3(split(inner), split(back))
    out_ref[...] = nulled
    size = volts.shape[0] // CHUNKS
    for n in range(CHUNKS):
        rows, both = slice(n * size, (n + 1) * size), slice(2 * n * size, 2 * (n + 1) * size)
        high, low = turn(nulled[rows, :antennas], nulled[rows, antennas:])
        high_ref[both, :], low_ref[both, :] = high, low


def exchange(value, axis, mask):
    return lax.ppermute(value, axis, [(i, i ^ mask) for i in range(lax.axis_size(axis))])


def choose(index, values):
    chosen = jnp.asarray(values[0], F32)
    for i, value in enumerate(values[1:], 1):
        chosen = jnp.where(index == i, value, chosen)
    return chosen


def earlier_chips(value, decay, mirrored=False, rider=None):
    chips = lax.axis_size("tm") // 2
    chip = lax.axis_index("tm") // 2
    length, total, before = 1, value, None
    while length < chips:
        last = 2 * length == chips
        mask = 2 * length - 1 if mirrored else length
        rows = total.shape[0]
        if last and rider is not None:
            total = jnp.concatenate([total, rider], axis=0)
        got = exchange(total, "tm", 2 * mask)
        if last and rider is not None:
            got, rider = got[:rows], got[rows:]
        upper = (chip // length) % 2 == 1
        weight = jnp.where(upper, choose(chip % length, [decay**i for i in range(length)]), 0.0)
        before = weight * got if before is None else before + weight * got
        if not last:
            far = decay**length
            total = jnp.where(upper, 1.0, far) * total + jnp.where(upper, far, 1.0) * got
        length *= 2
    before = jnp.zeros_like(value) if before is None else before
    return before if rider is None else (before, rider)


def earlier_levels(level, opposite, decay):
    chips = lax.axis_size("tm") // 2
    chip = lax.axis_index("tm") // 2
    before = 0.0
    for mask in range(1, chips):
        if mask == chips - 1:
            got = opposite
        else:
            got = exchange(level, "tm", 2 * mask)
        weights = [decay ** (c - 1 - (c ^ mask)) if c ^ mask < c else 0.0 for c in range(chips)]
        before = before + choose(chip, weights) * got
    return before


def sum_groups(value):
    groups = lax.axis_size("chan")
    if groups & (groups - 1):
        return lax.psum(value, "chan")
    if groups <= DIRECT:
        return sum((exchange(value, "chan", k) for k in range(1, groups)), value)
    step = 1
    while step < groups:
        value = value + exchange(value, "chan", step)
        step *= 2
    return value


def steps(volts, picks, angles):
    voltage = volts[0]
    rows, width = voltage.shape
    antennas = width // 2
    half = antennas // 2
    segments = rows // SEG
    odd = lax.axis_index("tm") % 2
    parity = odd.reshape(1).astype(jnp.int32)
    is_odd = odd == 1
    decay = (1.0 - 1.0 / HORIZON) ** segments

    keep, give, power = pl.pallas_call(
        gram_kernel,
        out_shape=(
            jax.ShapeDtypeStruct((half, antennas), F32),
            jax.ShapeDtypeStruct((half, antennas), F32),
            jax.ShapeDtypeStruct((8, 128), F32),
        ),
        in_specs=[SM, VM],
        out_specs=(VM, VM, VM),
        scratch_shapes=[pltpu.VMEM((antennas, antennas), F32)],
        cost_estimate=pl.CostEstimate(
            flops=4 * rows * width * antennas, bytes_accessed=rows * width * 2, transcendentals=0
        ),
        compiler_params=PARAMS,
        name="segment_gram",
    )(parity, voltage)

    got = exchange(give, "tm", 1)
    mine, theirs = jnp.where(is_odd, 1.0, decay), jnp.where(is_odd, decay, 1.0)
    pair = mine * keep + theirs * got
    level = sum_groups(power)
    direct = lax.axis_size("tm") // 2 == DIRECT
    if direct:
        wide = jnp.concatenate([level] * (antennas // level.shape[1]), axis=1)
        before, opposite = earlier_chips(pair, decay * decay, True, wide)
        level_before = earlier_levels(level, opposite[:, : level.shape[1]], decay * decay)
    else:
        before = earlier_chips(pair, decay * decay, True)
        level_before = earlier_chips(level, decay * decay)
    even_cov = decay * before + jnp.where(is_odd, got, keep)
    odd_cov = decay * decay * before + pair
    own = jnp.where(is_odd, odd_cov, even_cov)
    other = exchange(jnp.where(is_odd, even_cov, odd_cov), "tm", 1)

    levels = jnp.concatenate([level, level_before], axis=0)
    got_levels = exchange(levels, "tm", 1)
    level_even = jnp.where(is_odd, got_levels, levels)
    level_odd = jnp.where(is_odd, levels, got_levels)
    level_own = decay * (decay * level_even[8:] + level_odd[8:]) + level_even[:8]
    level_own = jnp.where(is_odd, decay * level_own + level_odd[:8], level_own)
    band = level_own / lax.axis_size("chan") + TINY_LEVEL

    projected, high, low = pl.pallas_call(
        null_kernel,
        out_shape=(
            jax.ShapeDtypeStruct((rows, width), F32),
            jax.ShapeDtypeStruct((2 * rows, width), BF16),
            jax.ShapeDtypeStruct((2 * rows, width), BF16),
        ),
        in_specs=[SM, SM, VM],
        out_specs=(VM, VM, VM),
        cost_estimate=pl.CostEstimate(
            flops=4 * rows * width * 128, bytes_accessed=rows * width * 6, transcendentals=0
        ),
        compiler_params=PARAMS,
        name="null",
    )(picks, angles, voltage)

    cov, square, stats = pl.pallas_call(
        square_kernel,
        out_shape=(
            jax.ShapeDtypeStruct((width, antennas), F32),
            jax.ShapeDtypeStruct((width, antennas), F32),
            jax.ShapeDtypeStruct((16, 128), F32),
        ),
        in_specs=[SM, VM, VM],
        out_specs=(VM, VM, VM),
        scratch_shapes=[pltpu.VMEM((antennas, antennas), F32)],
        cost_estimate=pl.CostEstimate(
            flops=6 * width * width * antennas, bytes_accessed=width * antennas * 8, transcendentals=0
        ),
        compiler_params=PARAMS,
        name="square",
    )(parity, own, other)

    cleaned = pl.pallas_call(
        whiten_kernel,
        out_shape=jax.ShapeDtypeStruct((rows, width), F32),
        in_specs=[VM] * 7,
        out_specs=pl.BlockSpec(memory_space=pl.ANY),
        scratch_shapes=[pltpu.VMEM((rows, width), F32), pltpu.SemaphoreType.DMA((CHUNKS,))],
        cost_estimate=pl.CostEstimate(
            flops=12 * rows * width * width, bytes_accessed=rows * width * 8, transcendentals=0
        ),
        compiler_params=PARAMS,
        name="whiten",
    )(band, stats, cov, square, projected, high, low)
    return cleaned[None]


def solution(mesh):
    placed = (P("chan", "tm", None), P("chan", None), P())
    return jax.shard_map(
        steps, mesh=mesh, in_specs=placed, out_specs=P("chan", "tm", None), check_vma=False
    )
```

```python
import jax
import jax.numpy as jnp
from jax import lax
from jax.experimental import pallas as pl
from jax.experimental.pallas import tpu as pltpu
from jax.sharding import PartitionSpec as P


SEG = 256
HORIZON = 256
CHUNKS = 4
DIRECT = 4
LOADING = 0.1
STEER_LOADING = 0.05
TINY_LEVEL = 1e-06
PRECISE = lax.Precision.HIGHEST
F32 = jnp.float32
BF16 = jnp.bfloat16
VM = pl.BlockSpec(memory_space=pltpu.VMEM)
SM = pl.BlockSpec(memory_space=pltpu.SMEM)
PARAMS = pltpu.CompilerParams(vmem_limit_bytes=24 * 2**20)


def gram_kernel(parity_ref, volts_ref, keep_ref, give_ref, power_ref, mixed_ref):
    antennas = volts_ref.shape[1] // 2
    segments = volts_ref.shape[0] // SEG
    half = antennas // 2
    forget = 1.0 - 1.0 / HORIZON
    mixed = None
    for seg in range(segments):
        a = volts_ref[seg * SEG : (seg + 1) * SEG, :antennas]
        b = volts_ref[seg * SEG : (seg + 1) * SEG, antennas:]
        left = jnp.concatenate([a, b, b, -a], axis=0)
        right = jnp.concatenate([a, b, a, b], axis=0)
        term = lax.dot_general(
            left, right, (((0,), (0,)), ((), ())), preferred_element_type=F32
        )
        mixed = term if mixed is None else forget * mixed + term
    mixed_ref[...] = mixed
    row = lax.broadcasted_iota(jnp.int32, mixed.shape, 0)
    column = lax.broadcasted_iota(jnp.int32, mixed.shape, 1)
    trace = jnp.sum(jnp.where(row == column, mixed, 0.0))
    power_ref[...] = jnp.full(power_ref.shape, trace / antennas, F32)
    parity = parity_ref[0]
    keep_ref[...] = mixed_ref[pl.ds(pl.multiple_of(parity * half, half), half), :]
    give_ref[...] = mixed_ref[pl.ds(pl.multiple_of((1 - parity) * half, half), half), :]


def split(value):
    high = value.astype(BF16)
    return high, (value - high.astype(F32)).astype(BF16)


def dot3(left, right):
    (lh, ll), (rh, rl) = left, right
    return (
        jnp.dot(lh, rh, preferred_element_type=F32)
        + jnp.dot(lh, rl, preferred_element_type=F32)
        + jnp.dot(ll, rh, preferred_element_type=F32)
    )


def beside(first, second):
    return jnp.concatenate([first, second], axis=1)


def over(first, second):
    return jnp.concatenate([first, second], axis=0)


def turn(u, v):
    parts = zip(split(u), split(v), strict=True)
    return tuple(over(beside(p, q), beside(q, -p)) for p, q in parts)


def square_kernel(parity_ref, own_ref, other_ref, cov_ref, square_ref, stats_ref, mixed_ref):
    half, antennas = own_ref.shape
    parity = parity_ref[0]
    mixed_ref[pl.ds(pl.multiple_of(parity * half, half), half), :] = own_ref[...]
    mixed_ref[pl.ds(pl.multiple_of((1 - parity) * half, half), half), :] = other_ref[...]
    mixed = mixed_ref[...]
    flipped = mixed.T
    re, im = 0.5 * (mixed + flipped), 0.5 * (mixed - flipped)
    cov_ref[:antennas, :], cov_ref[antennas:, :] = re, im
    (rh, rl), (ih, il) = split(re), split(im)
    full = tuple(over(beside(r, -i), beside(i, r)) for r, i in ((rh, ih), (rl, il)))
    square_ref[...] = dot3(full, (over(rh, ih), over(rl, il)))
    row = lax.broadcasted_iota(jnp.int32, mixed.shape, 0)
    column = lax.broadcasted_iota(jnp.int32, mixed.shape, 1)
    trace = jnp.sum(jnp.where(row == column, mixed, 0.0), keepdims=True)
    norm = jnp.sum(mixed * mixed, keepdims=True)
    stats_ref[:8, :] = jnp.broadcast_to(norm, (8, stats_ref.shape[1]))
    stats_ref[8:, :] = jnp.broadcast_to(trace, (8, stats_ref.shape[1]))


def whiten_kernel(
    band_ref, stats_ref, cov_ref, square_ref, w_ref, high_ref, low_ref, out_ref, done_ref, sems
):
    samples = w_ref.shape[0]
    antennas = cov_ref.shape[1]
    size = samples // CHUNKS

    def wide(row):
        return jnp.concatenate([row] * (antennas // row.shape[1]), axis=1)

    norm, trace, band = wide(stats_ref[0:1, :]), wide(stats_ref[8:9, :]), wide(band_ref[0:1, :])
    beta = 1.0 / band
    total = 2.0 * (beta * (beta * norm + 2.0 * LOADING * trace) + LOADING * LOADING * antennas)
    omega = 1.0 / jnp.sqrt(total)
    slope, shift = omega * beta, omega * LOADING
    cov, square = cov_ref[...], square_ref[...]
    bend = (slope * slope) * square
    first = split(bend + (2.0 * slope * (shift - 1.0)) * cov)
    second = split((slope * (3.0 - 2.0 * shift)) * cov - bend)
    left, right = slice(0, antennas), slice(antennas, 2 * antennas)
    keep_first, keep_second = 2.0 + shift * (shift - 2.0), 2.0 - shift * (3.0 - shift)

    def begin(n):
        both = slice(2 * n * size, 2 * (n + 1) * size)
        return dot3((high_ref[both, :], low_ref[both, :]), first)

    steps = [begin(n) for n in range(CHUNKS)]
    for n, step in enumerate(steps):
        rows = slice(n * size, (n + 1) * size)
        w_u, w_v = w_ref[rows, left], w_ref[rows, right]
        u, v = keep_first * w_u + step[:size], keep_first * w_v + step[size:]
        step = dot3(turn(u, v), second)
        done_ref[rows, left] = omega * (w_u + keep_second * u - step[:size])
        done_ref[rows, right] = omega * (w_v + keep_second * v - step[size:])
        pltpu.make_async_copy(done_ref.at[rows], out_ref.at[rows], sems.at[n]).start()
    for n in range(CHUNKS):
        rows = slice(n * size, (n + 1) * size)
        pltpu.make_async_copy(done_ref.at[rows], out_ref.at[rows], sems.at[n]).wait()


def complex_inverse(re, im):
    size = re.shape[0]
    row = lax.broadcasted_iota(jnp.int32, re.shape, 0)
    column = lax.broadcasted_iota(jnp.int32, re.shape, 1)
    for j in range(size):
        here = column[:1] == j
        col_re, col_im = re[:, j : j + 1], im[:, j : j + 1]
        scale = 1.0 / re[j : j + 1, j : j + 1]
        row_re = jnp.where(here, scale, re[j : j + 1] * scale)
        row_im = jnp.where(here, 0.0, im[j : j + 1] * scale)
        rest_re, rest_im = jnp.where(column == j, 0.0, re), jnp.where(column == j, 0.0, im)
        rest_re = rest_re - (col_re * row_re - col_im * row_im)
        rest_im = rest_im - (col_re * row_im + col_im * row_re)
        re = jnp.where(row == j, row_re, rest_re)
        im = jnp.where(row == j, row_im, rest_im)
    return re, im


def across(left, right):
    return lax.dot_general(
        left, right, (((1,), (1,)), ((), ())), precision=PRECISE, preferred_element_type=F32
    )


def null_kernel(picks_ref, angles_ref, volts_ref, out_ref, high_ref, low_ref):
    antennas = volts_ref.shape[1] // 2
    count = picks_ref.shape[1]
    row = lax.broadcasted_iota(jnp.int32, (count, 128), 0)
    angle = jnp.zeros((count, 128), F32)
    for k in range(count):
        angle = jnp.where(row == k, angles_ref[picks_ref[0, k]], angle)
    rate = (jnp.pi * jnp.sin(angle))[:, :1]
    position = lax.broadcasted_iota(jnp.int32, (count, antennas), 1).astype(F32)
    phase = rate * position
    norming = antennas**0.5
    re, im = jnp.cos(phase) / norming, jnp.sin(phase) / norming
    both = jnp.concatenate([re, im], axis=1)
    turned = jnp.concatenate([-im, re], axis=1)
    eye = lax.broadcasted_iota(jnp.int32, (count, count), 0) == lax.broadcasted_iota(
        jnp.int32, (count, count), 1
    )
    gram_re = across(both, both) + jnp.where(eye, STEER_LOADING, 0.0)
    gram_im = across(both, turned)
    inv_re, inv_im = complex_inverse(gram_re, gram_im)
    steer = jnp.concatenate([both, turned], axis=0)
    inverse = jnp.concatenate(
        [
            jnp.concatenate([inv_re, inv_im], axis=1),
            jnp.concatenate([-inv_im, inv_re], axis=1),
        ],
        axis=0,
    )
    back = jnp.dot(inverse, steer, precision=PRECISE, preferred_element_type=F32)
    volts = volts_ref[...]
    nt = (((1,), (1,)), ((), ()))
    inner = sum(
        lax.dot_general(volts, part, nt, preferred_element_type=F32) for part in split(steer)
    )
    nulled = volts.astype(F32) - dot3(split(inner), split(back))
    out_ref[...] = nulled
    size = volts.shape[0] // CHUNKS
    for n in range(CHUNKS):
        rows, both = slice(n * size, (n + 1) * size), slice(2 * n * size, 2 * (n + 1) * size)
        high, low = turn(nulled[rows, :antennas], nulled[rows, antennas:])
        high_ref[both, :], low_ref[both, :] = high, low


def exchange(value, axis, mask):
    return lax.ppermute(value, axis, [(i, i ^ mask) for i in range(lax.axis_size(axis))])


def choose(index, values):
    chosen = jnp.asarray(values[0], F32)
    for i, value in enumerate(values[1:], 1):
        chosen = jnp.where(index == i, value, chosen)
    return chosen


def earlier_chips(value, decay, mirrored=False):
    chips = lax.axis_size("tm") // 2
    chip = lax.axis_index("tm") // 2
    length, total, before = 1, value, None
    while length < chips:
        mask = 2 * length - 1 if mirrored else length
        got = exchange(total, "tm", 2 * mask)
        upper = (chip // length) % 2 == 1
        weight = jnp.where(upper, choose(chip % length, [decay**i for i in range(length)]), 0.0)
        before = weight * got if before is None else before + weight * got
        if 2 * length < chips:
            far = decay**length
            total = jnp.where(upper, 1.0, far) * total + jnp.where(upper, far, 1.0) * got
        length *= 2
    return jnp.zeros_like(value) if before is None else before


def earlier_levels(level, decay):
    chips = lax.axis_size("tm") // 2
    chip = lax.axis_index("tm") // 2
    before = jnp.zeros_like(level)
    for mask in range(1, chips):
        got = exchange(level, "tm", 2 * mask)
        weights = [decay ** (c - 1 - (c ^ mask)) if c ^ mask < c else 0.0 for c in range(chips)]
        before = before + choose(chip, weights) * got
    return before


def sum_groups(value):
    groups = lax.axis_size("chan")
    if groups & (groups - 1):
        return lax.psum(value, "chan")
    step = 1
    while step < groups:
        got = exchange(value, "chan", step)
        value = value + got
        step *= 2
    return value


def steps(volts, picks, angles):
    voltage = volts[0]
    rows, width = voltage.shape
    antennas = width // 2
    half = antennas // 2
    segments = rows // SEG
    odd = lax.axis_index("tm") % 2
    parity = odd.reshape(1).astype(jnp.int32)
    is_odd = odd == 1
    decay = (1.0 - 1.0 / HORIZON) ** segments

    keep, give, power = pl.pallas_call(
        gram_kernel,
        out_shape=(
            jax.ShapeDtypeStruct((half, antennas), F32),
            jax.ShapeDtypeStruct((half, antennas), F32),
            jax.ShapeDtypeStruct((8, 128), F32),
        ),
        in_specs=[SM, VM],
        out_specs=(VM, VM, VM),
        scratch_shapes=[pltpu.VMEM((antennas, antennas), F32)],
        cost_estimate=pl.CostEstimate(
            flops=4 * rows * width * antennas, bytes_accessed=rows * width * 2, transcendentals=0
        ),
        compiler_params=PARAMS,
        name="segment_gram",
    )(parity, voltage)

    got = exchange(give, "tm", 1)
    mine, theirs = jnp.where(is_odd, 1.0, decay), jnp.where(is_odd, decay, 1.0)
    pair = mine * keep + theirs * got
    before = earlier_chips(pair, decay * decay, True)
    level = sum_groups(power)
    if lax.axis_size("tm") // 2 <= DIRECT:
        level_before = earlier_levels(level, decay * decay)
    else:
        level_before = earlier_chips(level, decay * decay)
    even_cov = decay * before + jnp.where(is_odd, got, keep)
    odd_cov = decay * decay * before + pair
    own = jnp.where(is_odd, odd_cov, even_cov)
    other = exchange(jnp.where(is_odd, even_cov, odd_cov), "tm", 1)

    levels = jnp.concatenate([level, level_before], axis=0)
    got_levels = exchange(levels, "tm", 1)
    level_even = jnp.where(is_odd, got_levels, levels)
    level_odd = jnp.where(is_odd, levels, got_levels)
    level_own = decay * (decay * level_even[8:] + level_odd[8:]) + level_even[:8]
    level_own = jnp.where(is_odd, decay * level_own + level_odd[:8], level_own)
    band = level_own / lax.axis_size("chan") + TINY_LEVEL

    projected, high, low = pl.pallas_call(
        null_kernel,
        out_shape=(
            jax.ShapeDtypeStruct((rows, width), F32),
            jax.ShapeDtypeStruct((2 * rows, width), BF16),
            jax.ShapeDtypeStruct((2 * rows, width), BF16),
        ),
        in_specs=[SM, SM, VM],
        out_specs=(VM, VM, VM),
        cost_estimate=pl.CostEstimate(
            flops=4 * rows * width * 128, bytes_accessed=rows * width * 6, transcendentals=0
        ),
        compiler_params=PARAMS,
        name="null",
    )(picks, angles, voltage)

    cov, square, stats = pl.pallas_call(
        square_kernel,
        out_shape=(
            jax.ShapeDtypeStruct((width, antennas), F32),
            jax.ShapeDtypeStruct((width, antennas), F32),
            jax.ShapeDtypeStruct((16, 128), F32),
        ),
        in_specs=[SM, VM, VM],
        out_specs=(VM, VM, VM),
        scratch_shapes=[pltpu.VMEM((antennas, antennas), F32)],
        cost_estimate=pl.CostEstimate(
            flops=6 * width * width * antennas, bytes_accessed=width * antennas * 8, transcendentals=0
        ),
        compiler_params=PARAMS,
        name="square",
    )(parity, own, other)

    cleaned = pl.pallas_call(
        whiten_kernel,
        out_shape=jax.ShapeDtypeStruct((rows, width), F32),
        in_specs=[VM] * 7,
        out_specs=pl.BlockSpec(memory_space=pl.ANY),
        scratch_shapes=[pltpu.VMEM((rows, width), F32), pltpu.SemaphoreType.DMA((CHUNKS,))],
        cost_estimate=pl.CostEstimate(
            flops=12 * rows * width * width, bytes_accessed=rows * width * 8, transcendentals=0
        ),
        compiler_params=PARAMS,
        name="whiten",
    )(band, stats, cov, square, projected, high, low)
    return cleaned[None]


def solution(mesh):
    placed = (P("chan", "tm", None), P("chan", None), P())
    return jax.shard_map(
        steps, mesh=mesh, in_specs=placed, out_specs=P("chan", "tm", None), check_vma=False
    )
```

```python
import jax
import jax.numpy as jnp
from jax import lax
from jax.experimental import pallas as pl
from jax.experimental.pallas import tpu as pltpu
from jax.sharding import PartitionSpec as P


SEG = 256
HORIZON = 256
LANES = 128
CHUNKS = 4
DIRECT = 4
LOADING = 0.1
STEER_LOADING = 0.05
TINY_LEVEL = 1e-06
PRECISE = lax.Precision.HIGHEST
F32 = jnp.float32
BF16 = jnp.bfloat16
VM = pl.BlockSpec(memory_space=pltpu.VMEM)
SM = pl.BlockSpec(memory_space=pltpu.SMEM)
PARAMS = pltpu.CompilerParams(vmem_limit_bytes=24 * 2**20)


def gram_kernel(parity_ref, volts_ref, keep_ref, give_ref, power_ref, mixed_ref):
    antennas = volts_ref.shape[1] // 2
    segments = volts_ref.shape[0] // SEG
    half = antennas // 2
    forget = 1.0 - 1.0 / HORIZON
    mixed = None
    for seg in range(segments):
        a = volts_ref[seg * SEG : (seg + 1) * SEG, :antennas]
        b = volts_ref[seg * SEG : (seg + 1) * SEG, antennas:]
        left = jnp.concatenate([a, b, b, -a], axis=0)
        right = jnp.concatenate([a, b, a, b], axis=0)
        term = lax.dot_general(
            left, right, (((0,), (0,)), ((), ())), preferred_element_type=F32
        )
        mixed = term if mixed is None else forget * mixed + term
    mixed_ref[...] = mixed
    row = lax.broadcasted_iota(jnp.int32, mixed.shape, 0)
    column = lax.broadcasted_iota(jnp.int32, mixed.shape, 1)
    trace = jnp.sum(jnp.where(row == column, mixed, 0.0))
    power_ref[...] = jnp.full(power_ref.shape, trace / antennas, F32)
    parity = parity_ref[0]
    lanes = keep_ref.shape[1]
    for n in range(antennas // lanes):
        rows, columns = slice(n * half, (n + 1) * half), slice(n * lanes, (n + 1) * lanes)
        keep_ref[rows, :] = mixed_ref[pl.ds(pl.multiple_of(parity * half, half), half), columns]
        give_ref[rows, :] = mixed_ref[pl.ds(pl.multiple_of((1 - parity) * half, half), half), columns]


def split(value):
    high = value.astype(BF16)
    return high, (value - high.astype(F32)).astype(BF16)


def dot3(left, right):
    (lh, ll), (rh, rl) = left, right
    return (
        jnp.dot(lh, rh, preferred_element_type=F32)
        + jnp.dot(lh, rl, preferred_element_type=F32)
        + jnp.dot(ll, rh, preferred_element_type=F32)
    )


def beside(first, second):
    return jnp.concatenate([first, second], axis=1)


def over(first, second):
    return jnp.concatenate([first, second], axis=0)


def turn(u, v):
    parts = zip(split(u), split(v), strict=True)
    return tuple(over(beside(p, q), beside(q, -p)) for p, q in parts)


def square_kernel(parity_ref, own_ref, other_ref, cov_ref, square_ref, stats_ref, mixed_ref):
    antennas, lanes = mixed_ref.shape[1], own_ref.shape[1]
    half = antennas // 2
    parity = parity_ref[0]
    for n in range(antennas // lanes):
        rows, columns = slice(n * half, (n + 1) * half), slice(n * lanes, (n + 1) * lanes)
        mixed_ref[pl.ds(pl.multiple_of(parity * half, half), half), columns] = own_ref[rows, :]
        mixed_ref[pl.ds(pl.multiple_of((1 - parity) * half, half), half), columns] = other_ref[rows, :]
    mixed = mixed_ref[...]
    flipped = mixed.T
    re, im = 0.5 * (mixed + flipped), 0.5 * (mixed - flipped)
    cov_ref[:antennas, :], cov_ref[antennas:, :] = re, im
    (rh, rl), (ih, il) = split(re), split(im)
    full = tuple(over(beside(r, -i), beside(i, r)) for r, i in ((rh, ih), (rl, il)))
    square_ref[...] = dot3(full, (over(rh, ih), over(rl, il)))
    row = lax.broadcasted_iota(jnp.int32, mixed.shape, 0)
    column = lax.broadcasted_iota(jnp.int32, mixed.shape, 1)
    trace = jnp.sum(jnp.where(row == column, mixed, 0.0), keepdims=True)
    norm = jnp.sum(mixed * mixed, keepdims=True)
    stats_ref[:8, :] = jnp.broadcast_to(norm, (8, stats_ref.shape[1]))
    stats_ref[8:, :] = jnp.broadcast_to(trace, (8, stats_ref.shape[1]))


def whiten_kernel(
    band_ref, stats_ref, cov_ref, square_ref, w_ref, high_ref, low_ref, out_ref, done_ref, sems
):
    samples = w_ref.shape[0]
    antennas = cov_ref.shape[1]
    size = samples // CHUNKS

    def wide(row):
        return jnp.concatenate([row] * (antennas // row.shape[1]), axis=1)

    norm, trace, band = wide(stats_ref[0:1, :]), wide(stats_ref[8:9, :]), wide(band_ref[0:1, :])
    beta = 1.0 / band
    total = 2.0 * (beta * (beta * norm + 2.0 * LOADING * trace) + LOADING * LOADING * antennas)
    omega = 1.0 / jnp.sqrt(total)
    slope, shift = omega * beta, omega * LOADING
    cov, square = cov_ref[...], square_ref[...]
    bend = (slope * slope) * square
    first = split(bend + (2.0 * slope * (shift - 1.0)) * cov)
    second = split((slope * (3.0 - 2.0 * shift)) * cov - bend)
    left, right = slice(0, antennas), slice(antennas, 2 * antennas)
    keep_first, keep_second = 2.0 + shift * (shift - 2.0), 2.0 - shift * (3.0 - shift)

    def begin(n):
        both = slice(2 * n * size, 2 * (n + 1) * size)
        return dot3((high_ref[both, :], low_ref[both, :]), first)

    steps = {n: begin(n) for n in range(4)}
    for n in range(CHUNKS):
        rows = slice(n * size, (n + 1) * size)
        step = steps.pop(n)
        w_u, w_v = w_ref[rows, left], w_ref[rows, right]
        u, v = keep_first * w_u + step[:size], keep_first * w_v + step[size:]
        step = dot3(turn(u, v), second)
        if n + 4 < CHUNKS:
            steps[n + 4] = begin(n + 4)
        done_ref[rows, left] = omega * (w_u + keep_second * u - step[:size])
        done_ref[rows, right] = omega * (w_v + keep_second * v - step[size:])
        pltpu.make_async_copy(done_ref.at[rows], out_ref.at[rows], sems.at[n]).start()
    for n in range(CHUNKS):
        rows = slice(n * size, (n + 1) * size)
        pltpu.make_async_copy(done_ref.at[rows], out_ref.at[rows], sems.at[n]).wait()


def complex_inverse(re, im):
    size = re.shape[0]
    row = lax.broadcasted_iota(jnp.int32, re.shape, 0)
    column = lax.broadcasted_iota(jnp.int32, re.shape, 1)
    for j in range(size):
        here = column[:1] == j
        col_re, col_im = re[:, j : j + 1], im[:, j : j + 1]
        scale = 1.0 / re[j : j + 1, j : j + 1]
        row_re = jnp.where(here, scale, re[j : j + 1] * scale)
        row_im = jnp.where(here, 0.0, im[j : j + 1] * scale)
        rest_re, rest_im = jnp.where(column == j, 0.0, re), jnp.where(column == j, 0.0, im)
        rest_re = rest_re - (col_re * row_re - col_im * row_im)
        rest_im = rest_im - (col_re * row_im + col_im * row_re)
        re = jnp.where(row == j, row_re, rest_re)
        im = jnp.where(row == j, row_im, rest_im)
    return re, im


def across(left, right):
    return lax.dot_general(
        left, right, (((1,), (1,)), ((), ())), precision=PRECISE, preferred_element_type=F32
    )


def null_kernel(picks_ref, angles_ref, volts_ref, out_ref, high_ref, low_ref):
    antennas = volts_ref.shape[1] // 2
    count = picks_ref.shape[1]
    row = lax.broadcasted_iota(jnp.int32, (count, 128), 0)
    angle = jnp.zeros((count, 128), F32)
    for k in range(count):
        angle = jnp.where(row == k, angles_ref[picks_ref[0, k]], angle)
    rate = (jnp.pi * jnp.sin(angle))[:, :1]
    position = lax.broadcasted_iota(jnp.int32, (count, antennas), 1).astype(F32)
    phase = rate * position
    norming = antennas**0.5
    re, im = jnp.cos(phase) / norming, jnp.sin(phase) / norming
    both = jnp.concatenate([re, im], axis=1)
    turned = jnp.concatenate([-im, re], axis=1)
    eye = lax.broadcasted_iota(jnp.int32, (count, count), 0) == lax.broadcasted_iota(
        jnp.int32, (count, count), 1
    )
    gram_re = across(both, both) + jnp.where(eye, STEER_LOADING, 0.0)
    gram_im = across(both, turned)
    inv_re, inv_im = complex_inverse(gram_re, gram_im)
    steer = jnp.concatenate([both, turned], axis=0)
    inverse = jnp.concatenate(
        [
            jnp.concatenate([inv_re, inv_im], axis=1),
            jnp.concatenate([-inv_im, inv_re], axis=1),
        ],
        axis=0,
    )
    back = jnp.dot(inverse, steer, precision=PRECISE, preferred_element_type=F32)
    volts = volts_ref[...]
    nt = (((1,), (1,)), ((), ()))
    inner = sum(
        lax.dot_general(volts, part, nt, preferred_element_type=F32) for part in split(steer)
    )
    nulled = volts.astype(F32) - dot3(split(inner), split(back))
    out_ref[...] = nulled
    size = volts.shape[0] // CHUNKS
    for n in range(CHUNKS):
        rows, both = slice(n * size, (n + 1) * size), slice(2 * n * size, 2 * (n + 1) * size)
        high, low = turn(nulled[rows, :antennas], nulled[rows, antennas:])
        high_ref[both, :], low_ref[both, :] = high, low


def exchange(value, axis, mask):
    return lax.ppermute(value, axis, [(i, i ^ mask) for i in range(lax.axis_size(axis))])


def choose(index, values):
    chosen = jnp.asarray(values[0], F32)
    for i, value in enumerate(values[1:], 1):
        chosen = jnp.where(index == i, value, chosen)
    return chosen


def earlier_chips(value, decay, mirrored=False, rider=None):
    chips = lax.axis_size("tm") // 2
    chip = lax.axis_index("tm") // 2
    length, total, before = 1, value, None
    while length < chips:
        last = 2 * length == chips
        mask = 2 * length - 1 if mirrored else length
        rows = total.shape[0]
        if last and rider is not None:
            total = jnp.concatenate([total, rider], axis=0)
        got = exchange(total, "tm", 2 * mask)
        if last and rider is not None:
            got, rider = got[:rows], got[rows:]
        upper = (chip // length) % 2 == 1
        weight = jnp.where(upper, choose(chip % length, [decay**i for i in range(length)]), 0.0)
        before = weight * got if before is None else before + weight * got
        if not last:
            far = decay**length
            total = jnp.where(upper, 1.0, far) * total + jnp.where(upper, far, 1.0) * got
        length *= 2
    before = jnp.zeros_like(value) if before is None else before
    return before if rider is None else (before, rider)


def earlier_levels(level, opposite, decay):
    chips = lax.axis_size("tm") // 2
    chip = lax.axis_index("tm") // 2
    near, far = jnp.zeros_like(level), None
    for mask in range(1, chips):
        weights = [decay ** (c - 1 - (c ^ mask)) if c ^ mask < c else 0.0 for c in range(chips)]
        if mask == chips - 1:
            far = choose(chip, weights) * opposite
        else:
            near = near + choose(chip, weights) * exchange(level, "tm", 2 * mask)
    return near + far


def sum_groups(value):
    groups = lax.axis_size("chan")
    if groups & (groups - 1):
        return lax.psum(value, "chan")
    step = 1
    while step < groups:
        got = exchange(value, "chan", step)
        value = value + got
        step *= 2
    return value


def steps(volts, picks, angles):
    voltage = volts[0]
    rows, width = voltage.shape
    antennas = width // 2
    half = antennas // 2
    segments = rows // SEG
    core = lax.axis_index("tm") % 2
    parity = core.reshape(1).astype(jnp.int32)
    is_odd = core == 1
    decay = (1.0 - 1.0 / HORIZON) ** segments

    keep, give, power = pl.pallas_call(
        gram_kernel,
        out_shape=(
            jax.ShapeDtypeStruct((half * antennas // LANES, LANES), F32),
            jax.ShapeDtypeStruct((half * antennas // LANES, LANES), F32),
            jax.ShapeDtypeStruct((8, LANES), F32),
        ),
        in_specs=[SM, VM],
        out_specs=(VM, VM, VM),
        scratch_shapes=[pltpu.VMEM((antennas, antennas), F32)],
        cost_estimate=pl.CostEstimate(
            flops=4 * rows * width * antennas, bytes_accessed=rows * width * 2, transcendentals=0
        ),
        compiler_params=PARAMS,
        name="segment_gram",
    )(parity, voltage)

    got = exchange(give, "tm", 1)
    mine, theirs = jnp.where(is_odd, 1.0, decay), jnp.where(is_odd, decay, 1.0)
    pair = mine * keep + theirs * got
    tall = keep.shape[0]
    level = sum_groups(power)
    direct = lax.axis_size("tm") // 2 == DIRECT
    opposite = None
    if direct:
        before, opposite = earlier_chips(pair, decay * decay, True, level)
    else:
        before = earlier_chips(pair, decay * decay, True)
    even_cov = decay * before + jnp.where(is_odd, got, keep)
    odd_cov = decay * decay * before + pair
    own = jnp.where(is_odd, odd_cov, even_cov)
    other = jnp.where(is_odd, even_cov, odd_cov)
    if direct:
        other = jnp.concatenate([other, opposite], axis=0)
    other = exchange(other, "tm", 1)

    def parities(mine, theirs):
        return jnp.where(is_odd, theirs, mine), jnp.where(is_odd, mine, theirs)

    level_even, level_odd = parities(level, exchange(level, "tm", 1))
    chip_level = decay * level_even + level_odd
    if direct:
        even, odd = parities(opposite, other[tall:])
        level_before = earlier_levels(chip_level, decay * even + odd, decay * decay)
    else:
        level_before = earlier_chips(chip_level, decay * decay)
    level_own = decay * level_before + level_even
    level_own = jnp.where(is_odd, decay * level_own + level_odd, level_own)
    band = level_own / lax.axis_size("chan") + TINY_LEVEL

    projected, high, low = pl.pallas_call(
        null_kernel,
        out_shape=(
            jax.ShapeDtypeStruct((rows, width), F32),
            jax.ShapeDtypeStruct((2 * rows, width), BF16),
            jax.ShapeDtypeStruct((2 * rows, width), BF16),
        ),
        in_specs=[SM, SM, VM],
        out_specs=(VM, VM, VM),
        cost_estimate=pl.CostEstimate(
            flops=4 * rows * width * 128, bytes_accessed=rows * width * 6, transcendentals=0
        ),
        compiler_params=PARAMS,
        name="null",
    )(picks, angles, voltage)

    cov, square, stats = pl.pallas_call(
        square_kernel,
        out_shape=(
            jax.ShapeDtypeStruct((width, antennas), F32),
            jax.ShapeDtypeStruct((width, antennas), F32),
            jax.ShapeDtypeStruct((16, 128), F32),
        ),
        in_specs=[SM, VM, VM],
        out_specs=(VM, VM, VM),
        scratch_shapes=[pltpu.VMEM((antennas, antennas), F32)],
        cost_estimate=pl.CostEstimate(
            flops=6 * width * width * antennas, bytes_accessed=width * antennas * 8, transcendentals=0
        ),
        compiler_params=PARAMS,
        name="square",
    )(parity, own, other)

    cleaned = pl.pallas_call(
        whiten_kernel,
        out_shape=jax.ShapeDtypeStruct((rows, width), F32),
        in_specs=[VM] * 7,
        out_specs=pl.BlockSpec(memory_space=pl.ANY),
        scratch_shapes=[pltpu.VMEM((rows, width), F32), pltpu.SemaphoreType.DMA((CHUNKS,))],
        cost_estimate=pl.CostEstimate(
            flops=12 * rows * width * width, bytes_accessed=rows * width * 8, transcendentals=0
        ),
        compiler_params=PARAMS,
        name="whiten",
    )(band, stats, cov, square, projected, high, low)
    return cleaned[None]


def solution(mesh):
    placed = (P("chan", "tm", None), P("chan", None), P())
    return jax.shard_map(
        steps, mesh=mesh, in_specs=placed, out_specs=P("chan", "tm", None), check_vma=False
    )
```

```python
import jax
import jax.numpy as jnp
from jax import lax
from jax.experimental import pallas as pl
from jax.experimental.pallas import tpu as pltpu
from jax.sharding import PartitionSpec as P


SEG = 256
HORIZON = 256
LANES = 128
CHUNKS = 4
DIRECT = 4
LOADING = 0.1
STEER_LOADING = 0.05
TINY_LEVEL = 1e-06
PRECISE = lax.Precision.HIGHEST
F32 = jnp.float32
BF16 = jnp.bfloat16
VM = pl.BlockSpec(memory_space=pltpu.VMEM)
SM = pl.BlockSpec(memory_space=pltpu.SMEM)
PARAMS = pltpu.CompilerParams(vmem_limit_bytes=24 * 2**20)


def gram_kernel(parity_ref, volts_ref, keep_ref, give_ref, power_ref, mixed_ref):
    antennas = volts_ref.shape[1] // 2
    segments = volts_ref.shape[0] // SEG
    half = antennas // 2
    forget = 1.0 - 1.0 / HORIZON
    mixed = power = None
    for seg in range(segments):
        a = volts_ref[seg * SEG : (seg + 1) * SEG, :antennas]
        b = volts_ref[seg * SEG : (seg + 1) * SEG, antennas:]
        a_t, b_t = a.T, b.T
        left = jnp.concatenate([a_t, b_t, b_t, -a_t], axis=1)
        right = jnp.concatenate([a, b, a, b], axis=0)
        term = jnp.dot(left, right, preferred_element_type=F32)
        mixed = term if mixed is None else forget * mixed + term
        squares = a.astype(F32) ** 2 + b.astype(F32) ** 2
        squares = jnp.sum(squares.reshape(-1, 8, antennas), axis=0)
        power = squares if power is None else forget * power + squares
    mixed_ref[...] = mixed
    power_ref[...] = jnp.broadcast_to(jnp.sum(power, keepdims=True) / antennas, power_ref.shape)
    parity = parity_ref[0]
    lanes = keep_ref.shape[1]
    for n in range(antennas // lanes):
        rows, columns = slice(n * half, (n + 1) * half), slice(n * lanes, (n + 1) * lanes)
        keep_ref[rows, :] = mixed_ref[pl.ds(pl.multiple_of(parity * half, half), half), columns]
        give_ref[rows, :] = mixed_ref[pl.ds(pl.multiple_of((1 - parity) * half, half), half), columns]


def split(value):
    high = value.astype(BF16)
    return high, (value - high.astype(F32)).astype(BF16)


def dot3(left, right):
    (lh, ll), (rh, rl) = left, right
    return (
        jnp.dot(lh, rh, preferred_element_type=F32)
        + jnp.dot(lh, rl, preferred_element_type=F32)
        + jnp.dot(ll, rh, preferred_element_type=F32)
    )


def beside(first, second):
    return jnp.concatenate([first, second], axis=1)


def over(first, second):
    return jnp.concatenate([first, second], axis=0)


def turn(u, v):
    parts = zip(split(u), split(v), strict=True)
    return tuple(over(beside(p, q), beside(q, -p)) for p, q in parts)


def square_kernel(parity_ref, own_ref, other_ref, cov_ref, square_ref, stats_ref, mixed_ref):
    antennas, lanes = mixed_ref.shape[1], own_ref.shape[1]
    half = antennas // 2
    parity = parity_ref[0]
    for n in range(antennas // lanes):
        rows, columns = slice(n * half, (n + 1) * half), slice(n * lanes, (n + 1) * lanes)
        mixed_ref[pl.ds(pl.multiple_of(parity * half, half), half), columns] = own_ref[rows, :]
        mixed_ref[pl.ds(pl.multiple_of((1 - parity) * half, half), half), columns] = other_ref[rows, :]
    mixed = mixed_ref[...]
    flipped = mixed.T
    re, im = 0.5 * (mixed + flipped), 0.5 * (mixed - flipped)
    cov_ref[:antennas, :], cov_ref[antennas:, :] = re, im
    (rh, rl), (ih, il) = split(re), split(im)
    (sh, sl), (fh, fl) = split(mixed), split(flipped)
    product = dot3((beside(sh, fh), beside(sl, fl)), (over(rh, ih), over(rl, il)))
    turned = product.T
    square_ref[:antennas, :], square_ref[antennas:, :] = 0.5 * (product + turned), 0.5 * (product - turned)
    row = lax.broadcasted_iota(jnp.int32, mixed.shape, 0)
    column = lax.broadcasted_iota(jnp.int32, mixed.shape, 1)
    trace = jnp.sum(jnp.where(row == column, mixed, 0.0), keepdims=True)
    norm = jnp.sum(mixed * mixed, keepdims=True)
    stats_ref[:8, :] = jnp.broadcast_to(norm, (8, stats_ref.shape[1]))
    stats_ref[8:, :] = jnp.broadcast_to(trace, (8, stats_ref.shape[1]))


def whiten_kernel(
    band_ref, stats_ref, cov_ref, square_ref, w_ref, high_ref, low_ref, out_ref, done_ref, sems
):
    samples = w_ref.shape[0]
    antennas = cov_ref.shape[1]
    size = samples // CHUNKS

    def wide(row):
        return jnp.concatenate([row] * (antennas // row.shape[1]), axis=1)

    norm, trace, band = wide(stats_ref[0:1, :]), wide(stats_ref[8:9, :]), wide(band_ref[0:1, :])
    beta = 1.0 / band
    total = 2.0 * (beta * (beta * norm + 2.0 * LOADING * trace) + LOADING * LOADING * antennas)
    omega = 1.0 / jnp.sqrt(total)
    slope, shift = omega * beta, omega * LOADING
    cov, square = cov_ref[...], square_ref[...]
    bend = (slope * slope) * square
    first = split(bend + (2.0 * slope * (shift - 1.0)) * cov)
    second = split((slope * (3.0 - 2.0 * shift)) * cov - bend)
    left, right = slice(0, antennas), slice(antennas, 2 * antennas)
    keep_first, keep_second = 2.0 + shift * (shift - 2.0), 2.0 - shift * (3.0 - shift)

    def begin(n):
        both = slice(2 * n * size, 2 * (n + 1) * size)
        return dot3((high_ref[both, :], low_ref[both, :]), first)

    steps = {n: begin(n) for n in range(4)}
    for n in range(CHUNKS):
        rows = slice(n * size, (n + 1) * size)
        step = steps.pop(n)
        w_u, w_v = w_ref[rows, left], w_ref[rows, right]
        u, v = keep_first * w_u + step[:size], keep_first * w_v + step[size:]
        step = dot3(turn(u, v), second)
        if n + 4 < CHUNKS:
            steps[n + 4] = begin(n + 4)
        done_ref[rows, left] = omega * (w_u + keep_second * u - step[:size])
        done_ref[rows, right] = omega * (w_v + keep_second * v - step[size:])
        pltpu.make_async_copy(done_ref.at[rows], out_ref.at[rows], sems.at[n]).start()
    for n in range(CHUNKS):
        rows = slice(n * size, (n + 1) * size)
        pltpu.make_async_copy(done_ref.at[rows], out_ref.at[rows], sems.at[n]).wait()


def complex_inverse(re, im):
    size = re.shape[0]
    row = lax.broadcasted_iota(jnp.int32, re.shape, 0)
    column = lax.broadcasted_iota(jnp.int32, re.shape, 1)
    for j in range(size):
        here = column[:1] == j
        col_re, col_im = re[:, j : j + 1], im[:, j : j + 1]
        scale = 1.0 / re[j : j + 1, j : j + 1]
        row_re = jnp.where(here, scale, re[j : j + 1] * scale)
        row_im = jnp.where(here, 0.0, im[j : j + 1] * scale)
        rest_re, rest_im = jnp.where(column == j, 0.0, re), jnp.where(column == j, 0.0, im)
        rest_re = rest_re - (col_re * row_re - col_im * row_im)
        rest_im = rest_im - (col_re * row_im + col_im * row_re)
        re = jnp.where(row == j, row_re, rest_re)
        im = jnp.where(row == j, row_im, rest_im)
    return re, im


def across(left, right):
    return lax.dot_general(
        left, right, (((1,), (1,)), ((), ())), precision=PRECISE, preferred_element_type=F32
    )


def null_kernel(picks_ref, angles_ref, volts_ref, out_ref, high_ref, low_ref):
    antennas = volts_ref.shape[1] // 2
    count = picks_ref.shape[1]
    row = lax.broadcasted_iota(jnp.int32, (count, 128), 0)
    angle = jnp.zeros((count, 128), F32)
    for k in range(count):
        angle = jnp.where(row == k, angles_ref[picks_ref[0, k]], angle)
    rate = (jnp.pi * jnp.sin(angle))[:, :1]
    position = lax.broadcasted_iota(jnp.int32, (count, antennas), 1).astype(F32)
    phase = rate * position
    norming = antennas**0.5
    re, im = jnp.cos(phase) / norming, jnp.sin(phase) / norming
    both = jnp.concatenate([re, im], axis=1)
    turned = jnp.concatenate([-im, re], axis=1)
    eye = lax.broadcasted_iota(jnp.int32, (count, count), 0) == lax.broadcasted_iota(
        jnp.int32, (count, count), 1
    )
    gram_re = across(both, both) + jnp.where(eye, STEER_LOADING, 0.0)
    gram_im = across(both, turned)
    inv_re, inv_im = complex_inverse(gram_re, gram_im)
    steer = jnp.concatenate([both, turned], axis=0)
    inverse = jnp.concatenate(
        [
            jnp.concatenate([inv_re, inv_im], axis=1),
            jnp.concatenate([-inv_im, inv_re], axis=1),
        ],
        axis=0,
    )
    back = jnp.dot(inverse, steer, precision=PRECISE, preferred_element_type=F32)
    volts = volts_ref[...]
    nt = (((1,), (1,)), ((), ()))
    inner = sum(
        lax.dot_general(volts, part, nt, preferred_element_type=F32) for part in split(steer)
    )
    nulled = volts.astype(F32) - dot3(split(inner), split(back))
    out_ref[...] = nulled
    size = volts.shape[0] // CHUNKS
    for n in range(CHUNKS):
        rows, both = slice(n * size, (n + 1) * size), slice(2 * n * size, 2 * (n + 1) * size)
        high, low = turn(nulled[rows, :antennas], nulled[rows, antennas:])
        high_ref[both, :], low_ref[both, :] = high, low


def exchange(value, axis, mask):
    return lax.ppermute(value, axis, [(i, i ^ mask) for i in range(lax.axis_size(axis))])


def choose(index, values):
    chosen = jnp.asarray(values[0], F32)
    for i, value in enumerate(values[1:], 1):
        chosen = jnp.where(index == i, value, chosen)
    return chosen


def earlier_chips(value, decay, mirrored=False, rider=None):
    chips = lax.axis_size("tm") // 2
    chip = lax.axis_index("tm") // 2
    length, total, before = 1, value, None
    while length < chips:
        last = 2 * length == chips
        mask = 2 * length - 1 if mirrored else length
        rows = total.shape[0]
        if last and rider is not None:
            total = jnp.concatenate([total, rider], axis=0)
        got = exchange(total, "tm", 2 * mask)
        if last and rider is not None:
            got, rider = got[:rows], got[rows:]
        upper = (chip // length) % 2 == 1
        weight = jnp.where(upper, choose(chip % length, [decay**i for i in range(length)]), 0.0)
        before = weight * got if before is None else before + weight * got
        if not last:
            far = decay**length
            total = jnp.where(upper, 1.0, far) * total + jnp.where(upper, far, 1.0) * got
        length *= 2
    before = jnp.zeros_like(value) if before is None else before
    return before if rider is None else (before, rider)


def earlier_levels(level, opposite, decay):
    chips = lax.axis_size("tm") // 2
    chip = lax.axis_index("tm") // 2
    near, far = jnp.zeros_like(level), None
    for mask in range(1, chips):
        weights = [decay ** (c - 1 - (c ^ mask)) if c ^ mask < c else 0.0 for c in range(chips)]
        if mask == chips - 1:
            far = choose(chip, weights) * opposite
        else:
            near = near + choose(chip, weights) * exchange(level, "tm", 2 * mask)
    return near + far


def sum_groups(value):
    groups = lax.axis_size("chan")
    if groups & (groups - 1):
        return lax.psum(value, "chan")
    step = 1
    while step < groups:
        got = exchange(value, "chan", step)
        value = value + got
        step *= 2
    return value


def steps(volts, picks, angles):
    voltage = volts[0]
    rows, width = voltage.shape
    antennas = width // 2
    half = antennas // 2
    segments = rows // SEG
    core = lax.axis_index("tm") % 2
    parity = core.reshape(1).astype(jnp.int32)
    is_odd = core == 1
    decay = (1.0 - 1.0 / HORIZON) ** segments

    keep, give, power = pl.pallas_call(
        gram_kernel,
        out_shape=(
            jax.ShapeDtypeStruct((half * antennas // LANES, LANES), F32),
            jax.ShapeDtypeStruct((half * antennas // LANES, LANES), F32),
            jax.ShapeDtypeStruct((8, LANES), F32),
        ),
        in_specs=[SM, VM],
        out_specs=(VM, VM, VM),
        scratch_shapes=[pltpu.VMEM((antennas, antennas), F32)],
        cost_estimate=pl.CostEstimate(
            flops=4 * rows * width * antennas, bytes_accessed=rows * width * 2, transcendentals=0
        ),
        compiler_params=PARAMS,
        name="segment_gram",
    )(parity, voltage)

    got = exchange(give, "tm", 1)
    mine, theirs = jnp.where(is_odd, 1.0, decay), jnp.where(is_odd, decay, 1.0)
    pair = mine * keep + theirs * got
    tall = keep.shape[0]
    level = sum_groups(power)
    direct = lax.axis_size("tm") // 2 == DIRECT
    opposite = None
    if direct:
        before, opposite = earlier_chips(pair, decay * decay, True, level)
    else:
        before = earlier_chips(pair, decay * decay, True)
    even_cov = decay * before + jnp.where(is_odd, got, keep)
    odd_cov = decay * decay * before + pair
    own = jnp.where(is_odd, odd_cov, even_cov)
    other = jnp.where(is_odd, even_cov, odd_cov)
    if direct:
        other = jnp.concatenate([other, opposite], axis=0)
    other = exchange(other, "tm", 1)

    def parities(mine, theirs):
        return jnp.where(is_odd, theirs, mine), jnp.where(is_odd, mine, theirs)

    level_even, level_odd = parities(level, exchange(level, "tm", 1))
    chip_level = decay * level_even + level_odd
    if direct:
        even, odd = parities(opposite, other[tall:])
        level_before = earlier_levels(chip_level, decay * even + odd, decay * decay)
    else:
        level_before = earlier_chips(chip_level, decay * decay)
    level_own = decay * level_before + level_even
    level_own = jnp.where(is_odd, decay * level_own + level_odd, level_own)
    band = level_own / lax.axis_size("chan") + TINY_LEVEL

    projected, high, low = pl.pallas_call(
        null_kernel,
        out_shape=(
            jax.ShapeDtypeStruct((rows, width), F32),
            jax.ShapeDtypeStruct((2 * rows, width), BF16),
            jax.ShapeDtypeStruct((2 * rows, width), BF16),
        ),
        in_specs=[SM, SM, VM],
        out_specs=(VM, VM, VM),
        cost_estimate=pl.CostEstimate(
            flops=4 * rows * width * 128, bytes_accessed=rows * width * 6, transcendentals=0
        ),
        compiler_params=PARAMS,
        name="null",
    )(picks, angles, voltage)

    cov, square, stats = pl.pallas_call(
        square_kernel,
        out_shape=(
            jax.ShapeDtypeStruct((width, antennas), F32),
            jax.ShapeDtypeStruct((width, antennas), F32),
            jax.ShapeDtypeStruct((16, 128), F32),
        ),
        in_specs=[SM, VM, VM],
        out_specs=(VM, VM, VM),
        scratch_shapes=[pltpu.VMEM((antennas, antennas), F32)],
        cost_estimate=pl.CostEstimate(
            flops=6 * width * width * antennas, bytes_accessed=width * antennas * 8, transcendentals=0
        ),
        compiler_params=PARAMS,
        name="square",
    )(parity, own, other)

    cleaned = pl.pallas_call(
        whiten_kernel,
        out_shape=jax.ShapeDtypeStruct((rows, width), F32),
        in_specs=[VM] * 7,
        out_specs=pl.BlockSpec(memory_space=pl.ANY),
        scratch_shapes=[pltpu.VMEM((rows, width), F32), pltpu.SemaphoreType.DMA((CHUNKS,))],
        cost_estimate=pl.CostEstimate(
            flops=12 * rows * width * width, bytes_accessed=rows * width * 8, transcendentals=0
        ),
        compiler_params=PARAMS,
        name="whiten",
    )(band, stats, cov, square, projected, high, low)
    return cleaned[None]


def solution(mesh):
    placed = (P("chan", "tm", None), P("chan", None), P())
    return jax.shard_map(steps, mesh=mesh, in_specs=placed, out_specs=P("chan", "tm", None), check_vma=False)
```

```python
import jax
import jax.numpy as jnp
from jax import lax
from jax.experimental import pallas as pl
from jax.experimental.pallas import tpu as pltpu
from jax.sharding import PartitionSpec as P


SEG = 256
HORIZON = 256
LANES = 128
CHUNKS = 4
DIRECT = 4
LOADING = 0.1
STEER_LOADING = 0.05
TINY_LEVEL = 1e-06
PRECISE = lax.Precision.HIGHEST
F32 = jnp.float32
BF16 = jnp.bfloat16
VM = pl.BlockSpec(memory_space=pltpu.VMEM)
SM = pl.BlockSpec(memory_space=pltpu.SMEM)
PARAMS = pltpu.CompilerParams(vmem_limit_bytes=24 * 2**20)


def gram_kernel(parity_ref, volts_ref, keep_ref, give_ref, power_ref):
    antennas = volts_ref.shape[1] // 2
    segments = volts_ref.shape[0] // SEG
    half = antennas // 2
    forget = 1.0 - 1.0 / HORIZON
    mixed = power = None
    for seg in range(segments):
        a = volts_ref[seg * SEG : (seg + 1) * SEG, :antennas]
        b = volts_ref[seg * SEG : (seg + 1) * SEG, antennas:]
        a_t, b_t = a.T, b.T
        left = jnp.concatenate([a_t, b_t, b_t, -a_t], axis=1)
        right = jnp.concatenate([a, b, a, b], axis=0)
        term = jnp.dot(left, right, preferred_element_type=F32)
        mixed = term if mixed is None else forget * mixed + term
        squares = a.astype(F32) ** 2 + b.astype(F32) ** 2
        squares = jnp.sum(squares.reshape(-1, 8, antennas), axis=0)
        power = squares if power is None else forget * power + squares
    power_ref[...] = jnp.broadcast_to(jnp.sum(power, keepdims=True) / antennas, power_ref.shape)
    is_odd = parity_ref[0] == 1
    lanes = keep_ref.shape[1]
    for n in range(antennas // lanes):
        rows, columns = slice(n * half, (n + 1) * half), slice(n * lanes, (n + 1) * lanes)
        upper, lower = mixed[:half, columns], mixed[half:, columns]
        keep_ref[rows, :] = jnp.where(is_odd, lower, upper)
        give_ref[rows, :] = jnp.where(is_odd, upper, lower)


def split(value):
    high = value.astype(BF16)
    return high, (value - high.astype(F32)).astype(BF16)


def dot3(left, right):
    (lh, ll), (rh, rl) = left, right
    return (
        jnp.dot(lh, rh, preferred_element_type=F32)
        + jnp.dot(lh, rl, preferred_element_type=F32)
        + jnp.dot(ll, rh, preferred_element_type=F32)
    )


def beside(first, second):
    return jnp.concatenate([first, second], axis=1)


def over(first, second):
    return jnp.concatenate([first, second], axis=0)


def turn(u, v):
    parts = zip(split(u), split(v), strict=True)
    return tuple(over(beside(p, q), beside(q, -p)) for p, q in parts)


def square_kernel(parity_ref, own_ref, other_ref, cov_ref, square_ref, stats_ref):
    antennas, lanes = cov_ref.shape[1], own_ref.shape[1]
    half = antennas // 2
    is_odd = parity_ref[0] == 1
    blocks = [slice(n * half, (n + 1) * half) for n in range(antennas // lanes)]
    mixed = over(
        jnp.concatenate([jnp.where(is_odd, other_ref[b, :], own_ref[b, :]) for b in blocks], axis=1),
        jnp.concatenate([jnp.where(is_odd, own_ref[b, :], other_ref[b, :]) for b in blocks], axis=1),
    )
    flipped = mixed.T
    re, im = 0.5 * (mixed + flipped), 0.5 * (mixed - flipped)
    cov_ref[:antennas, :], cov_ref[antennas:, :] = re, im
    (rh, rl), (ih, il) = split(re), split(im)
    (sh, sl), (fh, fl) = split(mixed), split(flipped)
    product = dot3((beside(sh, fh), beside(sl, fl)), (over(rh, ih), over(rl, il)))
    turned = product.T
    square_ref[:antennas, :], square_ref[antennas:, :] = 0.5 * (product + turned), 0.5 * (product - turned)
    row = lax.broadcasted_iota(jnp.int32, mixed.shape, 0)
    column = lax.broadcasted_iota(jnp.int32, mixed.shape, 1)
    trace = jnp.sum(jnp.where(row == column, mixed, 0.0), keepdims=True)
    norm = jnp.sum(mixed * mixed, keepdims=True)
    stats_ref[:8, :] = jnp.broadcast_to(norm, (8, stats_ref.shape[1]))
    stats_ref[8:, :] = jnp.broadcast_to(trace, (8, stats_ref.shape[1]))


def whiten_kernel(
    band_ref, stats_ref, cov_ref, square_ref, w_ref, high_ref, low_ref, out_ref, done_ref, sems
):
    samples = w_ref.shape[0]
    antennas = cov_ref.shape[1]
    size = samples // CHUNKS

    def wide(row):
        return jnp.concatenate([row] * (antennas // row.shape[1]), axis=1)

    norm, trace, band = wide(stats_ref[0:1, :]), wide(stats_ref[8:9, :]), wide(band_ref[0:1, :])
    beta = 1.0 / band
    total = 2.0 * (beta * (beta * norm + 2.0 * LOADING * trace) + LOADING * LOADING * antennas)
    omega = 1.0 / jnp.sqrt(total)
    slope, shift = omega * beta, omega * LOADING
    cov, square = cov_ref[...], square_ref[...]
    bend = (slope * slope) * square
    first = split(bend + (2.0 * slope * (shift - 1.0)) * cov)
    second = split((slope * (3.0 - 2.0 * shift)) * cov - bend)
    left, right = slice(0, antennas), slice(antennas, 2 * antennas)
    keep_first, keep_second = 2.0 + shift * (shift - 2.0), 2.0 - shift * (3.0 - shift)

    def begin(n):
        both = slice(2 * n * size, 2 * (n + 1) * size)
        return dot3((high_ref[both, :], low_ref[both, :]), first)

    steps = [begin(n) for n in range(CHUNKS)]
    for n, step in enumerate(steps):
        rows = slice(n * size, (n + 1) * size)
        w_u, w_v = w_ref[rows, left], w_ref[rows, right]
        u, v = keep_first * w_u + step[:size], keep_first * w_v + step[size:]
        step = dot3(turn(u, v), second)
        done_ref[rows, left] = omega * (w_u + keep_second * u - step[:size])
        done_ref[rows, right] = omega * (w_v + keep_second * v - step[size:])
        pltpu.make_async_copy(done_ref.at[rows], out_ref.at[rows], sems.at[n]).start()
    for n in range(CHUNKS):
        rows = slice(n * size, (n + 1) * size)
        pltpu.make_async_copy(done_ref.at[rows], out_ref.at[rows], sems.at[n]).wait()


def complex_inverse(re, im):
    size = re.shape[0]
    row = lax.broadcasted_iota(jnp.int32, re.shape, 0)
    column = lax.broadcasted_iota(jnp.int32, re.shape, 1)
    for j in range(size):
        here = column[:1] == j
        col_re, col_im = re[:, j : j + 1], im[:, j : j + 1]
        scale = 1.0 / re[j : j + 1, j : j + 1]
        row_re = jnp.where(here, scale, re[j : j + 1] * scale)
        row_im = jnp.where(here, 0.0, im[j : j + 1] * scale)
        rest_re, rest_im = jnp.where(column == j, 0.0, re), jnp.where(column == j, 0.0, im)
        rest_re = rest_re - (col_re * row_re - col_im * row_im)
        rest_im = rest_im - (col_re * row_im + col_im * row_re)
        re = jnp.where(row == j, row_re, rest_re)
        im = jnp.where(row == j, row_im, rest_im)
    return re, im


def across(left, right):
    return lax.dot_general(
        left, right, (((1,), (1,)), ((), ())), precision=PRECISE, preferred_element_type=F32
    )


def null_kernel(picks_ref, angles_ref, volts_ref, out_ref, high_ref, low_ref):
    antennas = volts_ref.shape[1] // 2
    count = picks_ref.shape[1]
    row = lax.broadcasted_iota(jnp.int32, (count, 128), 0)
    angle = jnp.zeros((count, 128), F32)
    for k in range(count):
        angle = jnp.where(row == k, angles_ref[picks_ref[0, k]], angle)
    rate = (jnp.pi * jnp.sin(angle))[:, :1]
    position = lax.broadcasted_iota(jnp.int32, (count, antennas), 1).astype(F32)
    phase = rate * position
    norming = antennas**0.5
    re, im = jnp.cos(phase) / norming, jnp.sin(phase) / norming
    both = jnp.concatenate([re, im], axis=1)
    turned = jnp.concatenate([-im, re], axis=1)
    eye = lax.broadcasted_iota(jnp.int32, (count, count), 0) == lax.broadcasted_iota(
        jnp.int32, (count, count), 1
    )
    gram_re = across(both, both) + jnp.where(eye, STEER_LOADING, 0.0)
    gram_im = across(both, turned)
    inv_re, inv_im = complex_inverse(gram_re, gram_im)
    steer = jnp.concatenate([both, turned], axis=0)
    inverse = jnp.concatenate(
        [
            jnp.concatenate([inv_re, inv_im], axis=1),
            jnp.concatenate([-inv_im, inv_re], axis=1),
        ],
        axis=0,
    )
    back = jnp.dot(inverse, steer, precision=PRECISE, preferred_element_type=F32)
    volts = volts_ref[...]
    nt = (((1,), (1,)), ((), ()))
    inner = sum(
        lax.dot_general(volts, part, nt, preferred_element_type=F32) for part in split(steer)
    )
    nulled = volts.astype(F32) - dot3(split(inner), split(back))
    out_ref[...] = nulled
    size = volts.shape[0] // CHUNKS
    for n in range(CHUNKS):
        rows, both = slice(n * size, (n + 1) * size), slice(2 * n * size, 2 * (n + 1) * size)
        high, low = turn(nulled[rows, :antennas], nulled[rows, antennas:])
        high_ref[both, :], low_ref[both, :] = high, low


def exchange(value, axis, mask):
    return lax.ppermute(value, axis, [(i, i ^ mask) for i in range(lax.axis_size(axis))])


def choose(index, values):
    chosen = jnp.asarray(values[0], F32)
    for i, value in enumerate(values[1:], 1):
        chosen = jnp.where(index == i, value, chosen)
    return chosen


def earlier_chips(value, decay, mirrored=False, rider=None):
    chips = lax.axis_size("tm") // 2
    chip = lax.axis_index("tm") // 2
    length, total, before = 1, value, None
    while length < chips:
        last = 2 * length == chips
        mask = 2 * length - 1 if mirrored else length
        rows = total.shape[0]
        if last and rider is not None:
            total = jnp.concatenate([total, rider], axis=0)
        got = exchange(total, "tm", 2 * mask)
        if last and rider is not None:
            got, rider = got[:rows], got[rows:]
        upper = (chip // length) % 2 == 1
        weight = jnp.where(upper, choose(chip % length, [decay**i for i in range(length)]), 0.0)
        before = weight * got if before is None else before + weight * got
        if not last:
            far = decay**length
            total = jnp.where(upper, 1.0, far) * total + jnp.where(upper, far, 1.0) * got
        length *= 2
    before = jnp.zeros_like(value) if before is None else before
    return before if rider is None else (before, rider)


def earlier_levels(level, opposite, decay):
    chips = lax.axis_size("tm") // 2
    chip = lax.axis_index("tm") // 2
    near, far = jnp.zeros_like(level), None
    for mask in range(1, chips):
        weights = [decay ** (c - 1 - (c ^ mask)) if c ^ mask < c else 0.0 for c in range(chips)]
        if mask == chips - 1:
            far = choose(chip, weights) * opposite
        else:
            near = near + choose(chip, weights) * exchange(level, "tm", 2 * mask)
    return near + far


def sum_groups(value):
    groups = lax.axis_size("chan")
    if groups & (groups - 1):
        return lax.psum(value, "chan")
    step = 1
    while step < groups:
        got = exchange(value, "chan", step)
        value = value + got
        step *= 2
    return value


def steps(volts, picks, angles):
    voltage = volts[0]
    rows, width = voltage.shape
    antennas = width // 2
    half = antennas // 2
    segments = rows // SEG
    core = lax.axis_index("tm") % 2
    parity = core.reshape(1).astype(jnp.int32)
    is_odd = core == 1
    decay = (1.0 - 1.0 / HORIZON) ** segments

    keep, give, power = pl.pallas_call(
        gram_kernel,
        out_shape=(
            jax.ShapeDtypeStruct((half * antennas // LANES, LANES), F32),
            jax.ShapeDtypeStruct((half * antennas // LANES, LANES), F32),
            jax.ShapeDtypeStruct((8, LANES), F32),
        ),
        in_specs=[SM, VM],
        out_specs=(VM, VM, VM),
        cost_estimate=pl.CostEstimate(
            flops=4 * rows * width * antennas, bytes_accessed=rows * width * 2, transcendentals=0
        ),
        compiler_params=PARAMS,
        name="segment_gram",
    )(parity, voltage)

    got = exchange(give, "tm", 1)
    mine, theirs = jnp.where(is_odd, 1.0, decay), jnp.where(is_odd, decay, 1.0)
    pair = mine * keep + theirs * got
    tall = keep.shape[0]
    level = sum_groups(power)
    direct = lax.axis_size("tm") // 2 == DIRECT
    opposite = None
    if direct:
        before, opposite = earlier_chips(pair, decay * decay, True, level)
    else:
        before = earlier_chips(pair, decay * decay, True)
    even_cov = decay * before + jnp.where(is_odd, got, keep)
    odd_cov = decay * decay * before + pair
    own = jnp.where(is_odd, odd_cov, even_cov)
    other = jnp.where(is_odd, even_cov, odd_cov)
    if direct:
        other = jnp.concatenate([other, opposite], axis=0)
    other = exchange(other, "tm", 1)

    def parities(mine, theirs):
        return jnp.where(is_odd, theirs, mine), jnp.where(is_odd, mine, theirs)

    level_even, level_odd = parities(level, exchange(level, "tm", 1))
    chip_level = decay * level_even + level_odd
    if direct:
        even, odd = parities(opposite, other[tall:])
        level_before = earlier_levels(chip_level, decay * even + odd, decay * decay)
    else:
        level_before = earlier_chips(chip_level, decay * decay)
    level_own = decay * level_before + level_even
    level_own = jnp.where(is_odd, decay * level_own + level_odd, level_own)
    band = level_own / lax.axis_size("chan") + TINY_LEVEL

    projected, high, low = pl.pallas_call(
        null_kernel,
        out_shape=(
            jax.ShapeDtypeStruct((rows, width), F32),
            jax.ShapeDtypeStruct((2 * rows, width), BF16),
            jax.ShapeDtypeStruct((2 * rows, width), BF16),
        ),
        in_specs=[SM, SM, VM],
        out_specs=(VM, VM, VM),
        cost_estimate=pl.CostEstimate(
            flops=4 * rows * width * 128, bytes_accessed=rows * width * 6, transcendentals=0
        ),
        compiler_params=PARAMS,
        name="null",
    )(picks, angles, voltage)

    cov, square, stats = pl.pallas_call(
        square_kernel,
        out_shape=(
            jax.ShapeDtypeStruct((width, antennas), F32),
            jax.ShapeDtypeStruct((width, antennas), F32),
            jax.ShapeDtypeStruct((16, 128), F32),
        ),
        in_specs=[SM, VM, VM],
        out_specs=(VM, VM, VM),
        cost_estimate=pl.CostEstimate(
            flops=6 * width * width * antennas, bytes_accessed=width * antennas * 8, transcendentals=0
        ),
        compiler_params=PARAMS,
        name="square",
    )(parity, own, other)

    cleaned = pl.pallas_call(
        whiten_kernel,
        out_shape=jax.ShapeDtypeStruct((rows, width), F32),
        in_specs=[VM] * 7,
        out_specs=pl.BlockSpec(memory_space=pl.ANY),
        scratch_shapes=[pltpu.VMEM((rows, width), F32), pltpu.SemaphoreType.DMA((CHUNKS,))],
        cost_estimate=pl.CostEstimate(
            flops=12 * rows * width * width, bytes_accessed=rows * width * 8, transcendentals=0
        ),
        compiler_params=PARAMS,
        name="whiten",
    )(band, stats, cov, square, projected, high, low)
    return cleaned[None]


def solution(mesh):
    placed = (P("chan", "tm", None), P("chan", None), P())
    return jax.shard_map(steps, mesh=mesh, in_specs=placed, out_specs=P("chan", "tm", None), check_vma=False)
```

```python
import jax
import jax.numpy as jnp
from jax import lax
from jax.experimental import pallas as pl
from jax.experimental.pallas import tpu as pltpu
from jax.sharding import PartitionSpec as P


SEG = 256
HORIZON = 256
LANES = 128
CHUNKS = 4
DIRECT = 4
LOADING = 0.1
STEER_LOADING = 0.05
TINY_LEVEL = 1e-06
PRECISE = lax.Precision.HIGHEST
F32 = jnp.float32
BF16 = jnp.bfloat16
VM = pl.BlockSpec(memory_space=pltpu.VMEM)
SM = pl.BlockSpec(memory_space=pltpu.SMEM)
PARAMS = pltpu.CompilerParams(vmem_limit_bytes=24 * 2**20)


def gram_kernel(part_ref, volts_ref, out_ref, *power_ref):
    antennas = volts_ref.shape[1] // 2
    segments = volts_ref.shape[0] // SEG
    half, lanes = antennas // 2, out_ref.shape[1]
    forget = 1.0 - 1.0 / HORIZON
    start = pl.multiple_of(part_ref[0] * half, half)
    mixed = power = None
    for seg in range(segments):
        rows = slice(seg * SEG, (seg + 1) * SEG)
        a, b = volts_ref[rows, :antennas], volts_ref[rows, antennas:]
        a_t = volts_ref[rows, pl.ds(start, half)].T
        b_t = volts_ref[rows, pl.ds(antennas + start, half)].T
        left = jnp.concatenate([a_t, b_t, b_t, -a_t], axis=1)
        right = jnp.concatenate([a, b, a, b], axis=0)
        term = jnp.dot(left, right, preferred_element_type=F32)
        mixed = term if mixed is None else forget * mixed + term
        if power_ref:
            squares = a.astype(F32) ** 2 + b.astype(F32) ** 2
            squares = jnp.sum(squares.reshape(-1, 8, antennas), axis=0)
            power = squares if power is None else forget * power + squares
    if power_ref:
        power_ref[0][...] = jnp.broadcast_to(
            jnp.sum(power, keepdims=True) / antennas, power_ref[0].shape
        )
    for n in range(antennas // lanes):
        out_ref[n * half : (n + 1) * half, :] = mixed[:, n * lanes : (n + 1) * lanes]


def split(value):
    high = value.astype(BF16)
    return high, (value - high.astype(F32)).astype(BF16)


def dot3(left, right):
    (lh, ll), (rh, rl) = left, right
    return (
        jnp.dot(lh, rh, preferred_element_type=F32)
        + jnp.dot(lh, rl, preferred_element_type=F32)
        + jnp.dot(ll, rh, preferred_element_type=F32)
    )


def beside(first, second):
    return jnp.concatenate([first, second], axis=1)


def over(first, second):
    return jnp.concatenate([first, second], axis=0)


def turn(u, v):
    parts = zip(split(u), split(v), strict=True)
    return tuple(over(beside(p, q), beside(q, -p)) for p, q in parts)


def square_kernel(parity_ref, own_ref, other_ref, cov_ref, square_ref, stats_ref):
    antennas, lanes = cov_ref.shape[1], own_ref.shape[1]
    half = antennas // 2
    is_odd = parity_ref[0] == 1
    blocks = [slice(n * half, (n + 1) * half) for n in range(antennas // lanes)]
    mixed = over(
        jnp.concatenate([jnp.where(is_odd, other_ref[b, :], own_ref[b, :]) for b in blocks], axis=1),
        jnp.concatenate([jnp.where(is_odd, own_ref[b, :], other_ref[b, :]) for b in blocks], axis=1),
    )
    flipped = mixed.T
    re, im = 0.5 * (mixed + flipped), 0.5 * (mixed - flipped)
    cov_ref[:antennas, :], cov_ref[antennas:, :] = re, im
    (rh, rl), (ih, il) = split(re), split(im)
    (sh, sl), (fh, fl) = split(mixed), split(flipped)
    product = dot3((beside(sh, fh), beside(sl, fl)), (over(rh, ih), over(rl, il)))
    turned = product.T
    square_ref[:antennas, :], square_ref[antennas:, :] = 0.5 * (product + turned), 0.5 * (product - turned)
    row = lax.broadcasted_iota(jnp.int32, mixed.shape, 0)
    column = lax.broadcasted_iota(jnp.int32, mixed.shape, 1)
    trace = jnp.sum(jnp.where(row == column, mixed, 0.0), keepdims=True)
    norm = jnp.sum(mixed * mixed, keepdims=True)
    stats_ref[:8, :] = jnp.broadcast_to(norm, (8, stats_ref.shape[1]))
    stats_ref[8:, :] = jnp.broadcast_to(trace, (8, stats_ref.shape[1]))


def whiten_kernel(
    band_ref, stats_ref, cov_ref, square_ref, w_ref, high_ref, low_ref, out_ref, done_ref, sems
):
    samples = w_ref.shape[0]
    antennas = cov_ref.shape[1]
    size = samples // CHUNKS

    def wide(row):
        return jnp.concatenate([row] * (antennas // row.shape[1]), axis=1)

    norm, trace, band = wide(stats_ref[0:1, :]), wide(stats_ref[8:9, :]), wide(band_ref[0:1, :])
    beta = 1.0 / band
    total = 2.0 * (beta * (beta * norm + 2.0 * LOADING * trace) + LOADING * LOADING * antennas)
    omega = 1.0 / jnp.sqrt(total)
    slope, shift = omega * beta, omega * LOADING
    cov, square = cov_ref[...], square_ref[...]
    bend = (slope * slope) * square
    first = split(bend + (2.0 * slope * (shift - 1.0)) * cov)
    second = split((slope * (3.0 - 2.0 * shift)) * cov - bend)
    left, right = slice(0, antennas), slice(antennas, 2 * antennas)
    keep_first, keep_second = 2.0 + shift * (shift - 2.0), 2.0 - shift * (3.0 - shift)

    def begin(n):
        both = slice(2 * n * size, 2 * (n + 1) * size)
        return dot3((high_ref[both, :], low_ref[both, :]), first)

    steps = [begin(n) for n in range(CHUNKS)]
    for n, step in enumerate(steps):
        rows = slice(n * size, (n + 1) * size)
        w_u, w_v = w_ref[rows, left], w_ref[rows, right]
        u, v = keep_first * w_u + step[:size], keep_first * w_v + step[size:]
        step = dot3(turn(u, v), second)
        done_ref[rows, left] = omega * (w_u + keep_second * u - step[:size])
        done_ref[rows, right] = omega * (w_v + keep_second * v - step[size:])
        pltpu.make_async_copy(done_ref.at[rows], out_ref.at[rows], sems.at[n]).start()
    for n in range(CHUNKS):
        rows = slice(n * size, (n + 1) * size)
        pltpu.make_async_copy(done_ref.at[rows], out_ref.at[rows], sems.at[n]).wait()


def complex_inverse(re, im):
    size = re.shape[0]
    row = lax.broadcasted_iota(jnp.int32, re.shape, 0)
    column = lax.broadcasted_iota(jnp.int32, re.shape, 1)
    for j in range(size):
        here = column[:1] == j
        col_re, col_im = re[:, j : j + 1], im[:, j : j + 1]
        scale = 1.0 / re[j : j + 1, j : j + 1]
        row_re = jnp.where(here, scale, re[j : j + 1] * scale)
        row_im = jnp.where(here, 0.0, im[j : j + 1] * scale)
        rest_re, rest_im = jnp.where(column == j, 0.0, re), jnp.where(column == j, 0.0, im)
        rest_re = rest_re - (col_re * row_re - col_im * row_im)
        rest_im = rest_im - (col_re * row_im + col_im * row_re)
        re = jnp.where(row == j, row_re, rest_re)
        im = jnp.where(row == j, row_im, rest_im)
    return re, im


def across(left, right):
    return lax.dot_general(
        left, right, (((1,), (1,)), ((), ())), precision=PRECISE, preferred_element_type=F32
    )


def null_kernel(picks_ref, angles_ref, volts_ref, out_ref, high_ref, low_ref):
    antennas = volts_ref.shape[1] // 2
    count = picks_ref.shape[1]
    row = lax.broadcasted_iota(jnp.int32, (count, 128), 0)
    angle = jnp.zeros((count, 128), F32)
    for k in range(count):
        angle = jnp.where(row == k, angles_ref[picks_ref[0, k]], angle)
    rate = (jnp.pi * jnp.sin(angle))[:, :1]
    position = lax.broadcasted_iota(jnp.int32, (count, antennas), 1).astype(F32)
    phase = rate * position
    norming = antennas**0.5
    re, im = jnp.cos(phase) / norming, jnp.sin(phase) / norming
    both = jnp.concatenate([re, im], axis=1)
    turned = jnp.concatenate([-im, re], axis=1)
    eye = lax.broadcasted_iota(jnp.int32, (count, count), 0) == lax.broadcasted_iota(
        jnp.int32, (count, count), 1
    )
    gram_re = across(both, both) + jnp.where(eye, STEER_LOADING, 0.0)
    gram_im = across(both, turned)
    inv_re, inv_im = complex_inverse(gram_re, gram_im)
    steer = jnp.concatenate([both, turned], axis=0)
    inverse = jnp.concatenate(
        [
            jnp.concatenate([inv_re, inv_im], axis=1),
            jnp.concatenate([-inv_im, inv_re], axis=1),
        ],
        axis=0,
    )
    back = jnp.dot(inverse, steer, precision=PRECISE, preferred_element_type=F32)
    volts = volts_ref[...]
    nt = (((1,), (1,)), ((), ()))
    inner = sum(
        lax.dot_general(volts, part, nt, preferred_element_type=F32) for part in split(steer)
    )
    nulled = volts.astype(F32) - dot3(split(inner), split(back))
    out_ref[...] = nulled
    size = volts.shape[0] // CHUNKS
    for n in range(CHUNKS):
        rows, both = slice(n * size, (n + 1) * size), slice(2 * n * size, 2 * (n + 1) * size)
        high, low = turn(nulled[rows, :antennas], nulled[rows, antennas:])
        high_ref[both, :], low_ref[both, :] = high, low


def exchange(value, axis, mask):
    return lax.ppermute(value, axis, [(i, i ^ mask) for i in range(lax.axis_size(axis))])


def choose(index, values):
    chosen = jnp.asarray(values[0], F32)
    for i, value in enumerate(values[1:], 1):
        chosen = jnp.where(index == i, value, chosen)
    return chosen


def earlier_chips(value, decay, mirrored=False, rider=None):
    chips = lax.axis_size("tm") // 2
    chip = lax.axis_index("tm") // 2
    length, total, before = 1, value, None
    while length < chips:
        last = 2 * length == chips
        mask = 2 * length - 1 if mirrored else length
        rows = total.shape[0]
        if last and rider is not None:
            total = jnp.concatenate([total, rider], axis=0)
        got = exchange(total, "tm", 2 * mask)
        if last and rider is not None:
            got, rider = got[:rows], got[rows:]
        upper = (chip // length) % 2 == 1
        weight = jnp.where(upper, choose(chip % length, [decay**i for i in range(length)]), 0.0)
        before = weight * got if before is None else before + weight * got
        if not last:
            far = decay**length
            total = jnp.where(upper, 1.0, far) * total + jnp.where(upper, far, 1.0) * got
        length *= 2
    before = jnp.zeros_like(value) if before is None else before
    return before if rider is None else (before, rider)


def earlier_levels(level, opposite, decay):
    chips = lax.axis_size("tm") // 2
    chip = lax.axis_index("tm") // 2
    near, far = jnp.zeros_like(level), None
    for mask in range(1, chips):
        weights = [decay ** (c - 1 - (c ^ mask)) if c ^ mask < c else 0.0 for c in range(chips)]
        if mask == chips - 1:
            far = choose(chip, weights) * opposite
        else:
            near = near + choose(chip, weights) * exchange(level, "tm", 2 * mask)
    return near + far


def sum_groups(value):
    groups = lax.axis_size("chan")
    if groups & (groups - 1):
        return lax.psum(value, "chan")
    step = 1
    while step < groups:
        got = exchange(value, "chan", step)
        value = value + got
        step *= 2
    return value


def steps(volts, picks, angles):
    voltage = volts[0]
    rows, width = voltage.shape
    antennas = width // 2
    half = antennas // 2
    segments = rows // SEG
    core = lax.axis_index("tm") % 2
    parity = core.reshape(1).astype(jnp.int32)
    is_odd = core == 1
    decay = (1.0 - 1.0 / HORIZON) ** segments

    def gram(part, *more):
        return pl.pallas_call(
            gram_kernel,
            out_shape=(jax.ShapeDtypeStruct((half * antennas // LANES, LANES), F32), *more),
            in_specs=[SM, VM],
            out_specs=(VM,) * (1 + len(more)),
            cost_estimate=pl.CostEstimate(
                flops=2 * rows * width * antennas, bytes_accessed=rows * width * 2, transcendentals=0
            ),
            compiler_params=PARAMS,
        )(part, voltage)

    give, power = gram(1 - parity, jax.ShapeDtypeStruct((8, LANES), F32))
    (keep,) = gram(parity)
    got = exchange(give, "tm", 1)
    mine, theirs = jnp.where(is_odd, 1.0, decay), jnp.where(is_odd, decay, 1.0)
    pair = mine * keep + theirs * got
    tall = keep.shape[0]
    level = sum_groups(power)
    direct = lax.axis_size("tm") // 2 == DIRECT
    opposite = None
    if direct:
        before, opposite = earlier_chips(pair, decay * decay, True, level)
    else:
        before = earlier_chips(pair, decay * decay, True)
    even_cov = decay * before + jnp.where(is_odd, got, keep)
    odd_cov = decay * decay * before + pair
    own = jnp.where(is_odd, odd_cov, even_cov)
    other = jnp.where(is_odd, even_cov, odd_cov)
    if direct:
        other = jnp.concatenate([other, opposite], axis=0)
    other = exchange(other, "tm", 1)

    def parities(mine, theirs):
        return jnp.where(is_odd, theirs, mine), jnp.where(is_odd, mine, theirs)

    level_even, level_odd = parities(level, exchange(level, "tm", 1))
    chip_level = decay * level_even + level_odd
    if direct:
        even, odd = parities(opposite, other[tall:])
        level_before = earlier_levels(chip_level, decay * even + odd, decay * decay)
    else:
        level_before = earlier_chips(chip_level, decay * decay)
    level_own = decay * level_before + level_even
    level_own = jnp.where(is_odd, decay * level_own + level_odd, level_own)
    band = level_own / lax.axis_size("chan") + TINY_LEVEL

    projected, high, low = pl.pallas_call(
        null_kernel,
        out_shape=(
            jax.ShapeDtypeStruct((rows, width), F32),
            jax.ShapeDtypeStruct((2 * rows, width), BF16),
            jax.ShapeDtypeStruct((2 * rows, width), BF16),
        ),
        in_specs=[SM, SM, VM],
        out_specs=(VM, VM, VM),
        cost_estimate=pl.CostEstimate(
            flops=4 * rows * width * 128, bytes_accessed=rows * width * 6, transcendentals=0
        ),
        compiler_params=PARAMS,
        name="null",
    )(picks, angles, voltage)

    cov, square, stats = pl.pallas_call(
        square_kernel,
        out_shape=(
            jax.ShapeDtypeStruct((width, antennas), F32),
            jax.ShapeDtypeStruct((width, antennas), F32),
            jax.ShapeDtypeStruct((16, 128), F32),
        ),
        in_specs=[SM, VM, VM],
        out_specs=(VM, VM, VM),
        cost_estimate=pl.CostEstimate(
            flops=6 * width * width * antennas, bytes_accessed=width * antennas * 8, transcendentals=0
        ),
        compiler_params=PARAMS,
        name="square",
    )(parity, own, other)

    cleaned = pl.pallas_call(
        whiten_kernel,
        out_shape=jax.ShapeDtypeStruct((rows, width), F32),
        in_specs=[VM] * 7,
        out_specs=pl.BlockSpec(memory_space=pl.ANY),
        scratch_shapes=[pltpu.VMEM((rows, width), F32), pltpu.SemaphoreType.DMA((CHUNKS,))],
        cost_estimate=pl.CostEstimate(
            flops=12 * rows * width * width, bytes_accessed=rows * width * 8, transcendentals=0
        ),
        compiler_params=PARAMS,
        name="whiten",
    )(band, stats, cov, square, projected, high, low)
    return cleaned[None]


def solution(mesh):
    placed = (P("chan", "tm", None), P("chan", None), P())
    return jax.shard_map(steps, mesh=mesh, in_specs=placed, out_specs=P("chan", "tm", None), check_vma=False)
```

```python
import jax
import jax.numpy as jnp
from jax import lax
from jax.experimental import pallas as pl
from jax.experimental.pallas import tpu as pltpu
from jax.sharding import PartitionSpec as P


SEG = 256
HORIZON = 256
LANES = 128
CHUNKS = 4
DIRECT = 4
LOADING = 0.1
STEER_LOADING = 0.05
TINY_LEVEL = 1e-06
PRECISE = lax.Precision.HIGHEST
F32 = jnp.float32
BF16 = jnp.bfloat16
VM = pl.BlockSpec(memory_space=pltpu.VMEM)
SM = pl.BlockSpec(memory_space=pltpu.SMEM)
PARAMS = pltpu.CompilerParams(vmem_limit_bytes=24 * 2**20)


def gram_kernel(part_ref, volts_ref, out_ref, *power_ref):
    antennas = volts_ref.shape[1] // 2
    segments = volts_ref.shape[0] // SEG
    half, lanes = antennas // 2, out_ref.shape[1]
    forget = 1.0 - 1.0 / HORIZON
    start = pl.multiple_of(part_ref[0] * half, half)
    mixed = power = None
    for seg in range(segments):
        rows = slice(seg * SEG, (seg + 1) * SEG)
        a, b = volts_ref[rows, :antennas], volts_ref[rows, antennas:]
        a_t = volts_ref[rows, pl.ds(start, half)].T
        b_t = volts_ref[rows, pl.ds(antennas + start, half)].T
        left = jnp.concatenate([a_t, b_t, b_t, -a_t], axis=1)
        right = jnp.concatenate([a, b, a, b], axis=0)
        term = jnp.dot(left, right, preferred_element_type=F32)
        mixed = term if mixed is None else forget * mixed + term
        if power_ref:
            squares = a.astype(F32) ** 2 + b.astype(F32) ** 2
            squares = jnp.sum(squares.reshape(-1, 8, antennas), axis=0)
            power = squares if power is None else forget * power + squares
    if power_ref:
        power_ref[0][...] = jnp.broadcast_to(
            jnp.sum(power, keepdims=True) / antennas, power_ref[0].shape
        )
    for n in range(antennas // lanes):
        out_ref[n * half : (n + 1) * half, :] = mixed[:, n * lanes : (n + 1) * lanes]


def split(value):
    high = value.astype(BF16)
    return high, (value - high.astype(F32)).astype(BF16)


def dot3(left, right):
    (lh, ll), (rh, rl) = left, right
    count = lh.shape[0]
    both = jnp.dot(jnp.concatenate([lh, ll], axis=0), rh, preferred_element_type=F32)
    return both[:count] + both[count:] + jnp.dot(lh, rl, preferred_element_type=F32)


def beside(first, second):
    return jnp.concatenate([first, second], axis=1)


def over(first, second):
    return jnp.concatenate([first, second], axis=0)


def turn(u, v):
    parts = zip(split(u), split(v), strict=True)
    return tuple(over(beside(p, q), beside(q, -p)) for p, q in parts)


def square_kernel(parity_ref, own_ref, other_ref, cov_ref, square_ref, stats_ref):
    antennas, lanes = cov_ref.shape[1], own_ref.shape[1]
    half = antennas // 2
    is_odd = parity_ref[0] == 1
    blocks = [slice(n * half, (n + 1) * half) for n in range(antennas // lanes)]
    mixed = over(
        jnp.concatenate([jnp.where(is_odd, other_ref[b, :], own_ref[b, :]) for b in blocks], axis=1),
        jnp.concatenate([jnp.where(is_odd, own_ref[b, :], other_ref[b, :]) for b in blocks], axis=1),
    )
    flipped = mixed.T
    re, im = 0.5 * (mixed + flipped), 0.5 * (mixed - flipped)
    cov_ref[:antennas, :], cov_ref[antennas:, :] = re, im
    (rh, rl), (ih, il) = split(re), split(im)
    (sh, sl), (fh, fl) = split(mixed), split(flipped)
    product = dot3((beside(sh, fh), beside(sl, fl)), (over(rh, ih), over(rl, il)))
    turned = product.T
    square_ref[:antennas, :], square_ref[antennas:, :] = 0.5 * (product + turned), 0.5 * (product - turned)
    row = lax.broadcasted_iota(jnp.int32, mixed.shape, 0)
    column = lax.broadcasted_iota(jnp.int32, mixed.shape, 1)
    trace = jnp.sum(jnp.where(row == column, mixed, 0.0), keepdims=True)
    norm = jnp.sum(mixed * mixed, keepdims=True)
    stats_ref[:8, :] = jnp.broadcast_to(norm, (8, stats_ref.shape[1]))
    stats_ref[8:, :] = jnp.broadcast_to(trace, (8, stats_ref.shape[1]))


def whiten_kernel(
    band_ref, stats_ref, cov_ref, square_ref, w_ref, high_ref, low_ref, out_ref, done_ref, sems
):
    samples = w_ref.shape[0]
    antennas = cov_ref.shape[1]
    size = samples // CHUNKS

    def wide(row):
        return jnp.concatenate([row] * (antennas // row.shape[1]), axis=1)

    norm, trace, band = wide(stats_ref[0:1, :]), wide(stats_ref[8:9, :]), wide(band_ref[0:1, :])
    beta = 1.0 / band
    total = 2.0 * (beta * (beta * norm + 2.0 * LOADING * trace) + LOADING * LOADING * antennas)
    omega = 1.0 / jnp.sqrt(total)
    slope, shift = omega * beta, omega * LOADING
    cov, square = cov_ref[...], square_ref[...]
    bend = (slope * slope) * square
    first = split(bend + (2.0 * slope * (shift - 1.0)) * cov)
    second = split((slope * (3.0 - 2.0 * shift)) * cov - bend)
    left, right = slice(0, antennas), slice(antennas, 2 * antennas)
    keep_first, keep_second = 2.0 + shift * (shift - 2.0), 2.0 - shift * (3.0 - shift)

    def begin(n):
        both = slice(2 * n * size, 2 * (n + 1) * size)
        return dot3((high_ref[both, :], low_ref[both, :]), first)

    steps = [begin(n) for n in range(CHUNKS)]
    for n, step in enumerate(steps):
        rows = slice(n * size, (n + 1) * size)
        w_u, w_v = w_ref[rows, left], w_ref[rows, right]
        u, v = keep_first * w_u + step[:size], keep_first * w_v + step[size:]
        step = dot3(turn(u, v), second)
        done_ref[rows, left] = omega * (w_u + keep_second * u - step[:size])
        done_ref[rows, right] = omega * (w_v + keep_second * v - step[size:])
        pltpu.make_async_copy(done_ref.at[rows], out_ref.at[rows], sems.at[n]).start()
    for n in range(CHUNKS):
        rows = slice(n * size, (n + 1) * size)
        pltpu.make_async_copy(done_ref.at[rows], out_ref.at[rows], sems.at[n]).wait()


def complex_inverse(re, im):
    size = re.shape[0]
    row = lax.broadcasted_iota(jnp.int32, re.shape, 0)
    column = lax.broadcasted_iota(jnp.int32, re.shape, 1)
    for j in range(size):
        here = column[:1] == j
        col_re, col_im = re[:, j : j + 1], im[:, j : j + 1]
        scale = 1.0 / re[j : j + 1, j : j + 1]
        row_re = jnp.where(here, scale, re[j : j + 1] * scale)
        row_im = jnp.where(here, 0.0, im[j : j + 1] * scale)
        rest_re, rest_im = jnp.where(column == j, 0.0, re), jnp.where(column == j, 0.0, im)
        rest_re = rest_re - (col_re * row_re - col_im * row_im)
        rest_im = rest_im - (col_re * row_im + col_im * row_re)
        re = jnp.where(row == j, row_re, rest_re)
        im = jnp.where(row == j, row_im, rest_im)
    return re, im


def across(left, right):
    return lax.dot_general(
        left, right, (((1,), (1,)), ((), ())), precision=PRECISE, preferred_element_type=F32
    )


def null_kernel(picks_ref, angles_ref, volts_ref, out_ref, high_ref, low_ref):
    antennas = volts_ref.shape[1] // 2
    count = picks_ref.shape[1]
    row = lax.broadcasted_iota(jnp.int32, (count, 128), 0)
    angle = jnp.zeros((count, 128), F32)
    for k in range(count):
        angle = jnp.where(row == k, angles_ref[picks_ref[0, k]], angle)
    rate = (jnp.pi * jnp.sin(angle))[:, :1]
    position = lax.broadcasted_iota(jnp.int32, (count, antennas), 1).astype(F32)
    phase = rate * position
    norming = antennas**0.5
    re, im = jnp.cos(phase) / norming, jnp.sin(phase) / norming
    both = jnp.concatenate([re, im], axis=1)
    turned = jnp.concatenate([-im, re], axis=1)
    eye = lax.broadcasted_iota(jnp.int32, (count, count), 0) == lax.broadcasted_iota(
        jnp.int32, (count, count), 1
    )
    gram_re = across(both, both) + jnp.where(eye, STEER_LOADING, 0.0)
    gram_im = across(both, turned)
    inv_re, inv_im = complex_inverse(gram_re, gram_im)
    steer = jnp.concatenate([both, turned], axis=0)
    inverse = jnp.concatenate(
        [
            jnp.concatenate([inv_re, inv_im], axis=1),
            jnp.concatenate([-inv_im, inv_re], axis=1),
        ],
        axis=0,
    )
    back = jnp.dot(inverse, steer, precision=PRECISE, preferred_element_type=F32)
    volts = volts_ref[...]
    nt = (((1,), (1,)), ((), ()))
    inner = sum(
        lax.dot_general(volts, part, nt, preferred_element_type=F32) for part in split(steer)
    )
    nulled = volts.astype(F32) - dot3(split(inner), split(back))
    out_ref[...] = nulled
    size = volts.shape[0] // CHUNKS
    for n in range(CHUNKS):
        rows, both = slice(n * size, (n + 1) * size), slice(2 * n * size, 2 * (n + 1) * size)
        high, low = turn(nulled[rows, :antennas], nulled[rows, antennas:])
        high_ref[both, :], low_ref[both, :] = high, low


def exchange(value, axis, mask):
    return lax.ppermute(value, axis, [(i, i ^ mask) for i in range(lax.axis_size(axis))])


def choose(index, values):
    chosen = jnp.asarray(values[0], F32)
    for i, value in enumerate(values[1:], 1):
        chosen = jnp.where(index == i, value, chosen)
    return chosen


def earlier_chips(value, decay, mirrored=False, rider=None):
    chips = lax.axis_size("tm") // 2
    chip = lax.axis_index("tm") // 2
    length, total, before = 1, value, None
    while length < chips:
        last = 2 * length == chips
        mask = 2 * length - 1 if mirrored else length
        rows = total.shape[0]
        if last and rider is not None:
            total = jnp.concatenate([total, rider], axis=0)
        got = exchange(total, "tm", 2 * mask)
        if last and rider is not None:
            got, rider = got[:rows], got[rows:]
        upper = (chip // length) % 2 == 1
        weight = jnp.where(upper, choose(chip % length, [decay**i for i in range(length)]), 0.0)
        before = weight * got if before is None else before + weight * got
        if not last:
            far = decay**length
            total = jnp.where(upper, 1.0, far) * total + jnp.where(upper, far, 1.0) * got
        length *= 2
    before = jnp.zeros_like(value) if before is None else before
    return before if rider is None else (before, rider)


def earlier_levels(level, opposite, decay):
    chips = lax.axis_size("tm") // 2
    chip = lax.axis_index("tm") // 2
    near, far = jnp.zeros_like(level), None
    for mask in range(1, chips):
        weights = [decay ** (c - 1 - (c ^ mask)) if c ^ mask < c else 0.0 for c in range(chips)]
        if mask == chips - 1:
            far = choose(chip, weights) * opposite
        else:
            near = near + choose(chip, weights) * exchange(level, "tm", 2 * mask)
    return near + far


def sum_groups(value):
    groups = lax.axis_size("chan")
    if groups & (groups - 1):
        return lax.psum(value, "chan")
    step = 1
    while step < groups:
        got = exchange(value, "chan", step)
        value = value + got
        step *= 2
    return value


def steps(volts, picks, angles):
    voltage = volts[0]
    rows, width = voltage.shape
    antennas = width // 2
    half = antennas // 2
    segments = rows // SEG
    core = lax.axis_index("tm") % 2
    parity = core.reshape(1).astype(jnp.int32)
    is_odd = core == 1
    decay = (1.0 - 1.0 / HORIZON) ** segments

    def gram(part, *more):
        return pl.pallas_call(
            gram_kernel,
            out_shape=(jax.ShapeDtypeStruct((half * antennas // LANES, LANES), F32), *more),
            in_specs=[SM, VM],
            out_specs=(VM,) * (1 + len(more)),
            cost_estimate=pl.CostEstimate(
                flops=2 * rows * width * antennas, bytes_accessed=rows * width * 2, transcendentals=0
            ),
            compiler_params=PARAMS,
        )(part, voltage)

    give, power = gram(1 - parity, jax.ShapeDtypeStruct((8, LANES), F32))
    (keep,) = gram(parity)
    got = exchange(give, "tm", 1)
    mine, theirs = jnp.where(is_odd, 1.0, decay), jnp.where(is_odd, decay, 1.0)
    pair = mine * keep + theirs * got
    tall = keep.shape[0]
    level = sum_groups(power)
    direct = lax.axis_size("tm") // 2 == DIRECT
    opposite = None
    if direct:
        before, opposite = earlier_chips(pair, decay * decay, True, level)
    else:
        before = earlier_chips(pair, decay * decay, True)
    even_cov = decay * before + jnp.where(is_odd, got, keep)
    odd_cov = decay * decay * before + pair
    own = jnp.where(is_odd, odd_cov, even_cov)
    other = jnp.where(is_odd, even_cov, odd_cov)
    if direct:
        other = jnp.concatenate([other, opposite], axis=0)
    other = exchange(other, "tm", 1)

    def parities(mine, theirs):
        return jnp.where(is_odd, theirs, mine), jnp.where(is_odd, mine, theirs)

    level_even, level_odd = parities(level, exchange(level, "tm", 1))
    chip_level = decay * level_even + level_odd
    if direct:
        even, odd = parities(opposite, other[tall:])
        level_before = earlier_levels(chip_level, decay * even + odd, decay * decay)
    else:
        level_before = earlier_chips(chip_level, decay * decay)
    level_own = decay * level_before + level_even
    level_own = jnp.where(is_odd, decay * level_own + level_odd, level_own)
    band = level_own / lax.axis_size("chan") + TINY_LEVEL

    projected, high, low = pl.pallas_call(
        null_kernel,
        out_shape=(
            jax.ShapeDtypeStruct((rows, width), F32),
            jax.ShapeDtypeStruct((2 * rows, width), BF16),
            jax.ShapeDtypeStruct((2 * rows, width), BF16),
        ),
        in_specs=[SM, SM, VM],
        out_specs=(VM, VM, VM),
        cost_estimate=pl.CostEstimate(
            flops=4 * rows * width * 128, bytes_accessed=rows * width * 6, transcendentals=0
        ),
        compiler_params=PARAMS,
        name="null",
    )(picks, angles, voltage)

    cov, square, stats = pl.pallas_call(
        square_kernel,
        out_shape=(
            jax.ShapeDtypeStruct((width, antennas), F32),
            jax.ShapeDtypeStruct((width, antennas), F32),
            jax.ShapeDtypeStruct((16, 128), F32),
        ),
        in_specs=[SM, VM, VM],
        out_specs=(VM, VM, VM),
        cost_estimate=pl.CostEstimate(
            flops=6 * width * width * antennas, bytes_accessed=width * antennas * 8, transcendentals=0
        ),
        compiler_params=PARAMS,
        name="square",
    )(parity, own, other)

    cleaned = pl.pallas_call(
        whiten_kernel,
        out_shape=jax.ShapeDtypeStruct((rows, width), F32),
        in_specs=[VM] * 7,
        out_specs=pl.BlockSpec(memory_space=pl.ANY),
        scratch_shapes=[pltpu.VMEM((rows, width), F32), pltpu.SemaphoreType.DMA((CHUNKS,))],
        cost_estimate=pl.CostEstimate(
            flops=12 * rows * width * width, bytes_accessed=rows * width * 8, transcendentals=0
        ),
        compiler_params=PARAMS,
        name="whiten",
    )(band, stats, cov, square, projected, high, low)
    return cleaned[None]


def solution(mesh):
    placed = (P("chan", "tm", None), P("chan", None), P())
    return jax.shard_map(steps, mesh=mesh, in_specs=placed, out_specs=P("chan", "tm", None), check_vma=False)
```
